128 devices in a mesh: tm: 8 (over z, core), row: 16 (over y, x).
Axes of the slice: x: 4, y: 4, z: 4, core: 2. Of those that a mesh axis runs over, the one named last changes fastest.
Arguments:
- visible: bfloat16 [8, 16, 16, 4, 1024], P('tm', 'row'), may hold values from -6 to 6
- slot_pos: int32 [8, 16, 16, 4], P('tm', 'row'), may hold values from -1 to 255, as said below
- window_shift: int32 [2, 2], replicated, may hold values from 0 to 3, as said below
- mask_token: bfloat16 [1024], replicated, may hold values from -6 to 6
- w_qkv: bfloat16 [1024, 3072], replicated, may hold values from -6.25 to 6.25
- w_out: bfloat16 [1024, 1024], replicated, may hold values from -0.1875 to 0.1875
- w_head: bfloat16 [1024, 1536], replicated, may hold values from -0.1875 to 0.1875
- pixels: bfloat16 [32, 64, 16, 1536], P('tm', 'row'), may hold values from 0 to 1
Outputs:
- d_visible: bfloat16 [8, 16, 16, 4, 1024], P('tm', 'row')
- d_mask_token: float32 [1024], replicated
The draws below stay inside these ranges and needn't reach their ends.
Inputs may be any that keep to these rules, and one draw needn't show every extreme that they name: Each live entry slot_pos[i, s, d, c] is a token index of decoder shard (i, d) in frame, row, column order; the live entries aimed at one shard (i, d) are distinct; every slot slot_pos[i, s, s, c] is live, so each shard receives all 4 slots from the packed shard of its own band; other slots are live or -1 at rates that differ from packed shard to packed shard. window_shift[0, g] lies in 0 to 1 and window_shift[1, g] in 0 to 3; some block of columns has row offset 4 - 1 and some block has frame offset 0.
All inputs are finite; a program needn't handle non-finite values.
Results may differ from the reference program's by a relative error of at most 0.014.
Values may be sent and summed in bfloat16 or wider, within the bound.
No kernel may reach another device: no remote copies, remote signals or barrier semaphores. Data moves between devices by JAX's collectives and lax.ppermute only.
A program may use at most 128 MiB of HBM per device.

```python
import math
import jax
import jax.numpy as jnp
from jax import lax

D = 1024
HEADS = 16
PIX = 1536
WT = 2
WH = 4
WW = 8
CAP = 4
TL = 4
HL = 4
W = 16
NT = 32
NH = 64
TOKENS = 32768
N_TM = 8
N_ROW = 16


def draw_w_qkv(key, part):
    base = jnp.clip(jax.random.normal(key, (D, 3 * D), jnp.float32), -5.0, 5.0) * D ** (-0.5)
    return base.astype(jnp.bfloat16)


def draw_window_shift(key, part):
    group_count = W // WW
    frame_offsets = jax.random.randint(jax.random.fold_in(key, 31), (group_count,), 0, WT)
    row_offsets = jax.random.randint(jax.random.fold_in(key, 32), (group_count,), 0, WH)
    row_pick = jax.random.randint(jax.random.fold_in(key, 33), (), 0, group_count)
    frame_pick = jax.random.randint(jax.random.fold_in(key, 34), (), 0, group_count)
    group_ids = jnp.arange(group_count, dtype=jnp.int32)
    row_offsets = jnp.where(group_ids == row_pick, WH - 1, row_offsets)
    frame_offsets = jnp.where(group_ids == frame_pick, 0, frame_offsets)
    return jnp.stack([frame_offsets, row_offsets], axis=0).astype(jnp.int32)


def draw_slot_pos(key, part):
    tokens = TL * HL * W
    groups = N_TM * N_ROW

    def one_group(group_key):
        return jax.random.permutation(group_key, tokens)[:N_ROW * CAP]
    chosen = jax.vmap(one_group)(jax.random.split(key, groups)).reshape(N_TM, N_ROW, N_ROW, CAP)
    keep_rates = jax.random.randint(jax.random.fold_in(key, 11), (N_TM, 1, N_ROW, 1), 15, 66)
    roll_values = jax.random.randint(jax.random.fold_in(key, 12), (N_TM, N_ROW, N_ROW, CAP), 0, 100)
    same_peer = (jnp.arange(N_ROW)[:, None] == jnp.arange(N_ROW)[None, :])[None, :, :, None]
    is_live = (roll_values < keep_rates) | same_peer
    placed = jnp.where(is_live, chosen, -1)
    return jnp.transpose(placed, (0, 2, 1, 3)).astype(jnp.int32)


def levels(rng, dims, shards, least, largest):
    level = 1.0
    for axis_at, parts in shards:
        draws = jax.random.uniform(jax.random.fold_in(jax.random.fold_in(rng, 6), axis_at), (parts,), jnp.float32, least / len(shards), largest / len(shards))
        level = level * jnp.repeat(jnp.exp(draws), dims[axis_at] // parts).reshape((-1,) + (1,) * (len(dims) - 1 - axis_at))
    return level


def centred(stream_key, dims, deviation, limit, shards=(), kind=jnp.bfloat16):
    drawn = deviation * jax.random.normal(stream_key, dims, jnp.float32)
    if shards:
        drawn = drawn * levels(stream_key, dims, shards, -0.22, 0.18)
    return jnp.clip(drawn, -limit, limit).astype(kind)


def setup_inputs(seed: int = 0) -> dict:
    streams_of = jax.random.split(jax.random.key(seed), 9)
    return {
        "visible": centred(streams_of[0], (N_TM, N_ROW, N_ROW, CAP, D), 1.0, 6.0, ((0, 8), (1, 16))),
        "slot_pos": draw_slot_pos(jax.random.fold_in(streams_of[8], 71), 0),
        "window_shift": draw_window_shift(jax.random.fold_in(streams_of[8], 71), 0),
        "mask_token": centred(streams_of[3], (D,), 1.0, 6.0),
        "w_qkv": draw_w_qkv(jax.random.fold_in(streams_of[8], 71), 0),
        "w_out": centred(streams_of[5], (D, D), D ** -0.5, 0.1875),
        "w_head": centred(streams_of[6], (D, PIX), D ** -0.5, 0.1875),
        "pixels": jnp.clip(1.0 * jax.random.uniform(streams_of[7], (NT, NH, W, PIX), jnp.float32) ** levels(streams_of[7], (NT, NH, W, PIX), ((0, 8), (1, 16)), -0.2, 0.2), 0.0, 1.0).astype(jnp.bfloat16),
    }


def layer_norm(values):
    center = values - lax.optimization_barrier(jnp.mean(values, axis=-1, keepdims=True))
    return center * lax.rsqrt(lax.optimization_barrier(jnp.mean(center * center, axis=-1, keepdims=True)) + 1e-05)

def sinusoid(coordinate, channel_count):
    half_count = channel_count // 2
    frequency = jnp.exp(-math.log(10000.0) * jnp.arange(half_count, dtype=jnp.float32) / half_count)
    angles = coordinate.astype(jnp.float32)[..., None] * frequency
    return jnp.concatenate([jnp.sin(angles), jnp.cos(angles)], axis=-1)

def position_table(frame_pos, row_pos, column_pos, model_width):
    quarter = model_width // 4
    remainder = (model_width - quarter) // 2
    return jnp.concatenate([sinusoid(frame_pos, quarter), sinusoid(row_pos, remainder), sinusoid(column_pos, model_width - quarter - remainder)], axis=-1)

def window_core(grid_block, w_qkv, w_out):
    frame_count, row_count, column_count, model_width = grid_block.shape
    head_dim = model_width // HEADS
    normed = layer_norm(grid_block).astype(jnp.bfloat16)
    packed = jnp.dot(normed.reshape(-1, model_width), w_qkv, preferred_element_type=jnp.float32).astype(jnp.bfloat16)
    packed = packed.reshape(frame_count // WT, WT, row_count // WH, WH, column_count // WW, WW, 3, HEADS, head_dim)
    packed = packed.transpose(6, 0, 2, 4, 7, 1, 3, 5, 8).reshape(3, -1, HEADS, WT * WH * WW, head_dim)
    scores = jnp.einsum('nhqe,nhke->nhqk', packed[0].astype(jnp.float32), packed[1].astype(jnp.float32)) * head_dim ** (-0.5)
    weights = jax.nn.softmax(scores, axis=-1).astype(jnp.bfloat16)
    mixed_heads = jnp.einsum('nhqk,nhke->nhqe', weights.astype(jnp.float32), packed[2].astype(jnp.float32)).astype(jnp.bfloat16)
    mixed_heads = mixed_heads.reshape(frame_count // WT, row_count // WH, column_count // WW, HEADS, WT, WH, WW, head_dim)
    mixed_heads = mixed_heads.transpose(0, 4, 1, 5, 2, 6, 3, 7).reshape(-1, model_width)
    result_rows = jnp.dot(mixed_heads, w_out, preferred_element_type=jnp.float32)
    return result_rows.reshape(frame_count, row_count, column_count, model_width)

def pixel_gradient(stream_rows, pixel_rows, masked, w_head):
    row_total, pixel_count = pixel_rows.shape
    group_size = pixel_count // 3
    raw_pixels = pixel_rows.astype(jnp.float32).reshape(row_total, 3, group_size)
    center = raw_pixels - lax.optimization_barrier(jnp.mean(raw_pixels, axis=-1, keepdims=True))
    spread = jnp.sqrt(lax.optimization_barrier(jnp.sum(center * center, axis=-1, keepdims=True)) / (group_size - 1))
    target = (center / (spread + 1e-06)).reshape(row_total, pixel_count)

    def pixel_loss(values):
        normed = layer_norm(values).astype(jnp.bfloat16)
        predicted = jnp.dot(normed, w_head, preferred_element_type=jnp.float32)
        errors = predicted - target
        return 0.5 * jnp.sum(masked[:, None] * errors * errors)
    return jax.grad(pixel_loss)(stream_rows)

def reference(visible, slot_pos, window_shift, mask_token, w_qkv, w_out, w_head, pixels):
    is_live = slot_pos >= 0
    local_pos = jnp.where(is_live, slot_pos, 0).astype(jnp.int32)
    slab_index = jnp.arange(N_TM, dtype=jnp.int32)[:, None, None, None]
    band_index = jnp.arange(N_ROW, dtype=jnp.int32)[None, None, :, None]
    frame_pos = slab_index * TL + local_pos // (HL * W)
    row_pos = band_index * HL + local_pos // W % HL
    global_pos = (frame_pos * NH + row_pos) * W + local_pos % W
    global_pos = jnp.where(is_live, global_pos, TOKENS).astype(jnp.int32).reshape(-1)
    live_flat = is_live.reshape(-1)
    visible_grid = jnp.zeros((TOKENS, D), jnp.float32).at[global_pos].set(visible.reshape(-1, D).astype(jnp.float32), mode='drop')
    seen_flags = jnp.zeros((TOKENS,), jnp.float32).at[global_pos].set(1.0, mode='drop')
    token_index = jnp.arange(TOKENS, dtype=jnp.int32)
    position_rows = position_table(token_index // (NH * W), token_index // W % NH, token_index % W, D)
    start_rows = jnp.where(seen_flags[:, None] > 0, visible_grid, mask_token.astype(jnp.float32)[None, :])
    embedded = (start_rows + position_rows).astype(jnp.bfloat16)
    stream = embedded.astype(jnp.float32).reshape(NT, NH, W, D)

    def attend(grid_block):
        results = []
        for group in range(W // WW):
            piece = grid_block[:, :, group * WW:(group + 1) * WW]
            time_offset = window_shift[0, group]
            row_offset = window_shift[1, group]
            rolled = jnp.roll(piece, (time_offset, row_offset), axis=(0, 1))
            results.append(jnp.roll(window_core(rolled, w_qkv, w_out), (-time_offset, -row_offset), axis=(0, 1)))
        return jnp.concatenate(results, axis=2)
    attn_full, pull_back = jax.vjp(attend, stream)
    attn_value = attn_full.astype(jnp.bfloat16)
    residual = stream + attn_value.astype(jnp.float32)
    masked = 1.0 - seen_flags
    grad_stream = pixel_gradient(residual.reshape(TOKENS, D), pixels.reshape(TOKENS, PIX), masked, w_head)
    grad_attn = lax.optimization_barrier(grad_stream.astype(jnp.bfloat16)).astype(jnp.float32)
    grad_core = pull_back(grad_attn.reshape(NT, NH, W, D))[0]
    grad_embedded = grad_stream + grad_core.reshape(TOKENS, D)
    picked = grad_embedded[jnp.minimum(global_pos, TOKENS - 1)] * live_flat[:, None].astype(jnp.float32)
    d_visible = picked.astype(jnp.bfloat16).reshape(visible.shape)
    d_mask_token = lax.optimization_barrier(jnp.sum(masked[:, None] * grad_embedded, axis=0)) * TOKENS ** (-0.5)
    return (d_visible, d_mask_token)
```

```python
import math

import jax
import jax.numpy as jnp
from jax import lax
from jax.experimental import pallas as pl
from jax.experimental.pallas import tpu as pltpu
from jax.sharding import Mesh
from jax.sharding import PartitionSpec as P

WT = 2
WH = 4
WW = 8
D = 1024
PIX = 1536
GROUP = PIX // 3
TOK = 256
WIN = WT * WH * WW
PAIRS = D // 128
SLOTS = 128
TM = ("tm_0", "tm_1")
ROW = ("row_0", "row_1")
ALL = TM + ROW
BF = jnp.bfloat16
F32 = jnp.float32
NT_DIMS = (((1,), (1,)), ((), ()))
TN_DIMS = (((0,), (0,)), ((), ()))
NN_DIMS = (((1,), (0,)), ((), ()))
VMEM = pltpu.MemorySpace.VMEM
SMEM = pltpu.MemorySpace.SMEM


def dot(a, b, dims):
    return lax.dot_general(a, b, dims, preferred_element_type=F32)


def lane_mean(values):
    return jnp.sum(values, axis=-1, keepdims=True) * (1.0 / values.shape[-1])


def normalise(values):
    center = values - lane_mean(values)
    scale = lax.rsqrt(lane_mean(center * center) + 1e-05)
    return center * scale, scale


def normalise_back(cotangent, normed, scale):
    return scale * (cotangent - lane_mean(cotangent) - normed * lane_mean(cotangent * normed))


def two_heads(rows):
    first = lax.broadcasted_iota(jnp.int32, rows.shape, 1) < 64
    zero = jnp.zeros_like(rows)
    return jnp.concatenate([jnp.where(first, rows, zero), jnp.where(first, zero, rows)], axis=0)


def own_head(rows):
    first = lax.broadcasted_iota(jnp.int32, (WIN, 128), 1) < 64
    return jnp.where(first, rows[:WIN], rows[WIN:])


def slot_one_hot(shift_ref, rows_ref, behind):
    place = rows_ref[:, D : D + 128].astype(F32).astype(jnp.int32)
    frame = place >> 6
    row = (place >> 4) & 3
    column = place & 15
    group = column >> 3
    slot = lax.broadcasted_iota(jnp.int32, (SLOTS, 128), 0) & 7
    lane = lax.broadcasted_iota(jnp.int32, (SLOTS, 128), 1)
    time_offset = jnp.where(group == 0, shift_ref[0, 0], shift_ref[0, 1])
    row_offset = jnp.where(group == 0, shift_ref[1, 0], shift_ref[1, 1])
    frame = frame + time_offset - 4 * behind
    row = row + row_offset - jnp.where(slot >= 4, 4, 0)
    inside = (place >= 0) & (frame >= 0) & (frame < 4) & (row >= 0) & (row < 4)
    token = (((frame >> 1) * 2 + group) * 64) + ((frame & 1) * 32) + row * 8 + (column & 7)
    token = jnp.where(inside, token, -1)
    halves = [jnp.where(token == lane + 128 * half, 1.0, 0.0) for half in range(2)]
    return jnp.concatenate(halves, axis=1).astype(BF)


def forward_kernel(
    shift_ref, own_ref, behind_ref, mask_ref, frames_ref, rows_ref, columns_ref, w_qkv_hbm, w_out_hbm,
    embedded_ref, residual_ref, qkv_ref, probs_ref, seen_ref, one_hot_ref,
    w_qkv_ref, w_out_ref, chosen_ref, normed_ref, heads_ref, sems,
):
    copies = [
        pltpu.make_async_copy(
            w_qkv_hbm.at[:, pl.ds(at * D, D)], w_qkv_ref.at[:, pl.ds(at * D, D)], sems.at[at]
        )
        for at in range(3)
    ]
    copies.append(pltpu.make_async_copy(w_out_hbm, w_out_ref, sems.at[3]))
    for copy in copies:
        copy.start()
    one_hot_ref[:SLOTS] = slot_one_hot(shift_ref, own_ref, 0)
    one_hot_ref[SLOTS:] = slot_one_hot(shift_ref, behind_ref, 1)
    own_hot = one_hot_ref[:SLOTS]
    behind_hot = one_hot_ref[SLOTS:]
    chosen_ref[...] = dot(own_hot, own_ref[:, :D], TN_DIMS) + dot(behind_hot, behind_ref[:, :D], TN_DIMS)
    ones = jnp.ones((2 * SLOTS, 128), BF)
    seen_ref[...] = dot(one_hot_ref[...], ones, TN_DIMS)

    for block in range(TOK // 16):
        window, half = divmod(block, 4)
        frame_pair, group = divmod(window, 2)
        at_frame = group * 4 + frame_pair * 2 + half // 2
        rows = pl.ds(block * 16, 16)
        start = jnp.where(
            jnp.concatenate([seen_ref[rows]] * 8, axis=1) > 0,
            chosen_ref[rows],
            mask_ref[...].astype(F32),
        )
        position = []
        for at in range(2):
            at_row = group * 4 + (half % 2) * 2 + at
            position.append(
                jnp.concatenate(
                    [
                        jnp.broadcast_to(frames_ref[at_frame : at_frame + 1], (8, 256)),
                        jnp.broadcast_to(rows_ref[at_row : at_row + 1], (8, 384)),
                        columns_ref[group * 8 : group * 8 + 8],
                    ],
                    axis=1,
                )
            )
        embedded = (start + jnp.concatenate(position, axis=0)).astype(BF)
        embedded_ref[rows] = embedded
        normed_ref[rows] = normalise(embedded.astype(F32))[0].astype(BF)

    for at in range(3):
        copies[at].wait()
        for part in range(2):
            cols = slice(at * D + part * 512, at * D + part * 512 + 512)
            qkv_ref[:, cols] = dot(normed_ref[...], w_qkv_ref[:, cols], NN_DIMS).astype(BF)

    def one_window(window, carry):
        rows = pl.ds(pl.multiple_of(window * WIN, WIN), WIN)
        for pair in range(PAIRS):
            cols = slice(pair * 128, pair * 128 + 128)
            q = qkv_ref[rows, pair * 128 : pair * 128 + 128]
            k = qkv_ref[rows, D + pair * 128 : D + pair * 128 + 128]
            v = qkv_ref[rows, 2 * D + pair * 128 : 2 * D + pair * 128 + 128]
            scores = dot(k, two_heads(q), NT_DIMS) * 0.125
            weights = jnp.exp(scores - jnp.max(scores, axis=0, keepdims=True))
            probs = (weights * (1.0 / jnp.sum(weights, axis=0, keepdims=True))).astype(BF)
            probs_ref[window, pair] = probs
            heads_ref[rows, cols] = own_head(dot(probs, v, TN_DIMS)).astype(BF)
        return carry

    lax.fori_loop(0, TOK // WIN, one_window, 0)
    copies[3].wait()
    for part in range(2):
        cols = slice(part * 512, part * 512 + 512)
        attn = dot(heads_ref[...], w_out_ref[:, cols], NN_DIMS).astype(BF)
        residual_ref[:, cols] = embedded_ref[:, cols].astype(F32) + attn.astype(F32)


def backward_kernel(
    shift_ref, embedded_ref, residual_ref, qkv_ref, probs_ref, seen_ref, one_hot_ref,
    own_px, row_px, time_px, corner_px, w_head_hbm, w_out_hbm, w_qkv_hbm,
    picked_ref, total_ref,
    px_ref, w_head_ref, w_out_ref, w_qkv_ref, normed_ref, scale_ref, predicted_ref, error_ref,
    narrow_ref, wide_ref, stream_ref, dqkv_ref, sems,
):
    pixel_copies = [
        pltpu.make_async_copy(own_px, px_ref.at[pl.ds(1, 4), pl.ds(3, 4)], sems.at[0]),
        pltpu.make_async_copy(row_px, px_ref.at[pl.ds(1, 4), pl.ds(0, 3)], sems.at[1]),
        pltpu.make_async_copy(time_px, px_ref.at[pl.ds(0, 1), pl.ds(3, 4)], sems.at[2]),
        pltpu.make_async_copy(corner_px, px_ref.at[pl.ds(0, 1), pl.ds(0, 3)], sems.at[3]),
    ]
    head_copy = pltpu.make_async_copy(w_head_hbm, w_head_ref, sems.at[4])
    out_copy = pltpu.make_async_copy(w_out_hbm, w_out_ref, sems.at[5])
    qkv_copy = pltpu.make_async_copy(w_qkv_hbm, w_qkv_ref, sems.at[6])
    head_copy.start()
    for copy in pixel_copies:
        copy.start()
    out_copy.start()
    qkv_copy.start()

    def tokens_of(block):
        return pl.ds(pl.multiple_of(block * 16, 16), 16)

    def head_norm(block, carry):
        rows = tokens_of(block)
        normed, scale = normalise(residual_ref[rows])
        normed_ref[rows] = normed
        scale_ref[rows] = jnp.broadcast_to(scale, (16, 128))
        narrow_ref[rows] = normed.astype(BF)
        return carry

    lax.fori_loop(0, TOK // 16, head_norm, 0, unroll=2)
    head_copy.wait()
    for copy in pixel_copies:
        copy.wait()
    for part in range(3):
        cols = slice(part * GROUP, part * GROUP + GROUP)
        predicted_ref[...] = dot(narrow_ref[...], w_head_ref[:, cols], NN_DIMS)

        def pixel_block(block, carry, cols=cols):
            at_frame = block // 2
            half = block % 2
            for group in range(2):
                rows = tokens_of(((at_frame // 2) * 2 + group) * 4 + (at_frame % 2) * 2 + half)
                targets = []
                for at in range(2):
                    raw = px_ref[
                        at_frame - shift_ref[0, group] + 1,
                        half * 2 + at - shift_ref[1, group] + 3,
                        group * 8 : group * 8 + 8,
                        cols,
                    ].astype(F32)
                    center = raw - lane_mean(raw)
                    spread = jnp.sqrt(jnp.sum(center * center, axis=-1, keepdims=True) * (1.0 / (GROUP - 1)))
                    targets.append(center * (1.0 / (spread + 1e-06)))
                masked = 1.0 - jnp.concatenate([seen_ref[rows]] * 4, axis=1)
                gap = predicted_ref[rows] - jnp.concatenate(targets, axis=0)
                error_ref[rows, cols] = (masked * gap).astype(BF)
            return carry

        lax.fori_loop(0, 8, pixel_block, 0)

    for part in range(2):
        cols = slice(part * 512, part * 512 + 512)
        wide_ref[:, cols] = dot(error_ref[...], w_head_ref[cols, :], NT_DIMS)

    def head_norm_back(block, carry):
        rows = tokens_of(block)
        scale = jnp.concatenate([scale_ref[rows]] * 8, axis=1)
        cotangent = wide_ref[rows].astype(BF).astype(F32)
        grad = normalise_back(cotangent, normed_ref[rows], scale)
        stream_ref[rows] = grad
        narrow_ref[rows] = grad.astype(BF)
        return carry

    lax.fori_loop(0, TOK // 16, head_norm_back, 0, unroll=2)
    out_copy.wait()
    d_heads = dot(narrow_ref[...], w_out_ref[...], NT_DIMS).astype(BF)
    narrow_ref[...] = d_heads

    def one_window(window, carry):
        rows = pl.ds(pl.multiple_of(window * WIN, WIN), WIN)
        for pair in range(PAIRS):
            cols = [slice(at * D + pair * 128, at * D + pair * 128 + 128) for at in range(3)]
            q_heads = two_heads(qkv_ref[rows, cols[0]])
            k = qkv_ref[rows, cols[1]]
            v = qkv_ref[rows, cols[2]]
            out_heads = two_heads(narrow_ref[rows, cols[0]])
            narrow_probs = probs_ref[window, pair]
            probs = narrow_probs.astype(F32)
            d_probs = dot(v, out_heads, NT_DIMS).astype(BF).astype(F32)
            mean = jnp.sum(d_probs * probs, axis=0, keepdims=True)
            d_scores = (probs * (d_probs - mean) * 0.125).astype(BF)
            dqkv_ref[rows, cols[2]] = dot(narrow_probs, out_heads, NN_DIMS).astype(BF)
            dqkv_ref[rows, cols[1]] = dot(d_scores, q_heads, NN_DIMS).astype(BF)
            dqkv_ref[rows, cols[0]] = own_head(dot(d_scores, k, TN_DIMS)).astype(BF)
        return carry

    lax.fori_loop(0, TOK // WIN, one_window, 0)
    qkv_copy.wait()
    for part in range(2):
        cols = slice(part * 512, part * 512 + 512)
        wide_ref[:, cols] = dot(dqkv_ref[...], w_qkv_ref[cols, :], NT_DIMS)

    def first_norm_back(block, carry):
        rows = tokens_of(block)
        normed, scale = normalise(embedded_ref[rows].astype(F32))
        cotangent = wide_ref[rows].astype(BF).astype(F32)
        grad = stream_ref[rows] + normalise_back(cotangent, normed, scale)
        narrow_ref[rows] = grad.astype(BF)
        masked = 1.0 - jnp.concatenate([seen_ref[rows]] * 8, axis=1)
        part = masked * grad
        return carry + part[:8] + part[8:]

    total_ref[...] = lax.fori_loop(0, TOK // 16, first_norm_back, jnp.zeros((8, D), F32), unroll=2)
    picked_ref[...] = dot(one_hot_ref[...], narrow_ref[...], NN_DIMS).astype(BF)


def sinusoid(coordinate, channel_count):
    half_count = channel_count // 2
    frequency = jnp.exp(-math.log(10000.0) * jnp.arange(half_count, dtype=F32) / half_count)
    angles = coordinate.astype(F32)[..., None] * frequency
    return jnp.concatenate([jnp.sin(angles), jnp.cos(angles)], axis=-1)


def move(value, axis, steps):
    count = lax.axis_size(axis)
    return lax.ppermute(value, axis, [(at, (at + steps) % count) for at in range(count)])


def move_corner(value):
    count_tm = lax.axis_size(TM)
    count_row = lax.axis_size(ROW)
    pairs = [
        (i * count_row + d, (i + 1) % count_tm * count_row + (d + 1) % count_row)
        for i in range(count_tm)
        for d in range(count_row)
    ]
    return lax.ppermute(value, ALL, pairs)


def per_device(visible, slot_pos, window_shift, mask_token, w_qkv, w_out, w_head, pixels):
    frame_count, row_count = pixels.shape[:2]
    peers, slots = slot_pos.shape[2:]
    rows = visible.reshape(peers, slots, D)
    places = slot_pos.reshape(peers, slots).astype(BF)
    packed = jnp.concatenate([rows, jnp.broadcast_to(places[..., None], (peers, slots, 128))], axis=-1)
    packed = jnp.concatenate([packed, jnp.roll(packed, 1, axis=0)], axis=1)
    own = lax.all_to_all(packed, ROW, split_axis=0, concat_axis=0, tiled=True).reshape(SLOTS, D + 128)
    behind = move(own, TM, 1)

    row_px = move(pixels[:, 1:], ROW, 1)
    time_px = move(pixels[3:], TM, 1)
    corner_px = move_corner(pixels[3:, 1:])

    local = jnp.arange(4, dtype=jnp.int32)
    frame_total = frame_count * lax.axis_size(TM)
    row_total = row_count * lax.axis_size(ROW)
    frames = (lax.axis_index(TM) * frame_count + local[None] - window_shift[0][:, None]) % frame_total
    band = (lax.axis_index(ROW) * row_count + local[None] - window_shift[1][:, None]) % row_total
    frame_table = sinusoid(frames.reshape(-1), 256)
    row_table = sinusoid(band.reshape(-1), 384)
    column_table = sinusoid(jnp.arange(16, dtype=jnp.int32), 384)

    vmem = pl.BlockSpec(memory_space=VMEM)
    smem = pl.BlockSpec(memory_space=SMEM)
    hbm = pl.BlockSpec(memory_space=pl.ANY)
    embedded, residual, qkv, probs, seen, one_hot = pl.pallas_call(
        forward_kernel,
        name="forward_part",
        in_specs=[smem] + [vmem] * 6 + [hbm] * 2,
        out_specs=[vmem] * 6,
        out_shape=[
            jax.ShapeDtypeStruct((TOK, D), BF),
            jax.ShapeDtypeStruct((TOK, D), F32),
            jax.ShapeDtypeStruct((TOK, 3 * D), BF),
            jax.ShapeDtypeStruct((TOK // WIN, PAIRS, WIN, 128), BF),
            jax.ShapeDtypeStruct((TOK, 128), F32),
            jax.ShapeDtypeStruct((2 * SLOTS, TOK), BF),
        ],
        scratch_shapes=[
            pltpu.VMEM((D, 3 * D), BF),
            pltpu.VMEM((D, D), BF),
            pltpu.VMEM((TOK, D), F32),
            pltpu.VMEM((TOK, D), BF),
            pltpu.VMEM((TOK, D), BF),
            pltpu.SemaphoreType.DMA((4,)),
        ],
        compiler_params=pltpu.CompilerParams(vmem_limit_bytes=28 << 20),
    )(
        window_shift, own, behind, mask_token.reshape(1, D), frame_table, row_table, column_table,
        w_qkv, w_out,
    )
    picked, total = pl.pallas_call(
        backward_kernel,
        name="backward_part",
        in_specs=[smem] + [vmem] * 6 + [hbm] * 7,
        out_specs=[vmem] * 2,
        out_shape=[
            jax.ShapeDtypeStruct((2 * SLOTS, D), BF),
            jax.ShapeDtypeStruct((8, D), F32),
        ],
        scratch_shapes=[
            pltpu.VMEM((5, 7, 16, PIX), BF),
            pltpu.VMEM((D, PIX), BF),
            pltpu.VMEM((D, D), BF),
            pltpu.VMEM((D, 3 * D), BF),
            pltpu.VMEM((TOK, D), F32),
            pltpu.VMEM((TOK, 128), F32),
            pltpu.VMEM((TOK, GROUP), F32),
            pltpu.VMEM((TOK, PIX), BF),
            pltpu.VMEM((TOK, D), BF),
            pltpu.VMEM((TOK, D), F32),
            pltpu.VMEM((TOK, D), F32),
            pltpu.VMEM((TOK, 3 * D), BF),
            pltpu.SemaphoreType.DMA((7,)),
        ],
        compiler_params=pltpu.CompilerParams(vmem_limit_bytes=36 << 20),
    )(
        window_shift, embedded, residual, qkv, probs, seen, one_hot,
        pixels, row_px, time_px, corner_px, w_head, w_out, w_qkv,
    )
    mine = picked[:SLOTS] + move(picked[SLOTS:], TM, -1)
    local_total = jnp.sum(total, axis=0).reshape(8, 128)
    local_total = local_total + move(local_total, "tm_1", 1)
    turned = [move(local_total, "tm_0", step) for step in (1, 2, 3)]
    local_total = (local_total + turned[1]) + (turned[0] + turned[2])
    high = local_total.astype(BF)
    low = (local_total - high.astype(F32)).astype(BF)
    sums = jnp.broadcast_to(jnp.concatenate([high, low], axis=1)[None], (peers, 8, 256))
    sent = jnp.concatenate([mine.reshape(peers, 2 * slots, D), sums], axis=-1)
    back = lax.all_to_all(sent, ROW, split_axis=0, concat_axis=0, tiled=True)
    d_visible = back[:, :slots, :D] + jnp.roll(back[:, slots:, :D], -1, axis=0)
    halves = jnp.sum(back[:, :, D:].astype(F32), axis=0)
    grad_scale = (frame_total * row_total * pixels.shape[2]) ** (-0.5)
    d_mask = (halves[:, :128] + halves[:, 128:]).reshape(D) * grad_scale
    return (d_visible.reshape(visible.shape), d_mask)


def solution(mesh):
    torus = Mesh(mesh.devices.reshape(4, 2, 4, 4), ALL)
    return jax.shard_map(
        per_device,
        mesh=torus,
        in_specs=(
            P(TM, ROW, None, None, None),
            P(TM, ROW, None, None),
            P(),
            P(),
            P(),
            P(),
            P(),
            P(TM, ROW, None, None),
        ),
        out_specs=(P(TM, ROW, None, None, None), P()),
        check_vma=False,
    )
```

```python
import math

import jax
import jax.numpy as jnp
from jax import lax
from jax.experimental import pallas as pl
from jax.experimental.pallas import tpu as pltpu
from jax.sharding import Mesh
from jax.sharding import PartitionSpec as P

WT = 2
WH = 4
WW = 8
D = 1024
PIX = 1536
GROUP = PIX // 3
TOK = 256
WIN = WT * WH * WW
PAIRS = D // 128
SLOTS = 128
TM = ("tm_0", "tm_1")
ROW = ("row_0", "row_1")
ALL = TM + ROW
BF = jnp.bfloat16
F32 = jnp.float32
NT_DIMS = (((1,), (1,)), ((), ()))
TN_DIMS = (((0,), (0,)), ((), ()))
NN_DIMS = (((1,), (0,)), ((), ()))
VMEM = pltpu.MemorySpace.VMEM
SMEM = pltpu.MemorySpace.SMEM


def dot(a, b, dims):
    return lax.dot_general(a, b, dims, preferred_element_type=F32)


def lane_mean(values):
    return jnp.sum(values, axis=-1, keepdims=True) * (1.0 / values.shape[-1])


def normalise(values):
    center = values - lane_mean(values)
    scale = lax.rsqrt(lane_mean(center * center) + 1e-05)
    return center * scale, scale


def normalise_back(cotangent, normed, scale):
    return scale * (cotangent - lane_mean(cotangent) - normed * lane_mean(cotangent * normed))


def two_heads(rows):
    first = lax.broadcasted_iota(jnp.int32, rows.shape, 1) < 64
    zero = jnp.zeros_like(rows)
    return jnp.concatenate([jnp.where(first, rows, zero), jnp.where(first, zero, rows)], axis=0)


def own_head(rows):
    first = lax.broadcasted_iota(jnp.int32, (WIN, 128), 1) < 64
    return jnp.where(first, rows[:WIN], rows[WIN:])


def slot_one_hot(shift_ref, rows_ref, behind):
    place = rows_ref[:, D : D + 128].astype(F32).astype(jnp.int32)
    frame = place >> 6
    row = (place >> 4) & 3
    column = place & 15
    group = column >> 3
    slot = lax.broadcasted_iota(jnp.int32, (SLOTS, 128), 0) & 7
    lane = lax.broadcasted_iota(jnp.int32, (SLOTS, 128), 1)
    time_offset = jnp.where(group == 0, shift_ref[0, 0], shift_ref[0, 1])
    row_offset = jnp.where(group == 0, shift_ref[1, 0], shift_ref[1, 1])
    frame = frame + time_offset - 4 * behind
    row = row + row_offset - jnp.where(slot >= 4, 4, 0)
    inside = (place >= 0) & (frame >= 0) & (frame < 4) & (row >= 0) & (row < 4)
    token = (((frame >> 1) * 2 + group) * 64) + ((frame & 1) * 32) + row * 8 + (column & 7)
    token = jnp.where(inside, token, -1)
    halves = [jnp.where(token == lane + 128 * half, 1.0, 0.0) for half in range(2)]
    return jnp.concatenate(halves, axis=1).astype(BF)


def forward_kernel(
    shift_ref, own_ref, behind_ref, mask_ref, frames_ref, rows_ref, columns_ref, w_qkv_hbm, w_out_hbm,
    embedded_ref, residual_ref, qkv_ref, probs_ref, seen_ref, one_hot_ref,
    w_qkv_ref, w_out_ref, chosen_ref, normed_ref, heads_ref, sems,
):
    copies = [
        pltpu.make_async_copy(
            w_qkv_hbm.at[:, pl.ds(at * D, D)], w_qkv_ref.at[:, pl.ds(at * D, D)], sems.at[at]
        )
        for at in range(3)
    ]
    copies.append(pltpu.make_async_copy(w_out_hbm, w_out_ref, sems.at[3]))
    for copy in copies:
        copy.start()
    one_hot_ref[:SLOTS] = slot_one_hot(shift_ref, own_ref, 0)
    one_hot_ref[SLOTS:] = slot_one_hot(shift_ref, behind_ref, 1)
    own_hot = one_hot_ref[:SLOTS]
    behind_hot = one_hot_ref[SLOTS:]
    chosen_ref[...] = dot(own_hot, own_ref[:, :D], TN_DIMS) + dot(behind_hot, behind_ref[:, :D], TN_DIMS)
    ones = jnp.ones((2 * SLOTS, 128), BF)
    seen_ref[...] = dot(one_hot_ref[...], ones, TN_DIMS)

    for block in range(TOK // 16):
        window, half = divmod(block, 4)
        frame_pair, group = divmod(window, 2)
        at_frame = group * 4 + frame_pair * 2 + half // 2
        rows = pl.ds(block * 16, 16)
        start = jnp.where(
            jnp.concatenate([seen_ref[rows]] * 8, axis=1) > 0,
            chosen_ref[rows],
            mask_ref[...].astype(F32),
        )
        position = []
        for at in range(2):
            at_row = group * 4 + (half % 2) * 2 + at
            position.append(
                jnp.concatenate(
                    [
                        jnp.broadcast_to(frames_ref[at_frame : at_frame + 1], (8, 256)),
                        jnp.broadcast_to(rows_ref[at_row : at_row + 1], (8, 384)),
                        columns_ref[group * 8 : group * 8 + 8],
                    ],
                    axis=1,
                )
            )
        embedded = (start + jnp.concatenate(position, axis=0)).astype(BF)
        embedded_ref[rows] = embedded
        normed_ref[rows] = normalise(embedded.astype(F32))[0].astype(BF)

    for at in range(3):
        copies[at].wait()
        for part in range(2):
            cols = slice(at * D + part * 512, at * D + part * 512 + 512)
            qkv_ref[:, cols] = dot(normed_ref[...], w_qkv_ref[:, cols], NN_DIMS).astype(BF)

    def one_window(window):
        rows = slice(window * WIN, window * WIN + WIN)
        scores = []
        for pair in range(PAIRS):
            q = qkv_ref[rows, pair * 128 : pair * 128 + 128]
            k = qkv_ref[rows, D + pair * 128 : D + pair * 128 + 128]
            scores.append(dot(k, two_heads(q), NT_DIMS) * 0.125)
        probs = []
        for pair in range(PAIRS):
            weights = jnp.exp(scores[pair] - jnp.max(scores[pair], axis=0, keepdims=True))
            probs.append((weights * (1.0 / jnp.sum(weights, axis=0, keepdims=True))).astype(BF))
            probs_ref[window, pair] = probs[pair]
        for pair in range(PAIRS):
            v = qkv_ref[rows, 2 * D + pair * 128 : 2 * D + pair * 128 + 128]
            heads_ref[rows, pair * 128 : pair * 128 + 128] = own_head(dot(probs[pair], v, TN_DIMS)).astype(BF)

    for window in range(TOK // WIN):
        one_window(window)
    copies[3].wait()
    for part in range(2):
        cols = slice(part * 512, part * 512 + 512)
        attn = dot(heads_ref[...], w_out_ref[:, cols], NN_DIMS).astype(BF)
        residual_ref[:, cols] = embedded_ref[:, cols].astype(F32) + attn.astype(F32)


def backward_kernel(
    shift_ref, embedded_ref, residual_ref, qkv_ref, probs_ref, seen_ref, one_hot_ref,
    own_px, row_px, time_px, corner_px, w_head_hbm, w_out_hbm, w_qkv_hbm,
    picked_ref, total_ref,
    px_ref, w_head_ref, w_out_ref, w_qkv_ref, normed_ref, scale_ref, predicted_ref, error_ref,
    narrow_ref, wide_ref, stream_ref, dqkv_ref, sems,
):
    pixel_copy = pltpu.make_async_copy(own_px, px_ref.at[pl.ds(1, 4), pl.ds(3, 4)], sems.at[0])
    head_copy = pltpu.make_async_copy(w_head_hbm, w_head_ref, sems.at[1])
    out_copy = pltpu.make_async_copy(w_out_hbm, w_out_ref, sems.at[2])
    qkv_copy = pltpu.make_async_copy(w_qkv_hbm, w_qkv_ref, sems.at[3])
    head_copy.start()
    pixel_copy.start()
    out_copy.start()
    qkv_copy.start()
    px_ref[1:, :3] = row_px[...]
    px_ref[:1, 3:] = time_px[...]
    px_ref[:1, :3] = corner_px[...]

    def tokens_of(block):
        return pl.ds(pl.multiple_of(block * 16, 16), 16)

    def head_norm(block, carry):
        rows = tokens_of(block)
        normed, scale = normalise(residual_ref[rows])
        normed_ref[rows] = normed
        scale_ref[rows] = jnp.broadcast_to(scale, (16, 128))
        narrow_ref[rows] = normed.astype(BF)
        return carry

    lax.fori_loop(0, TOK // 16, head_norm, 0, unroll=16)
    head_copy.wait()
    pixel_copy.wait()
    for part in range(3):
        cols = slice(part * GROUP, part * GROUP + GROUP)
        predicted_ref[:, cols] = dot(narrow_ref[...], w_head_ref[:, cols], NN_DIMS)

    def pixel_block(block, carry):
        at_frame = block // 2
        half = block % 2
        for group in range(2):
            rows = tokens_of(((at_frame // 2) * 2 + group) * 4 + (at_frame % 2) * 2 + half)
            masked = 1.0 - jnp.concatenate([seen_ref[rows]] * 4, axis=1)
            for part in range(3):
                cols = slice(part * GROUP, part * GROUP + GROUP)
                targets = []
                for at in range(2):
                    raw = px_ref[
                        at_frame - shift_ref[0, group] + 1,
                        half * 2 + at - shift_ref[1, group] + 3,
                        group * 8 : group * 8 + 8,
                        cols,
                    ].astype(F32)
                    center = raw - lane_mean(raw)
                    spread = jnp.sqrt(jnp.sum(center * center, axis=-1, keepdims=True) * (1.0 / (GROUP - 1)))
                    targets.append(center * (1.0 / (spread + 1e-06)))
                gap = predicted_ref[rows, cols] - jnp.concatenate(targets, axis=0)
                error_ref[rows, cols] = (masked * gap).astype(BF)
        return carry

    lax.fori_loop(0, 8, pixel_block, 0, unroll=8)

    for part in range(2):
        cols = slice(part * 512, part * 512 + 512)
        wide_ref[:, cols] = dot(error_ref[...], w_head_ref[cols, :], NT_DIMS)

    def head_norm_back(block, carry):
        rows = tokens_of(block)
        scale = jnp.concatenate([scale_ref[rows]] * 8, axis=1)
        cotangent = wide_ref[rows].astype(BF).astype(F32)
        grad = normalise_back(cotangent, normed_ref[rows], scale)
        stream_ref[rows] = grad
        narrow_ref[rows] = grad.astype(BF)
        return carry

    lax.fori_loop(0, TOK // 16, head_norm_back, 0, unroll=16)
    out_copy.wait()
    d_heads = dot(narrow_ref[...], w_out_ref[...], NT_DIMS).astype(BF)
    narrow_ref[...] = d_heads

    def one_window(window):
        rows = slice(window * WIN, window * WIN + WIN)
        cols = [[slice(at * D + pair * 128, at * D + pair * 128 + 128) for at in range(3)] for pair in range(PAIRS)]
        d_probs = []
        out_heads = []
        for pair in range(PAIRS):
            out_heads.append(two_heads(narrow_ref[rows, cols[pair][0]]))
            d_probs.append(dot(qkv_ref[rows, cols[pair][2]], out_heads[pair], NT_DIMS))
        for pair in range(PAIRS):
            dqkv_ref[rows, cols[pair][2]] = dot(probs_ref[window, pair], out_heads[pair], NN_DIMS).astype(BF)
        d_scores = []
        for pair in range(PAIRS):
            probs = probs_ref[window, pair].astype(F32)
            cotangent = d_probs[pair].astype(BF).astype(F32)
            mean = jnp.sum(cotangent * probs, axis=0, keepdims=True)
            d_scores.append((probs * (cotangent - mean) * 0.125).astype(BF))
        for pair in range(PAIRS):
            q_heads = two_heads(qkv_ref[rows, cols[pair][0]])
            dqkv_ref[rows, cols[pair][1]] = dot(d_scores[pair], q_heads, NN_DIMS).astype(BF)
        for pair in range(PAIRS):
            d_q = own_head(dot(d_scores[pair], qkv_ref[rows, cols[pair][1]], TN_DIMS))
            dqkv_ref[rows, cols[pair][0]] = d_q.astype(BF)

    for window in range(TOK // WIN):
        one_window(window)
    qkv_copy.wait()
    for part in range(2):
        cols = slice(part * 512, part * 512 + 512)
        wide_ref[:, cols] = dot(dqkv_ref[...], w_qkv_ref[cols, :], NT_DIMS)

    def first_norm_back(block, carry):
        rows = tokens_of(block)
        normed, scale = normalise(embedded_ref[rows].astype(F32))
        cotangent = wide_ref[rows].astype(BF).astype(F32)
        grad = stream_ref[rows] + normalise_back(cotangent, normed, scale)
        narrow_ref[rows] = grad.astype(BF)
        masked = 1.0 - jnp.concatenate([seen_ref[rows]] * 8, axis=1)
        part = masked * grad
        return carry + part[:8] + part[8:]

    total_ref[...] = lax.fori_loop(0, TOK // 16, first_norm_back, jnp.zeros((8, D), F32), unroll=16)
    picked_ref[...] = dot(one_hot_ref[...], narrow_ref[...], NN_DIMS).astype(BF)


def forward_part(*operands):
    vmem = pl.BlockSpec(memory_space=VMEM)
    smem = pl.BlockSpec(memory_space=SMEM)
    hbm = pl.BlockSpec(memory_space=pltpu.MemorySpace.HBM)
    return pl.pallas_call(
        forward_kernel,
        name="forward_part",
        in_specs=[smem] + [vmem] * 6 + [hbm] * 2,
        out_specs=[vmem] * 6,
        out_shape=[
            jax.ShapeDtypeStruct((TOK, D), BF),
            jax.ShapeDtypeStruct((TOK, D), F32),
            jax.ShapeDtypeStruct((TOK, 3 * D), BF),
            jax.ShapeDtypeStruct((TOK // WIN, PAIRS, WIN, 128), BF),
            jax.ShapeDtypeStruct((TOK, 128), F32),
            jax.ShapeDtypeStruct((2 * SLOTS, TOK), BF),
        ],
        scratch_shapes=[
            pltpu.VMEM((D, 3 * D), BF),
            pltpu.VMEM((D, D), BF),
            pltpu.VMEM((TOK, D), F32),
            pltpu.VMEM((TOK, D), BF),
            pltpu.VMEM((TOK, D), BF),
            pltpu.SemaphoreType.DMA((4,)),
        ],
        compiler_params=pltpu.CompilerParams(vmem_limit_bytes=28 << 20),
    )(*operands)


def backward_part(*operands):
    vmem = pl.BlockSpec(memory_space=VMEM)
    smem = pl.BlockSpec(memory_space=SMEM)
    hbm = pl.BlockSpec(memory_space=pltpu.MemorySpace.HBM)
    return pl.pallas_call(
        backward_kernel,
        name="backward_part",
        in_specs=[smem] + [vmem] * 6 + [hbm] + [vmem] * 3 + [hbm] * 3,
        out_specs=[vmem] * 2,
        out_shape=[
            jax.ShapeDtypeStruct((2 * SLOTS, D), BF),
            jax.ShapeDtypeStruct((8, D), F32),
        ],
        scratch_shapes=[
            pltpu.VMEM((5, 7, 16, PIX), BF),
            pltpu.VMEM((D, PIX), BF),
            pltpu.VMEM((D, D), BF),
            pltpu.VMEM((D, 3 * D), BF),
            pltpu.VMEM((TOK, D), F32),
            pltpu.VMEM((TOK, 128), F32),
            pltpu.VMEM((TOK, PIX), F32),
            pltpu.VMEM((TOK, PIX), BF),
            pltpu.VMEM((TOK, D), BF),
            pltpu.VMEM((TOK, D), F32),
            pltpu.VMEM((TOK, D), F32),
            pltpu.VMEM((TOK, 3 * D), BF),
            pltpu.SemaphoreType.DMA((4,)),
        ],
        compiler_params=pltpu.CompilerParams(vmem_limit_bytes=36 << 20),
    )(*operands)


def sinusoid(coordinate, channel_count):
    half_count = channel_count // 2
    frequency = jnp.exp(-math.log(10000.0) * jnp.arange(half_count, dtype=F32) / half_count)
    angles = coordinate.astype(F32)[..., None] * frequency
    return jnp.concatenate([jnp.sin(angles), jnp.cos(angles)], axis=-1)


def move(value, axis, steps):
    count = lax.axis_size(axis)
    return lax.ppermute(value, axis, [(at, (at + steps) % count) for at in range(count)])


def move_corner(value):
    count_tm = lax.axis_size(TM)
    count_row = lax.axis_size(ROW)
    pairs = [
        (i * count_row + d, (i + 1) % count_tm * count_row + (d + 1) % count_row)
        for i in range(count_tm)
        for d in range(count_row)
    ]
    return lax.ppermute(value, ALL, pairs)


def per_device(visible, slot_pos, window_shift, mask_token, w_qkv, w_out, w_head, pixels):
    frame_count, row_count = pixels.shape[:2]
    peers, slots = slot_pos.shape[2:]
    rows = visible.reshape(peers, slots, D)
    places = slot_pos.reshape(peers, slots).astype(BF)
    packed = jnp.concatenate([rows, jnp.broadcast_to(places[..., None], (peers, slots, 128))], axis=-1)
    packed = jnp.concatenate([packed, jnp.roll(packed, 1, axis=0)], axis=1)
    own = lax.all_to_all(packed, ROW, split_axis=0, concat_axis=0, tiled=True).reshape(SLOTS, D + 128)
    behind = move(own, TM, 1)

    row_px = move(pixels[:, 1:], ROW, 1)
    time_px = move(pixels[3:], TM, 1)
    corner_px = move_corner(pixels[3:, 1:])

    local = jnp.arange(4, dtype=jnp.int32)
    frame_total = frame_count * lax.axis_size(TM)
    row_total = row_count * lax.axis_size(ROW)
    frames = (lax.axis_index(TM) * frame_count + local[None] - window_shift[0][:, None]) % frame_total
    band = (lax.axis_index(ROW) * row_count + local[None] - window_shift[1][:, None]) % row_total
    frame_table = sinusoid(frames.reshape(-1), 256)
    row_table = sinusoid(band.reshape(-1), 384)
    column_table = sinusoid(jnp.arange(16, dtype=jnp.int32), 384)

    w_qkv, w_out, w_head, own_px = (
        pltpu.with_memory_space_constraint(value, pltpu.MemorySpace.HBM)
        for value in (w_qkv, w_out, w_head, pixels)
    )
    kept = forward_part(
        window_shift, own, behind, mask_token.reshape(1, D), frame_table, row_table, column_table,
        w_qkv, w_out,
    )
    picked, total = backward_part(
        window_shift, *kept, own_px, row_px, time_px, corner_px, w_head, w_out, w_qkv
    )
    from_next = move(picked[SLOTS:], TM, -1)
    mine = picked[:SLOTS] + from_next
    local_total = jnp.sum(total, axis=0).reshape(8, 128)
    other = move(local_total, "tm_1", 1)
    local_total = local_total + other
    turned = [move(local_total, "tm_0", step) for step in (1, 2, 3)]
    local_total = (local_total + turned[1]) + (turned[0] + turned[2])
    high = local_total.astype(BF)
    low = (local_total - high.astype(F32)).astype(BF)
    sums = jnp.broadcast_to(jnp.concatenate([high, low], axis=1)[None], (peers, 8, 256))
    sent = jnp.concatenate([mine.reshape(peers, 2 * slots, D), sums], axis=-1)
    back = lax.all_to_all(sent, ROW, split_axis=0, concat_axis=0, tiled=True)
    d_visible = back[:, :slots, :D] + jnp.roll(back[:, slots:, :D], -1, axis=0)
    halves = jnp.sum(back[:, :, D:].astype(F32), axis=0)
    grad_scale = (frame_total * row_total * pixels.shape[2]) ** (-0.5)
    d_mask = (halves[:, :128] + halves[:, 128:]).reshape(D) * grad_scale
    return (d_visible.reshape(visible.shape), d_mask)


def solution(mesh):
    torus = Mesh(mesh.devices.reshape(4, 2, 4, 4), ALL)
    return jax.shard_map(
        per_device,
        mesh=torus,
        in_specs=(
            P(TM, ROW, None, None, None),
            P(TM, ROW, None, None),
            P(),
            P(),
            P(),
            P(),
            P(),
            P(TM, ROW, None, None),
        ),
        out_specs=(P(TM, ROW, None, None, None), P()),
        check_vma=False,
    )
```

```python
import functools
import math

import jax
import jax.numpy as jnp
from jax import lax
from jax.experimental import pallas as pl
from jax.experimental.pallas import tpu as pltpu
from jax.sharding import Mesh
from jax.sharding import PartitionSpec as P

WT = 2
WH = 4
WW = 8
D = 1024
PIX = 1536
GROUP = PIX // 3
TOK = 256
WIN = WT * WH * WW
PAIRS = D // 128
SLOTS = 128
TM = ("tm_0", "tm_1")
ROW = ("row_0", "row_1")
ALL = TM + ROW
BF = jnp.bfloat16
F32 = jnp.float32
NT_DIMS = (((1,), (1,)), ((), ()))
TN_DIMS = (((0,), (0,)), ((), ()))
NN_DIMS = (((1,), (0,)), ((), ()))
VMEM = pltpu.MemorySpace.VMEM
SMEM = pltpu.MemorySpace.SMEM


def dot(a, b, dims):
    return lax.dot_general(a, b, dims, preferred_element_type=F32)


def lane_mean(values):
    return jnp.sum(values, axis=-1, keepdims=True) * (1.0 / values.shape[-1])


def normalise(values):
    center = values - lane_mean(values)
    scale = lax.rsqrt(lane_mean(center * center) + 1e-05)
    return center * scale, scale


def normalise_back(cotangent, normed, scale):
    return scale * (cotangent - lane_mean(cotangent) - normed * lane_mean(cotangent * normed))


def two_heads(rows):
    first = lax.broadcasted_iota(jnp.int32, rows.shape, 1) < 64
    zero = jnp.zeros_like(rows)
    return jnp.concatenate([jnp.where(first, rows, zero), jnp.where(first, zero, rows)], axis=0)


def own_head(rows):
    first = lax.broadcasted_iota(jnp.int32, (WIN, 128), 1) < 64
    return jnp.where(first, rows[:WIN], rows[WIN:])


def slot_one_hot(shift_ref, rows_ref, behind):
    place = rows_ref[:, D : D + 128].astype(F32).astype(jnp.int32)
    frame = place >> 6
    row = (place >> 4) & 3
    column = place & 15
    group = column >> 3
    slot = lax.broadcasted_iota(jnp.int32, (SLOTS, 128), 0) & 7
    lane = lax.broadcasted_iota(jnp.int32, (SLOTS, 128), 1)
    time_offset = jnp.where(group == 0, shift_ref[0, 0], shift_ref[0, 1])
    row_offset = jnp.where(group == 0, shift_ref[1, 0], shift_ref[1, 1])
    frame = frame + time_offset - 4 * behind
    row = row + row_offset - jnp.where(slot >= 4, 4, 0)
    inside = (place >= 0) & (frame >= 0) & (frame < 4) & (row >= 0) & (row < 4)
    token = (((frame >> 1) * 2 + group) * 64) + ((frame & 1) * 32) + row * 8 + (column & 7)
    token = jnp.where(inside, token, -1)
    halves = [jnp.where(token == lane + 128 * half, 1.0, 0.0) for half in range(2)]
    return jnp.concatenate(halves, axis=1).astype(BF)


def forward_kernel(
    shift_ref, own_ref, behind_ref, mask_ref, frames_ref, rows_ref, columns_ref, w_qkv_hbm, w_out_hbm,
    embedded_ref, residual_ref, qkv_ref, probs_ref, seen_ref, one_hot_ref,
    w_qkv_ref, w_out_ref, chosen_ref, normed_ref, heads_ref, sems,
):
    copies = [
        pltpu.make_async_copy(
            w_qkv_hbm.at[:, pl.ds(at * D, D)], w_qkv_ref.at[:, pl.ds(at * D, D)], sems.at[at]
        )
        for at in range(3)
    ]
    copies.append(pltpu.make_async_copy(w_out_hbm, w_out_ref, sems.at[3]))
    for copy in copies:
        copy.start()
    one_hot_ref[:SLOTS] = slot_one_hot(shift_ref, own_ref, 0)
    one_hot_ref[SLOTS:] = slot_one_hot(shift_ref, behind_ref, 1)
    own_hot = one_hot_ref[:SLOTS]
    behind_hot = one_hot_ref[SLOTS:]
    chosen_ref[...] = dot(own_hot, own_ref[:, :D], TN_DIMS) + dot(behind_hot, behind_ref[:, :D], TN_DIMS)
    ones = jnp.ones((2 * SLOTS, 128), BF)
    seen_ref[...] = dot(one_hot_ref[...], ones, TN_DIMS)

    for block in range(TOK // 16):
        window, half = divmod(block, 4)
        frame_pair, group = divmod(window, 2)
        at_frame = group * 4 + frame_pair * 2 + half // 2
        rows = pl.ds(block * 16, 16)
        start = jnp.where(
            jnp.concatenate([seen_ref[rows]] * 8, axis=1) > 0,
            chosen_ref[rows],
            mask_ref[...].astype(F32),
        )
        position = []
        for at in range(2):
            at_row = group * 4 + (half % 2) * 2 + at
            position.append(
                jnp.concatenate(
                    [
                        jnp.broadcast_to(frames_ref[at_frame : at_frame + 1], (8, 256)),
                        jnp.broadcast_to(rows_ref[at_row : at_row + 1], (8, 384)),
                        columns_ref[group * 8 : group * 8 + 8],
                    ],
                    axis=1,
                )
            )
        embedded = (start + jnp.concatenate(position, axis=0)).astype(BF)
        embedded_ref[rows] = embedded
        normed_ref[rows] = normalise(embedded.astype(F32))[0].astype(BF)

    for at in range(3):
        copies[at].wait()
        for part in range(2):
            cols = slice(at * D + part * 512, at * D + part * 512 + 512)
            qkv_ref[:, cols] = dot(normed_ref[...], w_qkv_ref[:, cols], NN_DIMS).astype(BF)

    def one_window(window):
        rows = slice(window * WIN, window * WIN + WIN)
        scores = []
        for pair in range(PAIRS):
            q = qkv_ref[rows, pair * 128 : pair * 128 + 128]
            k = qkv_ref[rows, D + pair * 128 : D + pair * 128 + 128]
            scores.append(dot(k, two_heads(q), NT_DIMS) * 0.125)
        probs = []
        for pair in range(PAIRS):
            weights = jnp.exp(scores[pair] - jnp.max(scores[pair], axis=0, keepdims=True))
            probs.append((weights * (1.0 / jnp.sum(weights, axis=0, keepdims=True))).astype(BF))
            probs_ref[window, pair] = probs[pair]
        for pair in range(PAIRS):
            v = qkv_ref[rows, 2 * D + pair * 128 : 2 * D + pair * 128 + 128]
            heads_ref[rows, pair * 128 : pair * 128 + 128] = own_head(dot(probs[pair], v, TN_DIMS)).astype(BF)

    for window in range(TOK // WIN):
        one_window(window)
    copies[3].wait()
    for part in range(2):
        cols = slice(part * 512, part * 512 + 512)
        attn = dot(heads_ref[...], w_out_ref[:, cols], NN_DIMS).astype(BF)
        residual_ref[:, cols] = embedded_ref[:, cols].astype(F32) + attn.astype(F32)


def backward_kernel(
    shift_ref, embedded_ref, residual_ref, qkv_ref, probs_ref, seen_ref, one_hot_ref,
    own_target, row_target, time_target, corner_target, w_head_hbm, w_out_hbm, w_qkv_hbm,
    own_picked_ref, behind_picked_ref, total_ref,
    target_ref, w_head_ref, w_out_ref, w_qkv_ref, normed_ref, scale_ref, predicted_ref, error_ref,
    narrow_ref, wide_ref, stream_ref, dqkv_ref, sems,
):
    head_copy = pltpu.make_async_copy(w_head_hbm, w_head_ref, sems.at[0])
    out_copy = pltpu.make_async_copy(w_out_hbm, w_out_ref, sems.at[1])
    qkv_copy = pltpu.make_async_copy(w_qkv_hbm, w_qkv_ref, sems.at[2])
    head_copy.start()
    out_copy.start()
    qkv_copy.start()
    target_ref[1:, 3:] = own_target[...]
    target_ref[1:, :3] = row_target[...]
    target_ref[:1, 3:] = time_target[...]
    target_ref[:1, :3] = corner_target[...]

    def tokens_of(block):
        return pl.ds(pl.multiple_of(block * 16, 16), 16)

    def head_norm(block, carry):
        rows = tokens_of(block)
        normed, scale = normalise(residual_ref[rows])
        normed_ref[rows] = normed
        scale_ref[rows] = jnp.broadcast_to(scale, (16, 128))
        narrow_ref[rows] = normed.astype(BF)
        return carry

    lax.fori_loop(0, TOK // 16, head_norm, 0, unroll=16)
    head_copy.wait()
    for part in range(3):
        cols = slice(part * GROUP, part * GROUP + GROUP)
        predicted_ref[:, cols] = dot(narrow_ref[...], w_head_ref[:, cols], NN_DIMS)

    def pixel_block(block, carry):
        at_frame = block // 2
        half = block % 2
        for group in range(2):
            rows = tokens_of(((at_frame // 2) * 2 + group) * 4 + (at_frame % 2) * 2 + half)
            masked = 1.0 - jnp.concatenate([seen_ref[rows]] * 12, axis=1)
            target = jnp.concatenate(
                [
                    target_ref[
                        at_frame - shift_ref[0, group] + 1,
                        half * 2 + at - shift_ref[1, group] + 3,
                        group * 8 : group * 8 + 8,
                    ].astype(F32)
                    for at in range(2)
                ],
                axis=0,
            )
            error_ref[rows] = (masked * (predicted_ref[rows] - target)).astype(BF)
        return carry

    lax.fori_loop(0, 8, pixel_block, 0, unroll=8)

    for part in range(2):
        cols = slice(part * 512, part * 512 + 512)
        wide_ref[:, cols] = dot(error_ref[...], w_head_ref[cols, :], NT_DIMS)

    def head_norm_back(block, carry):
        rows = tokens_of(block)
        scale = jnp.concatenate([scale_ref[rows]] * 8, axis=1)
        cotangent = wide_ref[rows].astype(BF).astype(F32)
        grad = normalise_back(cotangent, normed_ref[rows], scale)
        stream_ref[rows] = grad
        narrow_ref[rows] = grad.astype(BF)
        return carry

    lax.fori_loop(0, TOK // 16, head_norm_back, 0, unroll=16)
    out_copy.wait()
    d_heads = dot(narrow_ref[...], w_out_ref[...], NT_DIMS).astype(BF)
    narrow_ref[...] = d_heads

    def one_window(window):
        rows = slice(window * WIN, window * WIN + WIN)
        cols = [[slice(at * D + pair * 128, at * D + pair * 128 + 128) for at in range(3)] for pair in range(PAIRS)]
        d_probs = []
        out_heads = []
        for pair in range(PAIRS):
            out_heads.append(two_heads(narrow_ref[rows, cols[pair][0]]))
            d_probs.append(dot(qkv_ref[rows, cols[pair][2]], out_heads[pair], NT_DIMS))
        for pair in range(PAIRS):
            dqkv_ref[rows, cols[pair][2]] = dot(probs_ref[window, pair], out_heads[pair], NN_DIMS).astype(BF)
        d_scores = []
        for pair in range(PAIRS):
            probs = probs_ref[window, pair].astype(F32)
            cotangent = d_probs[pair].astype(BF).astype(F32)
            mean = jnp.sum(cotangent * probs, axis=0, keepdims=True)
            d_scores.append((probs * (cotangent - mean) * 0.125).astype(BF))
        for pair in range(PAIRS):
            q_heads = two_heads(qkv_ref[rows, cols[pair][0]])
            dqkv_ref[rows, cols[pair][1]] = dot(d_scores[pair], q_heads, NN_DIMS).astype(BF)
        for pair in range(PAIRS):
            d_q = own_head(dot(d_scores[pair], qkv_ref[rows, cols[pair][1]], TN_DIMS))
            dqkv_ref[rows, cols[pair][0]] = d_q.astype(BF)

    for window in range(TOK // WIN):
        one_window(window)
    qkv_copy.wait()
    for part in range(2):
        cols = slice(part * 512, part * 512 + 512)
        wide_ref[:, cols] = dot(dqkv_ref[...], w_qkv_ref[cols, :], NT_DIMS)

    def first_norm_back(block, carry):
        rows = tokens_of(block)
        normed, scale = normalise(embedded_ref[rows].astype(F32))
        cotangent = wide_ref[rows].astype(BF).astype(F32)
        grad = stream_ref[rows] + normalise_back(cotangent, normed, scale)
        narrow_ref[rows] = grad.astype(BF)
        masked = 1.0 - jnp.concatenate([seen_ref[rows]] * 8, axis=1)
        part = masked * grad
        return carry + part[:8] + part[8:]

    total = lax.fori_loop(0, TOK // 16, first_norm_back, jnp.zeros((8, D), F32), unroll=16)
    total = jnp.sum(total, axis=0, keepdims=True)
    total_ref[...] = jnp.concatenate([total[:, at * 128 : at * 128 + 128] for at in range(8)], axis=0)
    own_picked_ref[...] = dot(one_hot_ref[:SLOTS], narrow_ref[...], NN_DIMS).astype(BF)
    behind_picked_ref[...] = dot(one_hot_ref[SLOTS:], narrow_ref[...], NN_DIMS).astype(BF)


def pack_kernel(place_ref, rows_ref, packed_ref):
    rows = rows_ref[...].astype(F32)
    before = jnp.concatenate([rows[-1:], rows[:-1]], axis=0)
    packed_ref[:, :, :D] = jnp.concatenate([rows, before], axis=1).astype(BF)
    slot = lax.broadcasted_iota(jnp.int32, (8, 128), 0)
    peers = rows_ref.shape[0]
    for peer in range(peers):
        places = jnp.zeros((8, 128), jnp.int32)
        for at in range(8):
            source = peer if at < 4 else (peer - 1) % peers
            places = jnp.where(slot == at, place_ref[source, at % 4], places)
        packed_ref[peer, :, D:] = places.astype(F32).astype(BF)


def target_kernel(pixel_ref, own_ref, row_ref, time_ref, corner_ref):
    for frame in range(4):
        for row in range(4):
            for part in range(3):
                cols = slice(part * GROUP, part * GROUP + GROUP)
                raw = pixel_ref[frame, row, :, cols].astype(F32)
                center = raw - lane_mean(raw)
                spread = jnp.sqrt(jnp.sum(center * center, axis=-1, keepdims=True) * (1.0 / (GROUP - 1)))
                target = (center * (1.0 / (spread + 1e-06))).astype(BF)
                own_ref[frame, row, :, cols] = target
                if row > 0:
                    row_ref[frame, row - 1, :, cols] = target
                if frame == 3:
                    time_ref[0, row, :, cols] = target
                if frame == 3 and row > 0:
                    corner_ref[0, row - 1, :, cols] = target


def unpack_kernel(scale, back_ref, rows_ref, total_ref):
    rows = back_ref[:, :4, :D].astype(F32)
    after = back_ref[:, 4:, :D].astype(F32)
    after = jnp.concatenate([after[1:], after[:1]], axis=0)
    rows_ref[...] = (rows + after).astype(BF)
    sums = jnp.sum(back_ref[:, :, D:].astype(F32), axis=0)
    total_ref[...] = (sums[:, :128] + sums[:, 128:]) * scale


def forward_part(*operands):
    vmem = pl.BlockSpec(memory_space=VMEM)
    smem = pl.BlockSpec(memory_space=SMEM)
    hbm = pl.BlockSpec(memory_space=pltpu.MemorySpace.HBM)
    return pl.pallas_call(
        forward_kernel,
        name="forward_part",
        in_specs=[smem] + [vmem] * 6 + [hbm] * 2,
        out_specs=[vmem] * 6,
        out_shape=[
            jax.ShapeDtypeStruct((TOK, D), BF),
            jax.ShapeDtypeStruct((TOK, D), F32),
            jax.ShapeDtypeStruct((TOK, 3 * D), BF),
            jax.ShapeDtypeStruct((TOK // WIN, PAIRS, WIN, 128), BF),
            jax.ShapeDtypeStruct((TOK, 128), F32),
            jax.ShapeDtypeStruct((2 * SLOTS, TOK), BF),
        ],
        scratch_shapes=[
            pltpu.VMEM((D, 3 * D), BF),
            pltpu.VMEM((D, D), BF),
            pltpu.VMEM((TOK, D), F32),
            pltpu.VMEM((TOK, D), BF),
            pltpu.VMEM((TOK, D), BF),
            pltpu.SemaphoreType.DMA((4,)),
        ],
        compiler_params=pltpu.CompilerParams(vmem_limit_bytes=28 << 20),
    )(*operands)


def backward_part(*operands):
    vmem = pl.BlockSpec(memory_space=VMEM)
    smem = pl.BlockSpec(memory_space=SMEM)
    hbm = pl.BlockSpec(memory_space=pltpu.MemorySpace.HBM)
    return pl.pallas_call(
        backward_kernel,
        name="backward_part",
        in_specs=[smem] + [vmem] * 10 + [hbm] * 3,
        out_specs=[vmem] * 3,
        out_shape=[
            jax.ShapeDtypeStruct((SLOTS, D), BF),
            jax.ShapeDtypeStruct((SLOTS, D), BF),
            jax.ShapeDtypeStruct((8, 128), F32),
        ],
        scratch_shapes=[
            pltpu.VMEM((5, 7, 16, PIX), BF),
            pltpu.VMEM((D, PIX), BF),
            pltpu.VMEM((D, D), BF),
            pltpu.VMEM((D, 3 * D), BF),
            pltpu.VMEM((TOK, D), F32),
            pltpu.VMEM((TOK, 128), F32),
            pltpu.VMEM((TOK, PIX), F32),
            pltpu.VMEM((TOK, PIX), BF),
            pltpu.VMEM((TOK, D), BF),
            pltpu.VMEM((TOK, D), F32),
            pltpu.VMEM((TOK, D), F32),
            pltpu.VMEM((TOK, 3 * D), BF),
            pltpu.SemaphoreType.DMA((3,)),
        ],
        compiler_params=pltpu.CompilerParams(vmem_limit_bytes=36 << 20),
    )(*operands)


def sinusoid(coordinate, channel_count):
    half_count = channel_count // 2
    frequency = jnp.exp(-math.log(10000.0) * jnp.arange(half_count, dtype=F32) / half_count)
    angles = coordinate.astype(F32)[..., None] * frequency
    return jnp.concatenate([jnp.sin(angles), jnp.cos(angles)], axis=-1)


def move(value, axis, steps):
    count = lax.axis_size(axis)
    return lax.ppermute(value, axis, [(at, (at + steps) % count) for at in range(count)])


def move_corner(value):
    count_tm = lax.axis_size(TM)
    count_row = lax.axis_size(ROW)
    pairs = [
        (i * count_row + d, (i + 1) % count_tm * count_row + (d + 1) % count_row)
        for i in range(count_tm)
        for d in range(count_row)
    ]
    return lax.ppermute(value, ALL, pairs)


def per_device(visible, slot_pos, window_shift, mask_token, w_qkv, w_out, w_head, pixels):
    frame_count, row_count = pixels.shape[:2]
    peers, slots = slot_pos.shape[2:]
    vmem = pl.BlockSpec(memory_space=VMEM)
    smem = pl.BlockSpec(memory_space=SMEM)
    packed = pl.pallas_call(
        pack_kernel,
        name="pack_part",
        in_specs=[smem, vmem],
        out_specs=vmem,
        out_shape=jax.ShapeDtypeStruct((peers, 2 * slots, D + 128), BF),
        compiler_params=pltpu.CompilerParams(vmem_limit_bytes=8 << 20),
    )(slot_pos.reshape(peers, slots), visible.reshape(peers, slots, D))
    own = lax.all_to_all(packed, ROW, split_axis=0, concat_axis=0, tiled=True).reshape(SLOTS, D + 128)
    behind = move(own, TM, 1)
    own_target, row_target, time_target, corner_target = pl.pallas_call(
        target_kernel,
        name="target_part",
        in_specs=[vmem],
        out_specs=[vmem] * 4,
        out_shape=[
            jax.ShapeDtypeStruct((frames, rows, 16, PIX), BF)
            for frames, rows in ((4, 4), (4, 3), (1, 4), (1, 3))
        ],
        compiler_params=pltpu.CompilerParams(vmem_limit_bytes=8 << 20),
    )(pixels)
    row_target = move(row_target, ROW, 1)
    corner_target = move_corner(corner_target)
    time_target = move(time_target, TM, 1)

    local = jnp.arange(4, dtype=jnp.int32)
    frame_total = frame_count * lax.axis_size(TM)
    row_total = row_count * lax.axis_size(ROW)
    frames = (lax.axis_index(TM) * frame_count + local[None] - window_shift[0][:, None]) % frame_total
    band = (lax.axis_index(ROW) * row_count + local[None] - window_shift[1][:, None]) % row_total
    frame_table = sinusoid(frames.reshape(-1), 256)
    row_table = sinusoid(band.reshape(-1), 384)
    column_table = sinusoid(jnp.arange(16, dtype=jnp.int32), 384)

    w_qkv, w_out, w_head = (
        pltpu.with_memory_space_constraint(value, pltpu.MemorySpace.HBM) for value in (w_qkv, w_out, w_head)
    )
    kept = forward_part(
        window_shift, own, behind, mask_token.reshape(1, D), frame_table, row_table, column_table,
        w_qkv, w_out,
    )
    own_picked, behind_picked, local_total = backward_part(
        window_shift, *kept, own_target, row_target, time_target, corner_target, w_head, w_out, w_qkv
    )
    from_next = move(behind_picked, TM, -1)
    mine = own_picked + from_next
    other = move(local_total, "tm_1", 1)
    local_total = local_total + other
    turned = [move(local_total, "tm_0", step) for step in (1, 2, 3)]
    local_total = (local_total + turned[1]) + (turned[0] + turned[2])
    high = local_total.astype(BF)
    low = (local_total - high.astype(F32)).astype(BF)
    sums = jnp.broadcast_to(jnp.concatenate([high, low], axis=1)[None], (peers, 8, 256))
    sent = jnp.concatenate([mine.reshape(peers, 2 * slots, D), sums], axis=-1)
    back = lax.all_to_all(sent, ROW, split_axis=0, concat_axis=0, tiled=True)
    grad_scale = (frame_total * row_total * pixels.shape[2]) ** (-0.5)
    d_visible, d_mask = pl.pallas_call(
        functools.partial(unpack_kernel, grad_scale),
        name="unpack_part",
        in_specs=[vmem],
        out_specs=[vmem] * 2,
        out_shape=[jax.ShapeDtypeStruct((peers, slots, D), BF), jax.ShapeDtypeStruct((8, 128), F32)],
        compiler_params=pltpu.CompilerParams(vmem_limit_bytes=8 << 20),
    )(back)
    return (d_visible.reshape(visible.shape), d_mask.reshape(D))


def solution(mesh):
    torus = Mesh(mesh.devices.reshape(4, 2, 4, 4), ALL)
    return jax.shard_map(
        per_device,
        mesh=torus,
        in_specs=(
            P(TM, ROW, None, None, None),
            P(TM, ROW, None, None),
            P(),
            P(),
            P(),
            P(),
            P(),
            P(TM, ROW, None, None),
        ),
        out_specs=(P(TM, ROW, None, None, None), P()),
        check_vma=False,
    )
```

```python
import functools
import math

import jax
import jax.numpy as jnp
from jax import lax
from jax.experimental import pallas as pl
from jax.experimental.pallas import tpu as pltpu
from jax.sharding import Mesh
from jax.sharding import PartitionSpec as P

WT = 2
WH = 4
WW = 8
D = 1024
PIX = 1536
GROUP = PIX // 3
TOK = 256
HALF = TOK // 2
WIN = WT * WH * WW
PAIRS = D // 128
SLOTS = 128
TM = ("tm_0", "tm_1")
ROW = ("row_0", "row_1")
ALL = TM + ROW
BF = jnp.bfloat16
F32 = jnp.float32
NT_DIMS = (((1,), (1,)), ((), ()))
TN_DIMS = (((0,), (0,)), ((), ()))
NN_DIMS = (((1,), (0,)), ((), ()))
VMEM = pltpu.MemorySpace.VMEM
SMEM = pltpu.MemorySpace.SMEM
HBM = pltpu.MemorySpace.HBM


def dot(a, b, dims):
    return lax.dot_general(a, b, dims, preferred_element_type=F32)


def lane_mean(values):
    return jnp.sum(values, axis=-1, keepdims=True) * (1.0 / values.shape[-1])


def normalise(values):
    center = values - lane_mean(values)
    scale = lax.rsqrt(lane_mean(center * center) + 1e-05)
    return center * scale, scale


def normalise_back(cotangent, normed, scale):
    return scale * (cotangent - lane_mean(cotangent) - normed * lane_mean(cotangent * normed))


def two_heads(rows):
    first = lax.broadcasted_iota(jnp.int32, rows.shape, 1) < 64
    zero = jnp.zeros_like(rows)
    return jnp.concatenate([jnp.where(first, rows, zero), jnp.where(first, zero, rows)], axis=0)


def own_head(rows):
    first = lax.broadcasted_iota(jnp.int32, (WIN, 128), 1) < 64
    return jnp.where(first, rows[:WIN], rows[WIN:])


def slot_one_hot(shift_ref, rows_ref, behind, frame_pair):
    place = rows_ref[:, D : D + 128].astype(F32).astype(jnp.int32)
    frame = place >> 6
    row = (place >> 4) & 3
    column = place & 15
    group = column >> 3
    slot = lax.broadcasted_iota(jnp.int32, (SLOTS, 128), 0) & 7
    lane = lax.broadcasted_iota(jnp.int32, (SLOTS, 128), 1)
    frame = frame + jnp.where(group == 0, shift_ref[0:1], shift_ref[1:2]) - 4 * behind
    row = row + jnp.where(group == 0, shift_ref[2:3], shift_ref[3:4]) - jnp.where(slot >= 4, 4, 0)
    inside = (place >= 0) & ((frame >> 1) == frame_pair) & (row >= 0) & (row < 4)
    token = group * 64 + ((frame & 1) * 32) + row * 8 + (column & 7)
    token = jnp.where(inside, token, -1)
    return jnp.where(token == lane, 1.0, 0.0).astype(BF)


def embed(frame_pair, mask_ref, frames_ref, rows_ref, columns_ref, chosen_ref, seen_ref, embedded_ref, normed_ref):
    mask = mask_ref[...].astype(F32)
    mask = jnp.concatenate([mask[at : at + 1] for at in range(8)], axis=1)
    for block in range(HALF // 16):
        group, half = divmod(block, 4)
        at_frame = group * 4 + frame_pair * 2 + half // 2
        rows = slice(block * 16, block * 16 + 16)
        start = jnp.where(jnp.concatenate([seen_ref[rows]] * 8, axis=1) > 0, chosen_ref[rows], mask)
        position = []
        for at in range(2):
            at_row = group * 4 + (half % 2) * 2 + at
            position.append(
                jnp.concatenate(
                    [
                        jnp.broadcast_to(frames_ref[at_frame : at_frame + 1], (8, 256)),
                        jnp.broadcast_to(rows_ref[at_row : at_row + 1], (8, 384)),
                        columns_ref[group * 8 : group * 8 + 8],
                    ],
                    axis=1,
                )
            )
        embedded = (start + jnp.concatenate(position, axis=0)).astype(BF)
        embedded_ref[rows] = embedded
        normed_ref[rows] = normalise(embedded.astype(F32))[0].astype(BF)


def project(at, normed_ref, w_qkv_ref, qkv_ref):
    for part in range(2):
        cols = slice(at * D + part * 512, at * D + part * 512 + 512)
        qkv_ref[:, cols] = dot(normed_ref[...], w_qkv_ref[:, cols], NN_DIMS).astype(BF)


def attend(qkv_ref, probs_ref, heads_ref):
    for window in range(HALF // WIN):
        rows = slice(window * WIN, window * WIN + WIN)
        scores = []
        for pair in range(PAIRS):
            q = qkv_ref[rows, pair * 128 : pair * 128 + 128]
            k = qkv_ref[rows, D + pair * 128 : D + pair * 128 + 128]
            scores.append(dot(k, two_heads(q), NT_DIMS) * 0.125)
        probs = []
        for pair in range(PAIRS):
            weights = jnp.exp(scores[pair] - jnp.max(scores[pair], axis=0, keepdims=True))
            probs.append((weights * (1.0 / jnp.sum(weights, axis=0, keepdims=True))).astype(BF))
            probs_ref[window, pair] = probs[pair]
        for pair in range(PAIRS):
            v = qkv_ref[rows, 2 * D + pair * 128 : 2 * D + pair * 128 + 128]
            heads_ref[rows, pair * 128 : pair * 128 + 128] = own_head(dot(probs[pair], v, TN_DIMS)).astype(BF)


def early_kernel(
    shift_ref, own_ref, mask_ref, frames_ref, rows_ref, columns_ref, w_qkv_hbm, w_out_hbm, w_head_hbm,
    embedded_ref, qkv_ref, probs_ref, seen_ref, one_hot_ref, heads_ref, w_qkv_ref, w_out_ref, w_head_ref,
    chosen_ref, normed_ref, sems,
):
    copies = [
        pltpu.make_async_copy(
            w_qkv_hbm.at[:, pl.ds(at * D, D)], w_qkv_ref.at[:, pl.ds(at * D, D)], sems.at[at]
        )
        for at in range(3)
    ]
    copies.append(pltpu.make_async_copy(w_out_hbm, w_out_ref, sems.at[3]))
    copies.append(pltpu.make_async_copy(w_head_hbm, w_head_ref, sems.at[4]))
    for copy in copies:
        copy.start()
    one_hot_ref[...] = slot_one_hot(shift_ref, own_ref, 0, 1)
    chosen_ref[...] = dot(one_hot_ref[...], own_ref[:, :D], TN_DIMS)
    seen_ref[...] = dot(one_hot_ref[...], jnp.ones((SLOTS, 128), BF), TN_DIMS)
    embed(1, mask_ref, frames_ref, rows_ref, columns_ref, chosen_ref, seen_ref, embedded_ref, normed_ref)
    for at in range(3):
        copies[at].wait()
        project(at, normed_ref, w_qkv_ref, qkv_ref)
    attend(qkv_ref, probs_ref, heads_ref)
    copies[3].wait()
    copies[4].wait()


def late_kernel(
    shift_ref, own_ref, behind_ref, mask_ref, frames_ref, rows_ref, columns_ref, embedded_1_ref, heads_1_ref,
    w_qkv_ref, w_out_ref, w_head_ref,
    embedded_ref, qkv_ref, probs_ref, seen_ref, one_hot_ref, head_normed_ref, scale_ref, predicted_ref,
    chosen_ref, normed_ref, heads_ref, residual_ref, narrow_ref,
):
    one_hot_ref[:SLOTS] = slot_one_hot(shift_ref, own_ref, 0, 0)
    one_hot_ref[SLOTS:] = slot_one_hot(shift_ref, behind_ref, 1, 0)
    own_hot = one_hot_ref[:SLOTS]
    behind_hot = one_hot_ref[SLOTS:]
    chosen_ref[...] = dot(own_hot, own_ref[:, :D], TN_DIMS) + dot(behind_hot, behind_ref[:, :D], TN_DIMS)
    seen_ref[...] = dot(one_hot_ref[...], jnp.ones((2 * SLOTS, 128), BF), TN_DIMS)
    embed(0, mask_ref, frames_ref, rows_ref, columns_ref, chosen_ref, seen_ref, embedded_ref, normed_ref)
    for at in range(3):
        project(at, normed_ref, w_qkv_ref, qkv_ref)
    heads_ref[HALF:] = heads_1_ref[...]
    attend(qkv_ref, probs_ref, heads_ref)
    for part in range(2):
        cols = slice(part * 512, part * 512 + 512)
        attn = dot(heads_ref[...], w_out_ref[:, cols], NN_DIMS).astype(BF).astype(F32)
        residual_ref[:HALF, cols] = embedded_ref[:, cols].astype(F32) + attn[:HALF]
        residual_ref[HALF:, cols] = embedded_1_ref[:, cols].astype(F32) + attn[HALF:]
    for block in range(TOK // 16):
        rows = slice(block * 16, block * 16 + 16)
        normed, scale = normalise(residual_ref[rows])
        head_normed_ref[rows] = normed
        scale_ref[rows] = jnp.broadcast_to(scale, (16, 128))
        narrow_ref[rows] = normed.astype(BF)
    for part in range(3):
        cols = slice(part * GROUP, part * GROUP + GROUP)
        predicted_ref[:, cols] = dot(narrow_ref[...], w_head_ref[:, cols], NN_DIMS)


def backward_kernel(
    shift_ref, embedded_0_ref, qkv_0_ref, probs_0_ref, seen_0_ref, one_hot_0_ref,
    embedded_1_ref, qkv_1_ref, probs_1_ref, seen_1_ref, one_hot_1_ref,
    normed_ref, scale_ref, predicted_ref, w_qkv_ref, w_out_ref, w_head_ref,
    own_target, row_target, last_row_target, time_target, corner_target,
    own_picked_ref, behind_picked_ref, total_ref,
    target_ref, error_ref, narrow_ref, wide_ref, stream_ref, dqkv_ref,
):
    embedded_refs = (embedded_0_ref, embedded_1_ref)
    qkv_refs = (qkv_0_ref, qkv_1_ref)
    probs_refs = (probs_0_ref, probs_1_ref)
    seen_refs = (seen_0_ref, seen_1_ref)
    target_ref[1:, 3:] = own_target[...]
    target_ref[1:4, :3] = row_target[...]
    target_ref[4:, :3] = last_row_target[...]
    target_ref[:1, 3:] = time_target[...]
    target_ref[:1, :3] = corner_target[...]

    for block in range(TOK // 16):
        frame_pair, rest = divmod(block, 8)
        group, half = divmod(rest, 4)
        rows = slice(block * 16, block * 16 + 16)
        local = slice(rest * 16, rest * 16 + 16)
        masked = 1.0 - jnp.concatenate([seen_refs[frame_pair][local]] * 12, axis=1)
        target = jnp.concatenate(
            [
                target_ref[
                    frame_pair * 2 + half // 2 - shift_ref[0, group] + 1,
                    (half % 2) * 2 + at - shift_ref[1, group] + 3,
                    group * 8 : group * 8 + 8,
                ].astype(F32)
                for at in range(2)
            ],
            axis=0,
        )
        error_ref[rows] = (masked * (predicted_ref[rows] - target)).astype(BF)

    for part in range(2):
        cols = slice(part * 512, part * 512 + 512)
        wide_ref[:, cols] = dot(error_ref[...], w_head_ref[cols, :], NT_DIMS)

    for block in range(TOK // 16):
        rows = slice(block * 16, block * 16 + 16)
        scale = jnp.concatenate([scale_ref[rows]] * 8, axis=1)
        cotangent = wide_ref[rows].astype(BF).astype(F32)
        grad = normalise_back(cotangent, normed_ref[rows], scale)
        stream_ref[rows] = grad
        narrow_ref[rows] = grad.astype(BF)

    narrow_ref[...] = dot(narrow_ref[...], w_out_ref[...], NT_DIMS).astype(BF)

    for window in range(TOK // WIN):
        rows = slice(window * WIN, window * WIN + WIN)
        frame_pair, group = divmod(window, 2)
        local = slice(group * WIN, group * WIN + WIN)
        qkv_ref = qkv_refs[frame_pair]
        probs_ref = probs_refs[frame_pair]
        cols = [[slice(at * D + pair * 128, at * D + pair * 128 + 128) for at in range(3)] for pair in range(PAIRS)]
        d_probs = []
        out_heads = []
        for pair in range(PAIRS):
            out_heads.append(two_heads(narrow_ref[rows, cols[pair][0]]))
            d_probs.append(dot(qkv_ref[local, cols[pair][2]], out_heads[pair], NT_DIMS))
        for pair in range(PAIRS):
            dqkv_ref[rows, cols[pair][2]] = dot(probs_ref[group, pair], out_heads[pair], NN_DIMS).astype(BF)
        d_scores = []
        for pair in range(PAIRS):
            probs = probs_ref[group, pair].astype(F32)
            cotangent = d_probs[pair].astype(BF).astype(F32)
            mean = jnp.sum(cotangent * probs, axis=0, keepdims=True)
            d_scores.append((probs * (cotangent - mean) * 0.125).astype(BF))
        for pair in range(PAIRS):
            q_heads = two_heads(qkv_ref[local, cols[pair][0]])
            dqkv_ref[rows, cols[pair][1]] = dot(d_scores[pair], q_heads, NN_DIMS).astype(BF)
        for pair in range(PAIRS):
            d_q = own_head(dot(d_scores[pair], qkv_ref[local, cols[pair][1]], TN_DIMS))
            dqkv_ref[rows, cols[pair][0]] = d_q.astype(BF)

    for part in range(2):
        cols = slice(part * 512, part * 512 + 512)
        wide_ref[:, cols] = dot(dqkv_ref[...], w_qkv_ref[cols, :], NT_DIMS)

    total = jnp.zeros((8, D), F32)
    for block in range(TOK // 16):
        frame_pair, rest = divmod(block, 8)
        rows = slice(block * 16, block * 16 + 16)
        local = slice(rest * 16, rest * 16 + 16)
        normed, scale = normalise(embedded_refs[frame_pair][local].astype(F32))
        cotangent = wide_ref[rows].astype(BF).astype(F32)
        grad = stream_ref[rows] + normalise_back(cotangent, normed, scale)
        narrow_ref[rows] = grad.astype(BF)
        part = (1.0 - jnp.concatenate([seen_refs[frame_pair][local]] * 8, axis=1)) * grad
        total = total + part[:8] + part[8:]
    total = jnp.sum(total, axis=0, keepdims=True)
    total_ref[...] = jnp.concatenate([total[:, at * 128 : at * 128 + 128] for at in range(8)], axis=0)
    behind_picked_ref[...] = dot(one_hot_0_ref[SLOTS:], narrow_ref[:HALF], NN_DIMS).astype(BF)
    own_picked = dot(one_hot_0_ref[:SLOTS], narrow_ref[:HALF], NN_DIMS)
    own_picked_ref[...] = (own_picked + dot(one_hot_1_ref[...], narrow_ref[HALF:], NN_DIMS)).astype(BF)


def pack_kernel(
    place_hbm, shift_hbm, rows_hbm, packed_ref, shift_rows_ref, place_ref, shift_ref, rows_ref, sems
):
    copies = [
        pltpu.make_async_copy(rows_hbm, rows_ref, sems.at[0]),
        pltpu.make_async_copy(place_hbm, place_ref, sems.at[1]),
        pltpu.make_async_copy(shift_hbm, shift_ref, sems.at[2]),
    ]
    for copy in copies:
        copy.start()
    copies[1].wait()
    slot = lax.broadcasted_iota(jnp.int32, (8, 128), 0)
    peers = rows_ref.shape[0]
    for peer in range(peers):
        places = jnp.zeros((8, 128), jnp.int32)
        for at in range(8):
            source = peer if at < 4 else (peer - 1) % peers
            places = jnp.where(slot == at, place_ref[source, at % 4], places)
        packed_ref[peer, :, D:] = places.astype(F32).astype(BF)
    copies[2].wait()
    shifts = jnp.zeros((8, 128), jnp.int32)
    for at in range(4):
        shifts = jnp.where(slot == at, shift_ref[at // 2, at % 2], shifts)
    shift_rows_ref[...] = shifts
    copies[0].wait()
    rows = rows_ref[...].astype(F32)
    before = jnp.concatenate([rows[-1:], rows[:-1]], axis=0)
    packed_ref[:, :, :D] = jnp.concatenate([rows, before], axis=1).astype(BF)


def target_kernel(pixel_hbm, own_ref, row_ref, last_row_ref, time_ref, pixel_ref, sems):
    copies = [pltpu.make_async_copy(pixel_hbm.at[at], pixel_ref.at[at], sems.at[at]) for at in range(4)]
    for frame in (3, 0, 1, 2):
        copies[frame].start()
    for frame in (3, 0, 1, 2):
        copies[frame].wait()
        for row in range(4):
            for part in range(3):
                cols = slice(part * GROUP, part * GROUP + GROUP)
                raw = pixel_ref[frame, row, :, cols].astype(F32)
                center = raw - lane_mean(raw)
                spread = jnp.sqrt(jnp.sum(center * center, axis=-1, keepdims=True) * (1.0 / (GROUP - 1)))
                target = (center * (1.0 / (spread + 1e-06))).astype(BF)
                own_ref[frame, row, :, cols] = target
                if row > 0 and frame < 3:
                    row_ref[frame, row - 1, :, cols] = target
                if row > 0 and frame == 3:
                    last_row_ref[0, row - 1, :, cols] = target
                if frame == 3:
                    time_ref[0, row, :, cols] = target


def unpack_kernel(scale, back_ref, rows_ref, total_ref):
    rows = back_ref[:, :4, :D].astype(F32)
    after = back_ref[:, 4:, :D].astype(F32)
    after = jnp.concatenate([after[1:], after[:1]], axis=0)
    rows_ref[...] = (rows + after).astype(BF)
    sums = jnp.sum(back_ref[:, :, D:].astype(F32), axis=0)
    total_ref[...] = (sums[:, :128] + sums[:, 128:]) * scale


def shapes(*items):
    return [jax.ShapeDtypeStruct(dims, kind) for dims, kind in items]


def call(kernel, outputs, scratch, in_specs, limit):
    return pl.pallas_call(
        kernel,
        in_specs=in_specs,
        out_specs=[pl.BlockSpec(memory_space=VMEM)] * len(outputs),
        out_shape=shapes(*outputs),
        scratch_shapes=scratch,
        compiler_params=pltpu.CompilerParams(vmem_limit_bytes=limit << 20),
    )


def in_space(space, count):
    return [pl.BlockSpec(memory_space=space)] * count


def half_outputs(slots):
    return [
        ((HALF, D), BF),
        ((HALF, 3 * D), BF),
        ((HALF // WIN, PAIRS, WIN, 128), BF),
        ((HALF, 128), F32),
        ((slots, HALF), BF),
    ]


def pack_part(*operands):
    outputs = [((16, 8, D + 128), BF), ((8, 128), jnp.int32)]
    scratch = [
        pltpu.SMEM((16, 4), jnp.int32),
        pltpu.SMEM((2, 2), jnp.int32),
        pltpu.VMEM((16, 4, D), BF),
        pltpu.SemaphoreType.DMA((3,)),
    ]
    return call(pack_kernel, outputs, scratch, in_space(HBM, 3), 8)(*operands)


def target_part(*operands):
    outputs = [((frames, rows, 16, PIX), BF) for frames, rows in ((4, 4), (3, 3), (1, 3), (1, 4))]
    scratch = [pltpu.VMEM((4, 4, 16, PIX), BF), pltpu.SemaphoreType.DMA((4,))]
    return call(target_kernel, outputs, scratch, in_space(HBM, 1), 8)(*operands)


def early_part(*operands):
    outputs = half_outputs(SLOTS) + [((HALF, D), BF), ((D, 3 * D), BF), ((D, D), BF), ((D, PIX), BF)]
    scratch = [pltpu.VMEM((HALF, D), F32), pltpu.VMEM((HALF, D), BF), pltpu.SemaphoreType.DMA((5,))]
    return call(early_kernel, outputs, scratch, in_space(VMEM, 6) + in_space(HBM, 3), 20)(*operands)


def late_part(*operands):
    outputs = half_outputs(2 * SLOTS) + [((TOK, D), F32), ((TOK, 128), F32), ((TOK, PIX), F32)]
    scratch = [
        pltpu.VMEM((HALF, D), F32),
        pltpu.VMEM((HALF, D), BF),
        pltpu.VMEM((TOK, D), BF),
        pltpu.VMEM((TOK, D), F32),
        pltpu.VMEM((TOK, D), BF),
    ]
    return call(late_kernel, outputs, scratch, in_space(VMEM, 12), 26)(*operands)


def backward_part(*operands):
    outputs = [((SLOTS, D), BF), ((SLOTS, D), BF), ((8, 128), F32)]
    scratch = [
        pltpu.VMEM((5, 7, 16, PIX), BF),
        pltpu.VMEM((TOK, PIX), BF),
        pltpu.VMEM((TOK, D), BF),
        pltpu.VMEM((TOK, D), F32),
        pltpu.VMEM((TOK, D), F32),
        pltpu.VMEM((TOK, 3 * D), BF),
    ]
    return call(backward_kernel, outputs, scratch, in_space(SMEM, 1) + in_space(VMEM, 21), 34)(*operands)


def sinusoid(coordinate, channel_count):
    half_count = channel_count // 2
    frequency = jnp.exp(-math.log(10000.0) * jnp.arange(half_count, dtype=F32) / half_count)
    angles = coordinate.astype(F32)[..., None] * frequency
    return jnp.concatenate([jnp.sin(angles), jnp.cos(angles)], axis=-1)


def move(value, axis, steps):
    count = lax.axis_size(axis)
    return lax.ppermute(value, axis, [(at, (at + steps) % count) for at in range(count)])


def per_device(visible, slot_pos, window_shift, mask_token, w_qkv, w_out, w_head, pixels):
    frame_count, row_count = pixels.shape[:2]
    peers, slots = slot_pos.shape[2:]
    hold = functools.partial(pltpu.with_memory_space_constraint, memory_space=HBM)
    packed, shift_rows = pack_part(
        hold(slot_pos.reshape(peers, slots)), hold(window_shift), hold(visible.reshape(peers, slots, D))
    )
    own = lax.all_to_all(packed, ROW, split_axis=0, concat_axis=0, tiled=True).reshape(SLOTS, D + 128)
    behind = move(own, TM, 1)
    own_target, row_target, last_row_target, time_target = target_part(hold(pixels))
    last_row_target = move(last_row_target, ROW, 1)
    row_target = move(row_target, ROW, 1)
    time_target = move(time_target, TM, 1)
    corner_target = move(last_row_target, TM, 1)

    local = jnp.arange(4, dtype=jnp.int32)
    frame_total = frame_count * lax.axis_size(TM)
    row_total = row_count * lax.axis_size(ROW)
    frames = (lax.axis_index(TM) * frame_count + local[None] - window_shift[0][:, None]) % frame_total
    band = (lax.axis_index(ROW) * row_count + local[None] - window_shift[1][:, None]) % row_total
    frame_table = sinusoid(frames.reshape(-1), 256)
    row_table = sinusoid(band.reshape(-1), 384)
    column_table = sinusoid(jnp.arange(16, dtype=jnp.int32), 384)

    tables = (mask_token.reshape(8, 128), frame_table, row_table, column_table)
    *half_1, heads_1, w_qkv, w_out, w_head = early_part(
        shift_rows, own, *tables, hold(w_qkv), hold(w_out), hold(w_head)
    )
    *half_0, head_normed, head_scale, predicted = late_part(
        shift_rows, own, behind, *tables, half_1[0], heads_1, w_qkv, w_out, w_head
    )
    own_picked, behind_picked, local_total = backward_part(
        window_shift, *half_0, *half_1, head_normed, head_scale, predicted, w_qkv, w_out, w_head,
        own_target, row_target, last_row_target, time_target, corner_target,
    )
    from_next = move(behind_picked, TM, -1)
    mine = own_picked + from_next
    other = move(local_total, "tm_1", 1)
    local_total = local_total + other
    turned = [move(local_total, "tm_0", step) for step in (1, 2, 3)]
    local_total = (local_total + turned[1]) + (turned[0] + turned[2])
    high = local_total.astype(BF)
    low = (local_total - high.astype(F32)).astype(BF)
    sums = jnp.broadcast_to(jnp.concatenate([high, low], axis=1)[None], (peers, 8, 256))
    sent = jnp.concatenate([mine.reshape(peers, 2 * slots, D), sums], axis=-1)
    back = lax.all_to_all(sent, ROW, split_axis=0, concat_axis=0, tiled=True)
    grad_scale = (frame_total * row_total * pixels.shape[2]) ** (-0.5)
    outputs = [((peers, slots, D), BF), ((8, 128), F32)]
    unpack = call(functools.partial(unpack_kernel, grad_scale), outputs, [], in_space(VMEM, 1), 8)
    d_visible, d_mask = unpack(back)
    return (d_visible.reshape(visible.shape), d_mask.reshape(D))


def solution(mesh):
    torus = Mesh(mesh.devices.reshape(4, 2, 4, 4), ALL)
    return jax.shard_map(
        per_device,
        mesh=torus,
        in_specs=(
            P(TM, ROW, None, None, None),
            P(TM, ROW, None, None),
            P(),
            P(),
            P(),
            P(),
            P(),
            P(TM, ROW, None, None),
        ),
        out_specs=(P(TM, ROW, None, None, None), P()),
        check_vma=False,
    )
```

```python
import functools
import math

import jax
import jax.numpy as jnp
from jax import lax
from jax.experimental import pallas as pl
from jax.experimental.pallas import tpu as pltpu
from jax.sharding import Mesh
from jax.sharding import PartitionSpec as P

WT = 2
WH = 4
WW = 8
D = 1024
PIX = 1536
GROUP = PIX // 3
TOK = 256
HALF = TOK // 2
WIN = WT * WH * WW
PAIRS = D // 128
SLOTS = 128
TM = ("tm_0", "tm_1")
ROW = ("row_0", "row_1")
ALL = TM + ROW
BF = jnp.bfloat16
F32 = jnp.float32
NT_DIMS = (((1,), (1,)), ((), ()))
TN_DIMS = (((0,), (0,)), ((), ()))
NN_DIMS = (((1,), (0,)), ((), ()))
VMEM = pltpu.MemorySpace.VMEM
SMEM = pltpu.MemorySpace.SMEM
HBM = pltpu.MemorySpace.HBM


def dot(a, b, dims):
    return lax.dot_general(a, b, dims, preferred_element_type=F32)


def lane_mean(values):
    return jnp.sum(values, axis=-1, keepdims=True) * (1.0 / values.shape[-1])


def normalise(values):
    center = values - lane_mean(values)
    scale = lax.rsqrt(lane_mean(center * center) + 1e-05)
    return center * scale, scale


def normalise_back(cotangent, normed, scale):
    return scale * (cotangent - lane_mean(cotangent) - normed * lane_mean(cotangent * normed))


def two_heads(rows):
    first = lax.broadcasted_iota(jnp.int32, rows.shape, 1) < 64
    zero = jnp.zeros_like(rows)
    return jnp.concatenate([jnp.where(first, rows, zero), jnp.where(first, zero, rows)], axis=0)


def own_head(rows):
    first = lax.broadcasted_iota(jnp.int32, (WIN, 128), 1) < 64
    return jnp.where(first, rows[:WIN], rows[WIN:])


def slot_one_hot(shift_ref, rows_ref, behind, frame_pair):
    place = rows_ref[:, D : D + 128].astype(F32).astype(jnp.int32)
    frame = place >> 6
    row = (place >> 4) & 3
    column = place & 15
    group = column >> 3
    slot = lax.broadcasted_iota(jnp.int32, (SLOTS, 128), 0) & 7
    lane = lax.broadcasted_iota(jnp.int32, (SLOTS, 128), 1)
    frame = frame + jnp.where(group == 0, shift_ref[0:1], shift_ref[1:2]) - 4 * behind
    row = row + jnp.where(group == 0, shift_ref[2:3], shift_ref[3:4]) - jnp.where(slot >= 4, 4, 0)
    inside = (place >= 0) & ((frame >> 1) == frame_pair) & (row >= 0) & (row < 4)
    token = group * 64 + ((frame & 1) * 32) + row * 8 + (column & 7)
    token = jnp.where(inside, token, -1)
    return jnp.where(token == lane, 1.0, 0.0).astype(BF)


def embed(frame_pair, mask_ref, frames_ref, rows_ref, columns_ref, chosen_ref, seen_ref, embedded_ref, normed_ref):
    mask = mask_ref[...].astype(F32)
    mask = jnp.concatenate([mask[at : at + 1] for at in range(8)], axis=1)
    for block in range(HALF // 16):
        group, half = divmod(block, 4)
        at_frame = group * 4 + frame_pair * 2 + half // 2
        rows = slice(block * 16, block * 16 + 16)
        start = jnp.where(jnp.concatenate([seen_ref[rows]] * 8, axis=1) > 0, chosen_ref[rows], mask)
        position = []
        for at in range(2):
            at_row = group * 4 + (half % 2) * 2 + at
            position.append(
                jnp.concatenate(
                    [
                        jnp.broadcast_to(frames_ref[at_frame : at_frame + 1], (8, 256)),
                        jnp.broadcast_to(rows_ref[at_row : at_row + 1], (8, 384)),
                        columns_ref[group * 8 : group * 8 + 8],
                    ],
                    axis=1,
                )
            )
        embedded = (start + jnp.concatenate(position, axis=0)).astype(BF)
        embedded_ref[rows] = embedded
        normed_ref[rows] = normalise(embedded.astype(F32))[0].astype(BF)


def project(at, normed_ref, w_qkv_ref, qkv_ref):
    for part in range(2):
        cols = slice(at * D + part * 512, at * D + part * 512 + 512)
        qkv_ref[:, cols] = dot(normed_ref[...], w_qkv_ref[:, cols], NN_DIMS).astype(BF)


def attend(qkv_ref, probs_ref, heads_ref):
    for window in range(HALF // WIN):
        rows = slice(window * WIN, window * WIN + WIN)
        scores = []
        for pair in range(PAIRS):
            q = qkv_ref[rows, pair * 128 : pair * 128 + 128]
            k = qkv_ref[rows, D + pair * 128 : D + pair * 128 + 128]
            scores.append(dot(k, two_heads(q), NT_DIMS) * 0.125)
        probs = []
        for pair in range(PAIRS):
            weights = jnp.exp(scores[pair] - jnp.max(scores[pair], axis=0, keepdims=True))
            probs.append((weights * (1.0 / jnp.sum(weights, axis=0, keepdims=True))).astype(BF))
            probs_ref[window, pair] = probs[pair]
        for pair in range(PAIRS):
            v = qkv_ref[rows, 2 * D + pair * 128 : 2 * D + pair * 128 + 128]
            heads_ref[rows, pair * 128 : pair * 128 + 128] = own_head(dot(probs[pair], v, TN_DIMS)).astype(BF)


def early_kernel(
    shift_ref, own_ref, mask_ref, frames_ref, rows_ref, columns_ref, w_qkv_hbm, w_out_hbm, w_head_hbm,
    embedded_ref, qkv_ref, probs_ref, seen_ref, one_hot_ref, heads_ref, w_qkv_ref, w_out_ref, w_head_ref,
    chosen_ref, normed_ref, sems,
):
    copies = [
        pltpu.make_async_copy(
            w_qkv_hbm.at[:, pl.ds(at * D, D)], w_qkv_ref.at[:, pl.ds(at * D, D)], sems.at[at]
        )
        for at in range(3)
    ]
    copies.append(pltpu.make_async_copy(w_out_hbm, w_out_ref, sems.at[3]))
    copies.append(pltpu.make_async_copy(w_head_hbm, w_head_ref, sems.at[4]))
    for copy in copies:
        copy.start()
    one_hot_ref[...] = slot_one_hot(shift_ref, own_ref, 0, 1)
    chosen_ref[...] = dot(one_hot_ref[...], own_ref[:, :D], TN_DIMS)
    seen_ref[...] = dot(one_hot_ref[...], jnp.ones((SLOTS, 128), BF), TN_DIMS)
    embed(1, mask_ref, frames_ref, rows_ref, columns_ref, chosen_ref, seen_ref, embedded_ref, normed_ref)
    for at in range(3):
        copies[at].wait()
        project(at, normed_ref, w_qkv_ref, qkv_ref)
    attend(qkv_ref, probs_ref, heads_ref)
    copies[3].wait()
    copies[4].wait()


def late_kernel(
    shift_ref, own_ref, behind_ref, mask_ref, frames_ref, rows_ref, columns_ref, embedded_1_ref, heads_1_ref,
    w_qkv_ref, w_out_ref, w_head_ref,
    embedded_ref, qkv_ref, probs_ref, seen_ref, one_hot_ref, head_normed_ref, scale_ref, predicted_ref,
    chosen_ref, normed_ref, heads_ref, residual_ref, narrow_ref,
):
    one_hot_ref[:SLOTS] = slot_one_hot(shift_ref, own_ref, 0, 0)
    one_hot_ref[SLOTS:] = slot_one_hot(shift_ref, behind_ref, 1, 0)
    own_hot = one_hot_ref[:SLOTS]
    behind_hot = one_hot_ref[SLOTS:]
    chosen_ref[...] = dot(own_hot, own_ref[:, :D], TN_DIMS) + dot(behind_hot, behind_ref[:, :D], TN_DIMS)
    seen_ref[...] = dot(one_hot_ref[...], jnp.ones((2 * SLOTS, 128), BF), TN_DIMS)
    embed(0, mask_ref, frames_ref, rows_ref, columns_ref, chosen_ref, seen_ref, embedded_ref, normed_ref)
    for at in range(3):
        project(at, normed_ref, w_qkv_ref, qkv_ref)
    heads_ref[HALF:] = heads_1_ref[...]
    attend(qkv_ref, probs_ref, heads_ref)
    for part in range(2):
        cols = slice(part * 512, part * 512 + 512)
        attn = dot(heads_ref[...], w_out_ref[:, cols], NN_DIMS).astype(BF).astype(F32)
        residual_ref[:HALF, cols] = embedded_ref[:, cols].astype(F32) + attn[:HALF]
        residual_ref[HALF:, cols] = embedded_1_ref[:, cols].astype(F32) + attn[HALF:]
    for block in range(TOK // 16):
        rows = slice(block * 16, block * 16 + 16)
        normed, scale = normalise(residual_ref[rows])
        head_normed_ref[rows] = normed
        scale_ref[rows] = jnp.broadcast_to(scale, (16, 128))
        narrow_ref[rows] = normed.astype(BF)
    for part in range(3):
        cols = slice(part * GROUP, part * GROUP + GROUP)
        predicted_ref[:, cols] = dot(narrow_ref[...], w_head_ref[:, cols], NN_DIMS)


def backward_kernel(
    shift_ref, embedded_0_ref, qkv_0_ref, probs_0_ref, seen_0_ref, one_hot_0_ref,
    embedded_1_ref, qkv_1_ref, probs_1_ref, seen_1_ref, one_hot_1_ref,
    normed_ref, scale_ref, predicted_ref, w_qkv_ref, w_out_ref, w_head_ref,
    own_target, row_target, last_row_target, time_target, corner_target,
    own_picked_ref, behind_picked_ref, total_ref,
    target_ref, error_ref, narrow_ref, wide_ref, stream_ref, dqkv_ref,
):
    embedded_refs = (embedded_0_ref, embedded_1_ref)
    qkv_refs = (qkv_0_ref, qkv_1_ref)
    probs_refs = (probs_0_ref, probs_1_ref)
    seen_refs = (seen_0_ref, seen_1_ref)
    target_ref[1:, 3:] = own_target[...]
    target_ref[1:4, :3] = row_target[...]
    target_ref[4:, :3] = last_row_target[...]
    target_ref[:1, 3:] = time_target[...]
    target_ref[:1, :3] = corner_target[...]

    for block in range(TOK // 16):
        frame_pair, rest = divmod(block, 8)
        group, half = divmod(rest, 4)
        rows = slice(block * 16, block * 16 + 16)
        local = slice(rest * 16, rest * 16 + 16)
        masked = 1.0 - jnp.concatenate([seen_refs[frame_pair][local]] * 12, axis=1)
        target = jnp.concatenate(
            [
                target_ref[
                    frame_pair * 2 + half // 2 - shift_ref[0, group] + 1,
                    (half % 2) * 2 + at - shift_ref[1, group] + 3,
                    group * 8 : group * 8 + 8,
                ].astype(F32)
                for at in range(2)
            ],
            axis=0,
        )
        error_ref[rows] = (masked * (predicted_ref[rows] - target)).astype(BF)

    for part in range(2):
        cols = slice(part * 512, part * 512 + 512)
        wide_ref[:, cols] = dot(error_ref[...], w_head_ref[cols, :], NT_DIMS)

    for block in range(TOK // 16):
        rows = slice(block * 16, block * 16 + 16)
        scale = jnp.concatenate([scale_ref[rows]] * 8, axis=1)
        cotangent = wide_ref[rows].astype(BF).astype(F32)
        grad = normalise_back(cotangent, normed_ref[rows], scale)
        stream_ref[rows] = grad
        narrow_ref[rows] = grad.astype(BF)

    narrow_ref[...] = dot(narrow_ref[...], w_out_ref[...], NT_DIMS).astype(BF)

    for window in range(TOK // WIN):
        rows = slice(window * WIN, window * WIN + WIN)
        frame_pair, group = divmod(window, 2)
        local = slice(group * WIN, group * WIN + WIN)
        qkv_ref = qkv_refs[frame_pair]
        probs_ref = probs_refs[frame_pair]
        cols = [[slice(at * D + pair * 128, at * D + pair * 128 + 128) for at in range(3)] for pair in range(PAIRS)]
        d_probs = []
        out_heads = []
        for pair in range(PAIRS):
            out_heads.append(two_heads(narrow_ref[rows, cols[pair][0]]))
            d_probs.append(dot(qkv_ref[local, cols[pair][2]], out_heads[pair], NT_DIMS))
        for pair in range(PAIRS):
            dqkv_ref[rows, cols[pair][2]] = dot(probs_ref[group, pair], out_heads[pair], NN_DIMS).astype(BF)
        d_scores = []
        for pair in range(PAIRS):
            probs = probs_ref[group, pair].astype(F32)
            cotangent = d_probs[pair].astype(BF).astype(F32)
            mean = jnp.sum(cotangent * probs, axis=0, keepdims=True)
            d_scores.append((probs * (cotangent - mean) * 0.125).astype(BF))
        for pair in range(PAIRS):
            q_heads = two_heads(qkv_ref[local, cols[pair][0]])
            dqkv_ref[rows, cols[pair][1]] = dot(d_scores[pair], q_heads, NN_DIMS).astype(BF)
        for pair in range(PAIRS):
            d_q = own_head(dot(d_scores[pair], qkv_ref[local, cols[pair][1]], TN_DIMS))
            dqkv_ref[rows, cols[pair][0]] = d_q.astype(BF)

    for part in range(2):
        cols = slice(part * 512, part * 512 + 512)
        wide_ref[:, cols] = dot(dqkv_ref[...], w_qkv_ref[cols, :], NT_DIMS)

    total = jnp.zeros((8, D), F32)
    for block in range(TOK // 16):
        frame_pair, rest = divmod(block, 8)
        rows = slice(block * 16, block * 16 + 16)
        local = slice(rest * 16, rest * 16 + 16)
        normed, scale = normalise(embedded_refs[frame_pair][local].astype(F32))
        cotangent = wide_ref[rows].astype(BF).astype(F32)
        grad = stream_ref[rows] + normalise_back(cotangent, normed, scale)
        narrow_ref[rows] = grad.astype(BF)
        part = (1.0 - jnp.concatenate([seen_refs[frame_pair][local]] * 8, axis=1)) * grad
        total = total + part[:8] + part[8:]
    total = jnp.sum(total, axis=0, keepdims=True)
    total_ref[...] = jnp.concatenate([total[:, at * 128 : at * 128 + 128] for at in range(8)], axis=0)
    behind_picked_ref[...] = dot(one_hot_0_ref[SLOTS:], narrow_ref[:HALF], NN_DIMS).astype(BF)
    own_picked = dot(one_hot_0_ref[:SLOTS], narrow_ref[:HALF], NN_DIMS)
    own_picked_ref[...] = (own_picked + dot(one_hot_1_ref[...], narrow_ref[HALF:], NN_DIMS)).astype(BF)


def pack_kernel(
    place_hbm, shift_hbm, mask_hbm, rows_hbm, pixel_hbm,
    packed_ref, shift_rows_ref, mask_ref, pixel_ref,
    place_ref, shift_ref, rows_ref, sems,
):
    copies = [
        pltpu.make_async_copy(source, target, sems.at[at])
        for at, (source, target) in enumerate(
            [
                (rows_hbm, rows_ref),
                (place_hbm, place_ref),
                (shift_hbm, shift_ref),
                (mask_hbm, mask_ref),
                (pixel_hbm, pixel_ref),
            ]
        )
    ]
    for copy in copies:
        copy.start()
    copies[1].wait()
    slot = lax.broadcasted_iota(jnp.int32, (8, 128), 0)
    peers = rows_ref.shape[0]
    for peer in range(peers):
        places = jnp.zeros((8, 128), jnp.int32)
        for at in range(8):
            source = peer if at < 4 else (peer - 1) % peers
            places = jnp.where(slot == at, place_ref[at % 4, source], places)
        packed_ref[peer, :, D:] = places.astype(F32).astype(BF)
    copies[2].wait()
    shifts = jnp.zeros((8, 128), jnp.int32)
    for at in range(4):
        shifts = jnp.where(slot == at, shift_ref[at // 2, at % 2], shifts)
    shift_rows_ref[...] = shifts
    copies[0].wait()
    rows = rows_ref[...].astype(F32)
    before = jnp.concatenate([rows[-1:], rows[:-1]], axis=0)
    packed_ref[:, :, :D] = jnp.concatenate([rows, before], axis=1).astype(BF)
    copies[3].wait()
    copies[4].wait()


def target_kernel(pixel_ref, own_ref, row_ref, last_row_ref, time_ref):
    for frame in range(4):
        for row in range(4):
            for part in range(3):
                cols = slice(part * GROUP, part * GROUP + GROUP)
                raw = pixel_ref[frame, row, :, cols].astype(F32)
                center = raw - lane_mean(raw)
                spread = jnp.sqrt(jnp.sum(center * center, axis=-1, keepdims=True) * (1.0 / (GROUP - 1)))
                target = (center * (1.0 / (spread + 1e-06))).astype(BF)
                own_ref[frame, row, :, cols] = target
                if row > 0 and frame < 3:
                    row_ref[frame, row - 1, :, cols] = target
                if row > 0 and frame == 3:
                    last_row_ref[0, row - 1, :, cols] = target
                if frame == 3:
                    time_ref[0, row, :, cols] = target


def unpack_kernel(scale, back_ref, rows_ref, total_ref):
    rows = back_ref[:, :4, :D].astype(F32)
    after = back_ref[:, 4:, :D].astype(F32)
    after = jnp.concatenate([after[1:], after[:1]], axis=0)
    rows_ref[...] = (rows + after).astype(BF)
    sums = jnp.sum(back_ref[:, :, D:].astype(F32), axis=0)
    total_ref[...] = (sums[:, :128] + sums[:, 128:]) * scale


def shapes(*items):
    return [jax.ShapeDtypeStruct(dims, kind) for dims, kind in items]


def call(kernel, outputs, scratch, in_specs, limit):
    return pl.pallas_call(
        kernel,
        in_specs=in_specs,
        out_specs=[pl.BlockSpec(memory_space=VMEM)] * len(outputs),
        out_shape=shapes(*outputs),
        scratch_shapes=scratch,
        compiler_params=pltpu.CompilerParams(vmem_limit_bytes=limit << 20),
    )


def in_space(space, count):
    return [pl.BlockSpec(memory_space=space)] * count


def half_outputs(slots):
    return [
        ((HALF, D), BF),
        ((HALF, 3 * D), BF),
        ((HALF // WIN, PAIRS, WIN, 128), BF),
        ((HALF, 128), F32),
        ((slots, HALF), BF),
    ]


def pack_part(*operands):
    outputs = [((16, 8, D + 128), BF), ((8, 128), jnp.int32), ((8, 128), BF), ((4, 4, 16, PIX), BF)]
    scratch = [
        pltpu.SMEM((4, 16), jnp.int32),
        pltpu.SMEM((2, 2), jnp.int32),
        pltpu.VMEM((16, 4, D), BF),
        pltpu.SemaphoreType.DMA((5,)),
    ]
    return call(pack_kernel, outputs, scratch, in_space(HBM, 5), 8)(*operands)


def target_part(*operands):
    outputs = [((frames, rows, 16, PIX), BF) for frames, rows in ((4, 4), (3, 3), (1, 3), (1, 4))]
    return call(target_kernel, outputs, [], in_space(VMEM, 1), 8)(*operands)


def early_part(*operands):
    outputs = half_outputs(SLOTS) + [((HALF, D), BF), ((D, 3 * D), BF), ((D, D), BF), ((D, PIX), BF)]
    scratch = [pltpu.VMEM((HALF, D), F32), pltpu.VMEM((HALF, D), BF), pltpu.SemaphoreType.DMA((5,))]
    return call(early_kernel, outputs, scratch, in_space(VMEM, 6) + in_space(HBM, 3), 20)(*operands)


def late_part(*operands):
    outputs = half_outputs(2 * SLOTS) + [((TOK, D), F32), ((TOK, 128), F32), ((TOK, PIX), F32)]
    scratch = [
        pltpu.VMEM((HALF, D), F32),
        pltpu.VMEM((HALF, D), BF),
        pltpu.VMEM((TOK, D), BF),
        pltpu.VMEM((TOK, D), F32),
        pltpu.VMEM((TOK, D), BF),
    ]
    return call(late_kernel, outputs, scratch, in_space(VMEM, 12), 26)(*operands)


def backward_part(*operands):
    outputs = [((SLOTS, D), BF), ((SLOTS, D), BF), ((8, 128), F32)]
    scratch = [
        pltpu.VMEM((5, 7, 16, PIX), BF),
        pltpu.VMEM((TOK, PIX), BF),
        pltpu.VMEM((TOK, D), BF),
        pltpu.VMEM((TOK, D), F32),
        pltpu.VMEM((TOK, D), F32),
        pltpu.VMEM((TOK, 3 * D), BF),
    ]
    return call(backward_kernel, outputs, scratch, in_space(SMEM, 1) + in_space(VMEM, 21), 34)(*operands)


def sinusoid(coordinate, channel_count):
    half_count = channel_count // 2
    frequency = jnp.exp(-math.log(10000.0) * jnp.arange(half_count, dtype=F32) / half_count)
    angles = coordinate.astype(F32)[..., None] * frequency
    return jnp.concatenate([jnp.sin(angles), jnp.cos(angles)], axis=-1)


def move(value, axis, steps):
    count = lax.axis_size(axis)
    return lax.ppermute(value, axis, [(at, (at + steps) % count) for at in range(count)])


def per_device(visible, slot_pos, window_shift, mask_token, w_qkv, w_out, w_head, pixels):
    frame_count, row_count = pixels.shape[:2]
    peers, slots = slot_pos.shape[2:]
    hold = functools.partial(pltpu.with_memory_space_constraint, memory_space=HBM)
    packed, shift_rows, mask_rows, near_pixels = pack_part(
        hold(slot_pos.reshape(peers, slots).T),
        hold(window_shift),
        hold(mask_token.reshape(8, 128)),
        hold(visible.reshape(peers, slots, D)),
        hold(pixels),
    )
    own = lax.all_to_all(packed, ROW, split_axis=0, concat_axis=0, tiled=True).reshape(SLOTS, D + 128)
    behind = move(own, TM, 1)
    own_target, row_target, last_row_target, time_target = target_part(near_pixels)
    last_row_target = move(last_row_target, ROW, 1)
    row_target = move(row_target, ROW, 1)
    time_target = move(time_target, TM, 1)
    corner_target = move(last_row_target, TM, 1)

    local = jnp.arange(4, dtype=jnp.int32)
    frame_total = frame_count * lax.axis_size(TM)
    row_total = row_count * lax.axis_size(ROW)
    frames = (lax.axis_index(TM) * frame_count + local[None] - window_shift[0][:, None]) % frame_total
    band = (lax.axis_index(ROW) * row_count + local[None] - window_shift[1][:, None]) % row_total
    frame_table = sinusoid(frames.reshape(-1), 256)
    row_table = sinusoid(band.reshape(-1), 384)
    column_table = sinusoid(jnp.arange(16, dtype=jnp.int32), 384)

    tables = (mask_rows, frame_table, row_table, column_table)
    *half_1, heads_1, w_qkv, w_out, w_head = early_part(
        shift_rows, own, *tables, hold(w_qkv), hold(w_out), hold(w_head)
    )
    *half_0, head_normed, head_scale, predicted = late_part(
        shift_rows, own, behind, *tables, half_1[0], heads_1, w_qkv, w_out, w_head
    )
    own_picked, behind_picked, local_total = backward_part(
        window_shift, *half_0, *half_1, head_normed, head_scale, predicted, w_qkv, w_out, w_head,
        own_target, row_target, last_row_target, time_target, corner_target,
    )
    from_next = move(behind_picked, TM, -1)
    mine = own_picked + from_next
    other = move(local_total, "tm_1", 1)
    local_total = local_total + other
    for bit in (1, 2):
        pairs = [(at, at ^ bit) for at in range(lax.axis_size("tm_0"))]
        local_total = local_total + lax.ppermute(local_total, "tm_0", pairs)
    high = local_total.astype(BF)
    low = (local_total - high.astype(F32)).astype(BF)
    sums = jnp.broadcast_to(jnp.concatenate([high, low], axis=1)[None], (peers, 8, 256))
    sent = jnp.concatenate([mine.reshape(peers, 2 * slots, D), sums], axis=-1)
    back = lax.all_to_all(sent, ROW, split_axis=0, concat_axis=0, tiled=True)
    grad_scale = (frame_total * row_total * pixels.shape[2]) ** (-0.5)
    outputs = [((peers, slots, D), BF), ((8, 128), F32)]
    unpack = call(functools.partial(unpack_kernel, grad_scale), outputs, [], in_space(VMEM, 1), 8)
    d_visible, d_mask = unpack(back)
    return (d_visible.reshape(visible.shape), d_mask.reshape(D))


def solution(mesh):
    torus = Mesh(mesh.devices.reshape(4, 2, 4, 4), ALL)
    return jax.shard_map(
        per_device,
        mesh=torus,
        in_specs=(
            P(TM, ROW, None, None, None),
            P(TM, ROW, None, None),
            P(),
            P(),
            P(),
            P(),
            P(),
            P(TM, ROW, None, None),
        ),
        out_specs=(P(TM, ROW, None, None, None), P()),
        check_vma=False,
    )
```

```python
import functools
import math

import jax
import jax.numpy as jnp
from jax import lax
from jax.experimental import pallas as pl
from jax.experimental.pallas import tpu as pltpu
from jax.sharding import Mesh
from jax.sharding import PartitionSpec as P

WT = 2
WH = 4
WW = 8
D = 1024
PIX = 1536
GROUP = PIX // 3
TOK = 256
HALF = TOK // 2
WIN = WT * WH * WW
PAIRS = D // 128
SLOTS = 128
TM = ("tm_0", "tm_1")
ROW = ("row_0", "row_1")
ALL = TM + ROW
BF = jnp.bfloat16
F32 = jnp.float32
NT_DIMS = (((1,), (1,)), ((), ()))
TN_DIMS = (((0,), (0,)), ((), ()))
NN_DIMS = (((1,), (0,)), ((), ()))
VMEM = pltpu.MemorySpace.VMEM
SMEM = pltpu.MemorySpace.SMEM
HBM = pltpu.MemorySpace.HBM


def dot(a, b, dims):
    return lax.dot_general(a, b, dims, preferred_element_type=F32)


def lane_mean(values):
    return jnp.sum(values, axis=-1, keepdims=True) * (1.0 / values.shape[-1])


def normalise(values):
    center = values - lane_mean(values)
    scale = lax.rsqrt(lane_mean(center * center) + 1e-05)
    return center * scale, scale


def normalise_back(cotangent, normed, scale):
    return scale * (cotangent - lane_mean(cotangent) - normed * lane_mean(cotangent * normed))


def two_heads(rows):
    first = lax.broadcasted_iota(jnp.int32, rows.shape, 1) < 64
    zero = jnp.zeros_like(rows)
    return jnp.concatenate([jnp.where(first, rows, zero), jnp.where(first, zero, rows)], axis=0)


def own_head(rows):
    first = lax.broadcasted_iota(jnp.int32, (WIN, 128), 1) < 64
    return jnp.where(first, rows[:WIN], rows[WIN:])


def slot_one_hot(shift_ref, rows_ref, behind, frame_pair):
    place = rows_ref[:, D : D + 128].astype(F32).astype(jnp.int32)
    frame = place >> 6
    row = (place >> 4) & 3
    column = place & 15
    group = column >> 3
    slot = lax.broadcasted_iota(jnp.int32, (SLOTS, 128), 0) & 7
    lane = lax.broadcasted_iota(jnp.int32, (SLOTS, 128), 1)
    frame = frame + jnp.where(group == 0, shift_ref[0:1], shift_ref[1:2]) - 4 * behind
    row = row + jnp.where(group == 0, shift_ref[2:3], shift_ref[3:4]) - jnp.where(slot >= 4, 4, 0)
    inside = (place >= 0) & ((frame >> 1) == frame_pair) & (row >= 0) & (row < 4)
    token = group * 64 + ((frame & 1) * 32) + row * 8 + (column & 7)
    token = jnp.where(inside, token, -1)
    return jnp.where(token == lane, 1.0, 0.0).astype(BF)


def embed(frame_pair, mask_ref, frames_ref, rows_ref, columns_ref, chosen_ref, seen_ref, embedded_ref, normed_ref):
    mask = mask_ref[...].astype(F32)
    mask = jnp.concatenate([mask[at : at + 1] for at in range(8)], axis=1)
    for block in range(HALF // 16):
        group, half = divmod(block, 4)
        at_frame = group * 4 + frame_pair * 2 + half // 2
        rows = slice(block * 16, block * 16 + 16)
        start = jnp.where(jnp.concatenate([seen_ref[rows]] * 8, axis=1) > 0, chosen_ref[rows], mask)
        position = []
        for at in range(2):
            at_row = group * 4 + (half % 2) * 2 + at
            position.append(
                jnp.concatenate(
                    [
                        jnp.broadcast_to(frames_ref[at_frame : at_frame + 1], (8, 256)),
                        jnp.broadcast_to(rows_ref[at_row : at_row + 1], (8, 384)),
                        columns_ref[group * 8 : group * 8 + 8],
                    ],
                    axis=1,
                )
            )
        embedded = (start + jnp.concatenate(position, axis=0)).astype(BF)
        embedded_ref[rows] = embedded
        normed_ref[rows] = normalise(embedded.astype(F32))[0].astype(BF)


def project(at, normed_ref, w_qkv_ref, qkv_ref):
    for part in range(2):
        cols = slice(at * D + part * 512, at * D + part * 512 + 512)
        qkv_ref[:, cols] = dot(normed_ref[...], w_qkv_ref[:, cols], NN_DIMS).astype(BF)


def attend(qkv_ref, probs_ref, heads_ref):
    for window in range(HALF // WIN):
        rows = slice(window * WIN, window * WIN + WIN)
        scores = []
        for pair in range(PAIRS):
            q = qkv_ref[rows, pair * 128 : pair * 128 + 128]
            k = qkv_ref[rows, D + pair * 128 : D + pair * 128 + 128]
            scores.append(dot(k, two_heads(q), NT_DIMS) * 0.125)
        probs = []
        for pair in range(PAIRS):
            weights = jnp.exp(scores[pair] - jnp.max(scores[pair], axis=0, keepdims=True))
            probs.append((weights * (1.0 / jnp.sum(weights, axis=0, keepdims=True))).astype(BF))
            probs_ref[window, pair] = probs[pair]
        for pair in range(PAIRS):
            v = qkv_ref[rows, 2 * D + pair * 128 : 2 * D + pair * 128 + 128]
            heads_ref[rows, pair * 128 : pair * 128 + 128] = own_head(dot(probs[pair], v, TN_DIMS)).astype(BF)


def early_kernel(
    shift_ref, own_ref, mask_ref, frames_ref, rows_ref, columns_ref, w_qkv_hbm, w_out_hbm, w_head_hbm,
    embedded_ref, qkv_ref, probs_ref, seen_ref, one_hot_ref, heads_ref, w_qkv_ref, w_out_ref, w_head_ref,
    chosen_ref, normed_ref, sems,
):
    copies = [
        pltpu.make_async_copy(
            w_qkv_hbm.at[:, pl.ds(at * D, D)], w_qkv_ref.at[:, pl.ds(at * D, D)], sems.at[at]
        )
        for at in range(3)
    ]
    copies.append(pltpu.make_async_copy(w_out_hbm, w_out_ref, sems.at[3]))
    copies.append(pltpu.make_async_copy(w_head_hbm, w_head_ref, sems.at[4]))
    for copy in copies:
        copy.start()
    one_hot_ref[...] = slot_one_hot(shift_ref, own_ref, 0, 1)
    chosen_ref[...] = dot(one_hot_ref[...], own_ref[:, :D], TN_DIMS)
    seen_ref[...] = dot(one_hot_ref[...], jnp.ones((SLOTS, 128), BF), TN_DIMS)
    embed(1, mask_ref, frames_ref, rows_ref, columns_ref, chosen_ref, seen_ref, embedded_ref, normed_ref)
    for at in range(3):
        copies[at].wait()
        project(at, normed_ref, w_qkv_ref, qkv_ref)
    attend(qkv_ref, probs_ref, heads_ref)
    copies[3].wait()
    copies[4].wait()


def late_kernel(
    shift_ref, own_ref, behind_ref, mask_ref, frames_ref, rows_ref, columns_ref, embedded_1_ref, heads_1_ref,
    w_qkv_ref, w_out_ref, w_head_ref,
    embedded_ref, qkv_ref, probs_ref, seen_ref, one_hot_ref, head_normed_ref, scale_ref, predicted_ref,
    chosen_ref, normed_ref, heads_ref, residual_ref, narrow_ref,
):
    one_hot_ref[:SLOTS] = slot_one_hot(shift_ref, own_ref, 0, 0)
    one_hot_ref[SLOTS:] = slot_one_hot(shift_ref, behind_ref, 1, 0)
    own_hot = one_hot_ref[:SLOTS]
    behind_hot = one_hot_ref[SLOTS:]
    chosen_ref[...] = dot(own_hot, own_ref[:, :D], TN_DIMS) + dot(behind_hot, behind_ref[:, :D], TN_DIMS)
    seen_ref[...] = dot(one_hot_ref[...], jnp.ones((2 * SLOTS, 128), BF), TN_DIMS)
    embed(0, mask_ref, frames_ref, rows_ref, columns_ref, chosen_ref, seen_ref, embedded_ref, normed_ref)
    for at in range(3):
        project(at, normed_ref, w_qkv_ref, qkv_ref)
    heads_ref[HALF:] = heads_1_ref[...]
    attend(qkv_ref, probs_ref, heads_ref)
    for part in range(2):
        cols = slice(part * 512, part * 512 + 512)
        attn = dot(heads_ref[...], w_out_ref[:, cols], NN_DIMS).astype(BF).astype(F32)
        residual_ref[:HALF, cols] = embedded_ref[:, cols].astype(F32) + attn[:HALF]
        residual_ref[HALF:, cols] = embedded_1_ref[:, cols].astype(F32) + attn[HALF:]
    for block in range(TOK // 16):
        rows = slice(block * 16, block * 16 + 16)
        normed, scale = normalise(residual_ref[rows])
        head_normed_ref[rows] = normed
        scale_ref[rows] = jnp.broadcast_to(scale, (16, 128))
        narrow_ref[rows] = normed.astype(BF)
    for part in range(3):
        cols = slice(part * GROUP, part * GROUP + GROUP)
        predicted_ref[:, cols] = dot(narrow_ref[...], w_head_ref[:, cols], NN_DIMS)


def backward_kernel(
    shift_ref, embedded_0_ref, qkv_0_ref, probs_0_ref, seen_0_ref, one_hot_0_ref,
    embedded_1_ref, qkv_1_ref, probs_1_ref, seen_1_ref, one_hot_1_ref,
    normed_ref, scale_ref, predicted_ref, w_qkv_ref, w_out_ref, w_head_ref,
    own_target, row_target, last_row_target, time_target, corner_target,
    own_picked_ref, behind_rows_ref, total_ref,
    target_ref, error_ref, narrow_ref, wide_ref, stream_ref, dqkv_ref,
):
    embedded_refs = (embedded_0_ref, embedded_1_ref)
    qkv_refs = (qkv_0_ref, qkv_1_ref)
    probs_refs = (probs_0_ref, probs_1_ref)
    seen_refs = (seen_0_ref, seen_1_ref)
    target_ref[1:, 3:] = own_target[...]
    target_ref[1:4, :3] = row_target[...]
    target_ref[4:, :3] = last_row_target[...]
    target_ref[:1, 3:] = time_target[...]
    target_ref[:1, :3] = corner_target[...]

    for block in range(TOK // 16):
        frame_pair, rest = divmod(block, 8)
        group, half = divmod(rest, 4)
        rows = slice(block * 16, block * 16 + 16)
        local = slice(rest * 16, rest * 16 + 16)
        masked = 1.0 - jnp.concatenate([seen_refs[frame_pair][local]] * 12, axis=1)
        target = jnp.concatenate(
            [
                target_ref[
                    frame_pair * 2 + half // 2 - shift_ref[0, group] + 1,
                    (half % 2) * 2 + at - shift_ref[1, group] + 3,
                    group * 8 : group * 8 + 8,
                ].astype(F32)
                for at in range(2)
            ],
            axis=0,
        )
        error_ref[rows] = (masked * (predicted_ref[rows] - target)).astype(BF)

    for part in range(2):
        cols = slice(part * 512, part * 512 + 512)
        wide_ref[:, cols] = dot(error_ref[...], w_head_ref[cols, :], NT_DIMS)

    for block in range(TOK // 16):
        rows = slice(block * 16, block * 16 + 16)
        scale = jnp.concatenate([scale_ref[rows]] * 8, axis=1)
        cotangent = wide_ref[rows].astype(BF).astype(F32)
        grad = normalise_back(cotangent, normed_ref[rows], scale)
        stream_ref[rows] = grad
        narrow_ref[rows] = grad.astype(BF)

    narrow_ref[...] = dot(narrow_ref[...], w_out_ref[...], NT_DIMS).astype(BF)

    for window in range(TOK // WIN):
        rows = slice(window * WIN, window * WIN + WIN)
        frame_pair, group = divmod(window, 2)
        local = slice(group * WIN, group * WIN + WIN)
        qkv_ref = qkv_refs[frame_pair]
        probs_ref = probs_refs[frame_pair]
        cols = [[slice(at * D + pair * 128, at * D + pair * 128 + 128) for at in range(3)] for pair in range(PAIRS)]
        d_probs = []
        out_heads = []
        for pair in range(PAIRS):
            out_heads.append(two_heads(narrow_ref[rows, cols[pair][0]]))
            d_probs.append(dot(qkv_ref[local, cols[pair][2]], out_heads[pair], NT_DIMS))
        for pair in range(PAIRS):
            dqkv_ref[rows, cols[pair][2]] = dot(probs_ref[group, pair], out_heads[pair], NN_DIMS).astype(BF)
        d_scores = []
        for pair in range(PAIRS):
            probs = probs_ref[group, pair].astype(F32)
            cotangent = d_probs[pair].astype(BF).astype(F32)
            mean = jnp.sum(cotangent * probs, axis=0, keepdims=True)
            d_scores.append((probs * (cotangent - mean) * 0.125).astype(BF))
        for pair in range(PAIRS):
            q_heads = two_heads(qkv_ref[local, cols[pair][0]])
            dqkv_ref[rows, cols[pair][1]] = dot(d_scores[pair], q_heads, NN_DIMS).astype(BF)
        for pair in range(PAIRS):
            d_q = own_head(dot(d_scores[pair], qkv_ref[local, cols[pair][1]], TN_DIMS))
            dqkv_ref[rows, cols[pair][0]] = d_q.astype(BF)

    for part in range(2):
        cols = slice(part * 512, part * 512 + 512)
        wide_ref[:, cols] = dot(dqkv_ref[...], w_qkv_ref[cols, :], NT_DIMS)

    total = jnp.zeros((8, D), F32)
    for block in range(TOK // 16):
        frame_pair, rest = divmod(block, 8)
        rows = slice(block * 16, block * 16 + 16)
        local = slice(rest * 16, rest * 16 + 16)
        normed, scale = normalise(embedded_refs[frame_pair][local].astype(F32))
        cotangent = wide_ref[rows].astype(BF).astype(F32)
        grad = stream_ref[rows] + normalise_back(cotangent, normed, scale)
        narrow_ref[rows] = grad.astype(BF)
        part = (1.0 - jnp.concatenate([seen_refs[frame_pair][local]] * 8, axis=1)) * grad
        total = total + part[:8] + part[8:]
    total = jnp.sum(total, axis=0, keepdims=True)
    total_ref[...] = jnp.concatenate([total[:, at * 128 : at * 128 + 128] for at in range(8)], axis=0)
    behind_rows_ref[...] = jnp.where(
        shift_ref[0, 1] == 1, narrow_ref[WIN : WIN + 32].astype(F32), narrow_ref[:32].astype(F32)
    ).astype(BF)
    own_picked = dot(one_hot_0_ref[:SLOTS], narrow_ref[:HALF], NN_DIMS)
    own_picked_ref[...] = (own_picked + dot(one_hot_1_ref[...], narrow_ref[HALF:], NN_DIMS)).astype(BF)


def give_kernel(
    shift_ref, own_ref, picked_ref, next_ref, total_ref, turned_1_ref, turned_2_ref, turned_3_ref, sent_ref
):
    place = own_ref[:, D : D + 128].astype(F32).astype(jnp.int32)
    row = (place >> 4) & 3
    column = place & 15
    slot = lax.broadcasted_iota(jnp.int32, (SLOTS, 128), 0) & 7
    lane = lax.broadcasted_iota(jnp.int32, (SLOTS, 128), 1)
    late = jnp.where(column < 8, shift_ref[0:1], shift_ref[1:2])
    row = row + jnp.where(column < 8, shift_ref[2:3], shift_ref[3:4]) - jnp.where(slot >= 4, 4, 0)
    inside = (place >= 192) & (late == 1) & (row >= 0) & (row < 4)
    token = jnp.where(inside, row * 8 + (column & 7), -1)
    one_hot = jnp.where(token == lane, 1.0, 0.0).astype(BF)
    rows = jnp.concatenate([next_ref[...], jnp.zeros((SLOTS - 32, D), BF)], axis=0)
    picked = picked_ref[...].astype(F32) + dot(one_hot, rows, NN_DIMS)
    sent_ref[:, :, :D] = picked.reshape(16, 8, D).astype(BF)
    total = (total_ref[...] + turned_2_ref[...]) + (turned_1_ref[...] + turned_3_ref[...])
    high = total.astype(BF)
    low = (total - high.astype(F32)).astype(BF)
    for peer in range(16):
        sent_ref[peer, :, D : D + 128] = high
        sent_ref[peer, :, D + 128 :] = low


def pack_kernel(
    place_hbm, shift_hbm, mask_hbm, rows_hbm, pixel_hbm,
    packed_ref, shift_rows_ref, mask_ref, pixel_ref,
    place_ref, shift_ref, rows_ref, sems,
):
    copies = [
        pltpu.make_async_copy(source, target, sems.at[at])
        for at, (source, target) in enumerate(
            [
                (rows_hbm, rows_ref),
                (place_hbm, place_ref),
                (shift_hbm, shift_ref),
                (mask_hbm, mask_ref),
                (pixel_hbm, pixel_ref),
            ]
        )
    ]
    for copy in copies:
        copy.start()
    copies[1].wait()
    slot = lax.broadcasted_iota(jnp.int32, (8, 128), 0)
    peers = rows_ref.shape[0]
    for peer in range(peers):
        places = jnp.zeros((8, 128), jnp.int32)
        for at in range(8):
            source = peer if at < 4 else (peer - 1) % peers
            places = jnp.where(slot == at, place_ref[at % 4, source], places)
        packed_ref[peer, :, D:] = places.astype(F32).astype(BF)
    copies[2].wait()
    shifts = jnp.zeros((8, 128), jnp.int32)
    for at in range(4):
        shifts = jnp.where(slot == at, shift_ref[at // 2, at % 2], shifts)
    shift_rows_ref[...] = shifts
    copies[0].wait()
    rows = rows_ref[...].astype(F32)
    before = jnp.concatenate([rows[-1:], rows[:-1]], axis=0)
    packed_ref[:, :, :D] = jnp.concatenate([rows, before], axis=1).astype(BF)
    copies[3].wait()
    copies[4].wait()


def sinusoid(coordinate, channel_count):
    half_count = channel_count // 2
    lane = lax.broadcasted_iota(jnp.int32, (coordinate.shape[0], channel_count), 1)
    channel = jnp.where(lane < half_count, lane, lane - half_count).astype(F32)
    angles = coordinate.astype(F32) * jnp.exp(-math.log(10000.0) * channel / half_count)
    return jnp.where(lane < half_count, jnp.sin(angles), jnp.cos(angles))


def grid_coordinates(start, offsets_ref, first, total, channel_count):
    row = lax.broadcasted_iota(jnp.int32, (8, 128), 0)
    offset = jnp.where(row < 4, offsets_ref[first : first + 1], offsets_ref[first + 1 : first + 2])
    coordinate = start + (row & 3) - offset
    coordinate = jnp.where(coordinate < 0, coordinate + total, coordinate)
    return jnp.concatenate([coordinate] * (channel_count // 128), axis=1)


def target_kernel(
    totals, shift_rows_ref, pixel_ref, own_ref, row_ref, last_row_ref, time_ref, frames_ref, rows_ref, columns_ref
):
    frames = grid_coordinates(lax.axis_index(TM) * 4, shift_rows_ref, 0, totals[0], 256)
    rows = grid_coordinates(lax.axis_index(ROW) * 4, shift_rows_ref, 2, totals[1], 384)
    frames_ref[...] = sinusoid(frames, 256)
    rows_ref[...] = sinusoid(rows, 384)
    columns_ref[...] = sinusoid(lax.broadcasted_iota(jnp.int32, (16, 384), 0), 384)
    for frame in range(4):
        for row in range(4):
            for part in range(3):
                cols = slice(part * GROUP, part * GROUP + GROUP)
                raw = pixel_ref[frame, row, :, cols].astype(F32)
                center = raw - lane_mean(raw)
                spread = jnp.sqrt(jnp.sum(center * center, axis=-1, keepdims=True) * (1.0 / (GROUP - 1)))
                target = (center * (1.0 / (spread + 1e-06))).astype(BF)
                own_ref[frame, row, :, cols] = target
                if row > 0 and frame < 3:
                    row_ref[frame, row - 1, :, cols] = target
                if row > 0 and frame == 3:
                    last_row_ref[0, row - 1, :, cols] = target
                if frame == 3:
                    time_ref[0, row, :, cols] = target


def unpack_kernel(scale, back_ref, rows_ref, total_ref):
    rows = back_ref[:, :4, :D].astype(F32)
    after = back_ref[:, 4:, :D].astype(F32)
    after = jnp.concatenate([after[1:], after[:1]], axis=0)
    rows_ref[...] = (rows + after).astype(BF)
    sums = jnp.sum(back_ref[:, :, D:].astype(F32), axis=0)
    total_ref[...] = (sums[:, :128] + sums[:, 128:]) * scale


def shapes(*items):
    return [jax.ShapeDtypeStruct(dims, kind) for dims, kind in items]


def call(kernel, outputs, scratch, in_specs, limit):
    return pl.pallas_call(
        kernel,
        in_specs=in_specs,
        out_specs=[pl.BlockSpec(memory_space=VMEM)] * len(outputs),
        out_shape=shapes(*outputs),
        scratch_shapes=scratch,
        compiler_params=pltpu.CompilerParams(vmem_limit_bytes=limit << 20),
    )


def in_space(space, count):
    return [pl.BlockSpec(memory_space=space)] * count


def half_outputs(slots):
    return [
        ((HALF, D), BF),
        ((HALF, 3 * D), BF),
        ((HALF // WIN, PAIRS, WIN, 128), BF),
        ((HALF, 128), F32),
        ((slots, HALF), BF),
    ]


def pack_part(*operands):
    outputs = [((16, 8, D + 128), BF), ((8, 128), jnp.int32), ((8, 128), BF), ((4, 4, 16, PIX), BF)]
    scratch = [
        pltpu.SMEM((4, 16), jnp.int32),
        pltpu.SMEM((2, 2), jnp.int32),
        pltpu.VMEM((16, 4, D), BF),
        pltpu.SemaphoreType.DMA((5,)),
    ]
    return call(pack_kernel, outputs, scratch, in_space(HBM, 5), 8)(*operands)


def target_part(totals, *operands):
    outputs = [((frames, rows, 16, PIX), BF) for frames, rows in ((4, 4), (3, 3), (1, 3), (1, 4))]
    outputs += [((8, 256), F32), ((8, 384), F32), ((16, 384), F32)]
    kernel = functools.partial(target_kernel, totals)
    return call(kernel, outputs, [], in_space(VMEM, 2), 8)(*operands)


def early_part(*operands):
    outputs = half_outputs(SLOTS) + [((HALF, D), BF), ((D, 3 * D), BF), ((D, D), BF), ((D, PIX), BF)]
    scratch = [pltpu.VMEM((HALF, D), F32), pltpu.VMEM((HALF, D), BF), pltpu.SemaphoreType.DMA((5,))]
    return call(early_kernel, outputs, scratch, in_space(VMEM, 6) + in_space(HBM, 3), 20)(*operands)


def late_part(*operands):
    outputs = half_outputs(2 * SLOTS) + [((TOK, D), F32), ((TOK, 128), F32), ((TOK, PIX), F32)]
    scratch = [
        pltpu.VMEM((HALF, D), F32),
        pltpu.VMEM((HALF, D), BF),
        pltpu.VMEM((TOK, D), BF),
        pltpu.VMEM((TOK, D), F32),
        pltpu.VMEM((TOK, D), BF),
    ]
    return call(late_kernel, outputs, scratch, in_space(VMEM, 12), 26)(*operands)


def backward_part(*operands):
    outputs = [((SLOTS, D), BF), ((32, D), BF), ((8, 128), F32)]
    scratch = [
        pltpu.VMEM((5, 7, 16, PIX), BF),
        pltpu.VMEM((TOK, PIX), BF),
        pltpu.VMEM((TOK, D), BF),
        pltpu.VMEM((TOK, D), F32),
        pltpu.VMEM((TOK, D), F32),
        pltpu.VMEM((TOK, 3 * D), BF),
    ]
    return call(backward_kernel, outputs, scratch, in_space(SMEM, 1) + in_space(VMEM, 21), 34)(*operands)


def move(value, axis, steps):
    count = lax.axis_size(axis)
    return lax.ppermute(value, axis, [(at, (at + steps) % count) for at in range(count)])


def per_device(visible, slot_pos, window_shift, mask_token, w_qkv, w_out, w_head, pixels):
    frame_count, row_count = pixels.shape[:2]
    peers, slots = slot_pos.shape[2:]
    hold = functools.partial(pltpu.with_memory_space_constraint, memory_space=HBM)
    packed, shift_rows, mask_rows, near_pixels = pack_part(
        hold(slot_pos.reshape(peers, slots).T),
        hold(window_shift),
        hold(mask_token.reshape(8, 128)),
        hold(visible.reshape(peers, slots, D)),
        hold(pixels),
    )
    own = lax.all_to_all(packed, ROW, split_axis=0, concat_axis=0, tiled=True).reshape(SLOTS, D + 128)
    behind = move(own, TM, 1)
    frame_total = frame_count * lax.axis_size(TM)
    row_total = row_count * lax.axis_size(ROW)
    own_target, row_target, last_row_target, time_target, *positions = target_part(
        (frame_total, row_total), shift_rows, near_pixels
    )
    last_row_target = move(last_row_target, ROW, 1)
    row_target = move(row_target, ROW, 1)
    time_target = move(time_target, TM, 1)
    corner_target = move(last_row_target, TM, 1)

    tables = (mask_rows, *positions)
    *half_1, heads_1, w_qkv, w_out, w_head = early_part(
        shift_rows, own, *tables, hold(w_qkv), hold(w_out), hold(w_head)
    )
    *half_0, head_normed, head_scale, predicted = late_part(
        shift_rows, own, behind, *tables, half_1[0], heads_1, w_qkv, w_out, w_head
    )
    own_picked, behind_rows, local_total = backward_part(
        window_shift, *half_0, *half_1, head_normed, head_scale, predicted, w_qkv, w_out, w_head,
        own_target, row_target, last_row_target, time_target, corner_target,
    )
    other = move(local_total, "tm_1", 1)
    from_next = move(behind_rows, TM, -1)
    local_total = local_total + other
    turned = [move(local_total, "tm_0", step) for step in (1, 2, 3)]
    give = call(give_kernel, [((peers, 8, D + 256), BF)], [], in_space(VMEM, 8), 8)
    (sent,) = give(shift_rows, own, own_picked, from_next, local_total, *turned)
    back = lax.all_to_all(sent, ROW, split_axis=0, concat_axis=0, tiled=True)
    grad_scale = (frame_total * row_total * pixels.shape[2]) ** (-0.5)
    outputs = [((peers, slots, D), BF), ((8, 128), F32)]
    unpack = call(functools.partial(unpack_kernel, grad_scale), outputs, [], in_space(VMEM, 1), 8)
    d_visible, d_mask = unpack(back)
    return (d_visible.reshape(visible.shape), d_mask.reshape(D))


def solution(mesh):
    torus = Mesh(mesh.devices.reshape(4, 2, 4, 4), ALL)
    return jax.shard_map(
        per_device,
        mesh=torus,
        in_specs=(
            P(TM, ROW, None, None, None),
            P(TM, ROW, None, None),
            P(),
            P(),
            P(),
            P(),
            P(),
            P(TM, ROW, None, None),
        ),
        out_specs=(P(TM, ROW, None, None, None), P()),
        check_vma=False,
    )
```

```python
import functools
import math

import jax
import jax.numpy as jnp
from jax import lax
from jax.experimental import pallas as pl
from jax.experimental.pallas import tpu as pltpu
from jax.sharding import Mesh
from jax.sharding import PartitionSpec as P

WT = 2
WH = 4
WW = 8
D = 1024
PIX = 1536
GROUP = PIX // 3
TOK = 256
HALF = TOK // 2
WIN = WT * WH * WW
PAIRS = D // 128
SLOTS = 128
TM = ("tm_0", "tm_1")
ROW = ("row_0", "row_1")
ALL = TM + ROW
BF = jnp.bfloat16
F32 = jnp.float32
NT_DIMS = (((1,), (1,)), ((), ()))
TN_DIMS = (((0,), (0,)), ((), ()))
NN_DIMS = (((1,), (0,)), ((), ()))
VMEM = pltpu.MemorySpace.VMEM
SMEM = pltpu.MemorySpace.SMEM
HBM = pltpu.MemorySpace.HBM


def dot(a, b, dims):
    return lax.dot_general(a, b, dims, preferred_element_type=F32)


def lane_mean(values):
    return jnp.sum(values, axis=-1, keepdims=True) * (1.0 / values.shape[-1])


def normalise(values):
    center = values - lane_mean(values)
    scale = lax.rsqrt(lane_mean(center * center) + 1e-05)
    return center * scale, scale


def normalise_back(cotangent, normed, scale):
    return scale * (cotangent - lane_mean(cotangent) - normed * lane_mean(cotangent * normed))


def two_heads(rows):
    first = lax.broadcasted_iota(jnp.int32, rows.shape, 1) < 64
    zero = jnp.zeros_like(rows)
    return jnp.concatenate([jnp.where(first, rows, zero), jnp.where(first, zero, rows)], axis=0)


def own_head(rows):
    first = lax.broadcasted_iota(jnp.int32, (WIN, 128), 1) < 64
    return jnp.where(first, rows[:WIN], rows[WIN:])


def slot_one_hot(shift_ref, rows_ref, behind, frame_pair):
    place = rows_ref[:, D : D + 128].astype(F32).astype(jnp.int32)
    frame = place >> 6
    row = (place >> 4) & 3
    column = place & 15
    group = column >> 3
    slot = lax.broadcasted_iota(jnp.int32, (SLOTS, 128), 0) & 7
    lane = lax.broadcasted_iota(jnp.int32, (SLOTS, 128), 1)
    frame = frame + jnp.where(group == 0, shift_ref[0:1], shift_ref[1:2]) - 4 * behind
    row = row + jnp.where(group == 0, shift_ref[2:3], shift_ref[3:4]) - jnp.where(slot >= 4, 4, 0)
    inside = (place >= 0) & ((frame >> 1) == frame_pair) & (row >= 0) & (row < 4)
    token = group * 64 + ((frame & 1) * 32) + row * 8 + (column & 7)
    token = jnp.where(inside, token, -1)
    return jnp.where(token == lane, 1.0, 0.0).astype(BF)


def embed(frame_pair, mask_ref, frames_ref, rows_ref, columns_ref, chosen_ref, seen_ref, embedded_ref, normed_ref):
    mask = mask_ref[...].astype(F32)
    mask = jnp.concatenate([mask[at : at + 1] for at in range(8)], axis=1)
    for block in range(HALF // 16):
        group, half = divmod(block, 4)
        at_frame = group * 4 + frame_pair * 2 + half // 2
        rows = slice(block * 16, block * 16 + 16)
        start = jnp.where(jnp.concatenate([seen_ref[rows]] * 8, axis=1) > 0, chosen_ref[rows], mask)
        position = []
        for at in range(2):
            at_row = group * 4 + (half % 2) * 2 + at
            position.append(
                jnp.concatenate(
                    [
                        jnp.broadcast_to(frames_ref[at_frame : at_frame + 1], (8, 256)),
                        jnp.broadcast_to(rows_ref[at_row : at_row + 1], (8, 384)),
                        columns_ref[group * 8 : group * 8 + 8],
                    ],
                    axis=1,
                )
            )
        embedded = (start + jnp.concatenate(position, axis=0)).astype(BF)
        embedded_ref[rows] = embedded
        normed_ref[rows] = normalise(embedded.astype(F32))[0].astype(BF)


def project(at, normed_ref, w_qkv_ref, qkv_ref):
    for part in range(2):
        cols = slice(at * D + part * 512, at * D + part * 512 + 512)
        qkv_ref[:, cols] = dot(normed_ref[...], w_qkv_ref[:, cols], NN_DIMS).astype(BF)


def attend(qkv_ref, probs_ref, heads_ref):
    for window in range(HALF // WIN):
        rows = slice(window * WIN, window * WIN + WIN)
        scores = []
        for pair in range(PAIRS):
            q = qkv_ref[rows, pair * 128 : pair * 128 + 128]
            k = qkv_ref[rows, D + pair * 128 : D + pair * 128 + 128]
            scores.append(dot(k, two_heads(q), NT_DIMS) * 0.125)
        probs = []
        for pair in range(PAIRS):
            weights = jnp.exp(scores[pair] - jnp.max(scores[pair], axis=0, keepdims=True))
            probs.append((weights * (1.0 / jnp.sum(weights, axis=0, keepdims=True))).astype(BF))
            probs_ref[window, pair] = probs[pair]
        for pair in range(PAIRS):
            v = qkv_ref[rows, 2 * D + pair * 128 : 2 * D + pair * 128 + 128]
            heads_ref[rows, pair * 128 : pair * 128 + 128] = own_head(dot(probs[pair], v, TN_DIMS)).astype(BF)


def early_kernel(
    shift_ref, own_ref, mask_ref, frames_ref, rows_ref, columns_ref, w_qkv_hbm, w_out_hbm,
    embedded_ref, qkv_ref, probs_ref, seen_ref, one_hot_ref, heads_ref, w_qkv_ref, w_out_ref,
    chosen_ref, normed_ref, sems,
):
    copies = [
        pltpu.make_async_copy(
            w_qkv_hbm.at[:, pl.ds(at * D, D)], w_qkv_ref.at[:, pl.ds(at * D, D)], sems.at[at]
        )
        for at in range(3)
    ]
    copies.append(pltpu.make_async_copy(w_out_hbm, w_out_ref, sems.at[3]))
    for copy in copies:
        copy.start()
    one_hot_ref[...] = slot_one_hot(shift_ref, own_ref, 0, 1)
    chosen_ref[...] = dot(one_hot_ref[...], own_ref[:, :D], TN_DIMS)
    seen_ref[...] = dot(one_hot_ref[...], jnp.ones((SLOTS, 128), BF), TN_DIMS)
    embed(1, mask_ref, frames_ref, rows_ref, columns_ref, chosen_ref, seen_ref, embedded_ref, normed_ref)
    for at in range(3):
        copies[at].wait()
        project(at, normed_ref, w_qkv_ref, qkv_ref)
    attend(qkv_ref, probs_ref, heads_ref)
    copies[3].wait()


def late_kernel(
    shift_ref, own_ref, behind_ref, mask_ref, frames_ref, rows_ref, columns_ref, embedded_1_ref, heads_1_ref,
    w_qkv_ref, w_out_ref, w_head_hbm,
    embedded_ref, qkv_ref, probs_ref, seen_ref, one_hot_ref, head_normed_ref, scale_ref, predicted_ref, w_head_ref,
    chosen_ref, normed_ref, heads_ref, residual_ref, narrow_ref, sem,
):
    head_copy = pltpu.make_async_copy(w_head_hbm, w_head_ref, sem)
    head_copy.start()
    one_hot_ref[:SLOTS] = slot_one_hot(shift_ref, own_ref, 0, 0)
    one_hot_ref[SLOTS:] = slot_one_hot(shift_ref, behind_ref, 1, 0)
    own_hot = one_hot_ref[:SLOTS]
    behind_hot = one_hot_ref[SLOTS:]
    chosen_ref[...] = dot(own_hot, own_ref[:, :D], TN_DIMS) + dot(behind_hot, behind_ref[:, :D], TN_DIMS)
    seen_ref[...] = dot(one_hot_ref[...], jnp.ones((2 * SLOTS, 128), BF), TN_DIMS)
    embed(0, mask_ref, frames_ref, rows_ref, columns_ref, chosen_ref, seen_ref, embedded_ref, normed_ref)
    for at in range(3):
        project(at, normed_ref, w_qkv_ref, qkv_ref)
    heads_ref[HALF:] = heads_1_ref[...]
    attend(qkv_ref, probs_ref, heads_ref)
    for part in range(2):
        cols = slice(part * 512, part * 512 + 512)
        attn = dot(heads_ref[...], w_out_ref[:, cols], NN_DIMS).astype(BF).astype(F32)
        residual_ref[:HALF, cols] = embedded_ref[:, cols].astype(F32) + attn[:HALF]
        residual_ref[HALF:, cols] = embedded_1_ref[:, cols].astype(F32) + attn[HALF:]
    for block in range(TOK // 16):
        rows = slice(block * 16, block * 16 + 16)
        normed, scale = normalise(residual_ref[rows])
        head_normed_ref[rows] = normed
        scale_ref[rows] = jnp.broadcast_to(scale, (16, 128))
        narrow_ref[rows] = normed.astype(BF)
    head_copy.wait()
    for part in range(3):
        cols = slice(part * GROUP, part * GROUP + GROUP)
        predicted_ref[:, cols] = dot(narrow_ref[...], w_head_ref[:, cols], NN_DIMS)


def backward_kernel(
    shift_ref, embedded_0_ref, qkv_0_ref, probs_0_ref, seen_0_ref, one_hot_0_ref,
    embedded_1_ref, qkv_1_ref, probs_1_ref, seen_1_ref, one_hot_1_ref,
    normed_ref, scale_ref, predicted_ref, w_qkv_ref, w_out_ref, w_head_ref,
    own_target, first_row_target, row_target, last_row_target, time_target, corner_target,
    own_picked_ref, behind_rows_ref, total_ref,
    target_ref, error_ref, narrow_ref, wide_ref, stream_ref, dqkv_ref,
):
    embedded_refs = (embedded_0_ref, embedded_1_ref)
    qkv_refs = (qkv_0_ref, qkv_1_ref)
    probs_refs = (probs_0_ref, probs_1_ref)
    seen_refs = (seen_0_ref, seen_1_ref)
    target_ref[1:, 3:] = own_target[...]
    target_ref[1:2, :3] = first_row_target[...]
    target_ref[2:4, :3] = row_target[...]
    target_ref[4:, :3] = last_row_target[...]
    target_ref[:1, 3:] = time_target[...]
    target_ref[:1, :3] = corner_target[...]

    for block in range(TOK // 16):
        frame_pair, rest = divmod(block, 8)
        group, half = divmod(rest, 4)
        rows = slice(block * 16, block * 16 + 16)
        local = slice(rest * 16, rest * 16 + 16)
        masked = 1.0 - jnp.concatenate([seen_refs[frame_pair][local]] * 12, axis=1)
        target = jnp.concatenate(
            [
                target_ref[
                    frame_pair * 2 + half // 2 - shift_ref[0, group] + 1,
                    (half % 2) * 2 + at - shift_ref[1, group] + 3,
                    group * 8 : group * 8 + 8,
                ].astype(F32)
                for at in range(2)
            ],
            axis=0,
        )
        error_ref[rows] = (masked * (predicted_ref[rows] - target)).astype(BF)

    for part in range(2):
        cols = slice(part * 512, part * 512 + 512)
        wide_ref[:, cols] = dot(error_ref[...], w_head_ref[cols, :], NT_DIMS)

    for block in range(TOK // 16):
        rows = slice(block * 16, block * 16 + 16)
        scale = jnp.concatenate([scale_ref[rows]] * 8, axis=1)
        cotangent = wide_ref[rows].astype(BF).astype(F32)
        grad = normalise_back(cotangent, normed_ref[rows], scale)
        stream_ref[rows] = grad
        narrow_ref[rows] = grad.astype(BF)

    narrow_ref[...] = dot(narrow_ref[...], w_out_ref[...], NT_DIMS).astype(BF)

    for window in range(TOK // WIN):
        rows = slice(window * WIN, window * WIN + WIN)
        frame_pair, group = divmod(window, 2)
        local = slice(group * WIN, group * WIN + WIN)
        qkv_ref = qkv_refs[frame_pair]
        probs_ref = probs_refs[frame_pair]
        cols = [[slice(at * D + pair * 128, at * D + pair * 128 + 128) for at in range(3)] for pair in range(PAIRS)]
        d_probs = []
        out_heads = []
        for pair in range(PAIRS):
            out_heads.append(two_heads(narrow_ref[rows, cols[pair][0]]))
            d_probs.append(dot(qkv_ref[local, cols[pair][2]], out_heads[pair], NT_DIMS))
        for pair in range(PAIRS):
            dqkv_ref[rows, cols[pair][2]] = dot(probs_ref[group, pair], out_heads[pair], NN_DIMS).astype(BF)
        d_scores = []
        for pair in range(PAIRS):
            probs = probs_ref[group, pair].astype(F32)
            cotangent = d_probs[pair].astype(BF).astype(F32)
            mean = jnp.sum(cotangent * probs, axis=0, keepdims=True)
            d_scores.append((probs * (cotangent - mean) * 0.125).astype(BF))
        for pair in range(PAIRS):
            q_heads = two_heads(qkv_ref[local, cols[pair][0]])
            dqkv_ref[rows, cols[pair][1]] = dot(d_scores[pair], q_heads, NN_DIMS).astype(BF)
        for pair in range(PAIRS):
            d_q = own_head(dot(d_scores[pair], qkv_ref[local, cols[pair][1]], TN_DIMS))
            dqkv_ref[rows, cols[pair][0]] = d_q.astype(BF)

    for part in range(2):
        cols = slice(part * 512, part * 512 + 512)
        wide_ref[:, cols] = dot(dqkv_ref[...], w_qkv_ref[cols, :], NT_DIMS)

    total = jnp.zeros((8, D), F32)
    for block in range(TOK // 16):
        frame_pair, rest = divmod(block, 8)
        rows = slice(block * 16, block * 16 + 16)
        local = slice(rest * 16, rest * 16 + 16)
        normed, scale = normalise(embedded_refs[frame_pair][local].astype(F32))
        cotangent = wide_ref[rows].astype(BF).astype(F32)
        grad = stream_ref[rows] + normalise_back(cotangent, normed, scale)
        narrow_ref[rows] = grad.astype(BF)
        part = (1.0 - jnp.concatenate([seen_refs[frame_pair][local]] * 8, axis=1)) * grad
        total = total + part[:8] + part[8:]
    total = jnp.sum(total, axis=0, keepdims=True)
    total_ref[...] = jnp.concatenate([total[:, at * 128 : at * 128 + 128] for at in range(8)], axis=0)
    behind_rows_ref[...] = jnp.where(
        shift_ref[0, 1] == 1, narrow_ref[WIN : WIN + 32].astype(F32), narrow_ref[:32].astype(F32)
    ).astype(BF)
    own_picked = dot(one_hot_0_ref[:SLOTS], narrow_ref[:HALF], NN_DIMS)
    own_picked_ref[...] = (own_picked + dot(one_hot_1_ref[...], narrow_ref[HALF:], NN_DIMS)).astype(BF)


def give_kernel(
    shift_ref, own_ref, picked_ref, next_ref, total_ref, far_ref, sent_ref
):
    place = own_ref[:, D : D + 128].astype(F32).astype(jnp.int32)
    row = (place >> 4) & 3
    column = place & 15
    slot = lax.broadcasted_iota(jnp.int32, (SLOTS, 128), 0) & 7
    lane = lax.broadcasted_iota(jnp.int32, (SLOTS, 128), 1)
    late = jnp.where(column < 8, shift_ref[0:1], shift_ref[1:2])
    row = row + jnp.where(column < 8, shift_ref[2:3], shift_ref[3:4]) - jnp.where(slot >= 4, 4, 0)
    inside = (place >= 192) & (late == 1) & (row >= 0) & (row < 4)
    token = jnp.where(inside, row * 8 + (column & 7), -1)
    one_hot = jnp.where(token == lane, 1.0, 0.0).astype(BF)
    rows = jnp.concatenate([next_ref[...], jnp.zeros((SLOTS - 32, D), BF)], axis=0)
    picked = picked_ref[...].astype(F32) + dot(one_hot, rows, NN_DIMS)
    sent_ref[:, :, :D] = picked.reshape(16, 8, D).astype(BF)
    total = total_ref[...] + far_ref[...]
    high = total.astype(BF)
    low = (total - high.astype(F32)).astype(BF)
    for peer in range(16):
        sent_ref[peer, :, D : D + 128] = high
        sent_ref[peer, :, D + 128 :] = low


def pack_kernel(
    place_hbm, shift_hbm, mask_hbm, rows_hbm, pixel_hbm,
    packed_ref, shift_rows_ref, mask_ref, pixel_ref,
    place_ref, shift_ref, rows_ref, sems,
):
    copies = [
        pltpu.make_async_copy(source, target, sems.at[at])
        for at, (source, target) in enumerate(
            [
                (rows_hbm, rows_ref),
                (place_hbm, place_ref),
                (shift_hbm, shift_ref),
                (mask_hbm, mask_ref),
                (pixel_hbm, pixel_ref),
            ]
        )
    ]
    for copy in copies:
        copy.start()
    copies[1].wait()
    slot = lax.broadcasted_iota(jnp.int32, (8, 128), 0)
    peers = rows_ref.shape[0]
    for peer in range(peers):
        places = jnp.zeros((8, 128), jnp.int32)
        for at in range(8):
            source = peer if at < 4 else (peer - 1) % peers
            places = jnp.where(slot == at, place_ref[at % 4, source], places)
        packed_ref[peer, :, D:] = places.astype(F32).astype(BF)
    copies[2].wait()
    shifts = jnp.zeros((8, 128), jnp.int32)
    for at in range(4):
        shifts = jnp.where(slot == at, shift_ref[at // 2, at % 2], shifts)
    shift_rows_ref[...] = shifts
    copies[0].wait()
    rows = rows_ref[...].astype(F32)
    before = jnp.concatenate([rows[-1:], rows[:-1]], axis=0)
    packed_ref[:, :, :D] = jnp.concatenate([rows, before], axis=1).astype(BF)
    copies[3].wait()
    copies[4].wait()


def sinusoid(coordinate, channel_count):
    half_count = channel_count // 2
    lane = lax.broadcasted_iota(jnp.int32, (coordinate.shape[0], channel_count), 1)
    channel = jnp.where(lane < half_count, lane, lane - half_count).astype(F32)
    angles = coordinate.astype(F32) * jnp.exp(-math.log(10000.0) * channel / half_count)
    return jnp.where(lane < half_count, jnp.sin(angles), jnp.cos(angles))


def grid_coordinates(start, offsets_ref, first, total, channel_count):
    row = lax.broadcasted_iota(jnp.int32, (8, 128), 0)
    offset = jnp.where(row < 4, offsets_ref[first : first + 1], offsets_ref[first + 1 : first + 2])
    coordinate = start + (row & 3) - offset
    coordinate = jnp.where(coordinate < 0, coordinate + total, coordinate)
    return jnp.concatenate([coordinate] * (channel_count // 128), axis=1)


def target_kernel(
    totals, shift_rows_ref, pixel_ref, own_ref, first_row_ref, row_ref, last_row_ref, time_ref, frames_ref, rows_ref, columns_ref
):
    frames = grid_coordinates(lax.axis_index(TM) * 4, shift_rows_ref, 0, totals[0], 256)
    rows = grid_coordinates(lax.axis_index(ROW) * 4, shift_rows_ref, 2, totals[1], 384)
    frames_ref[...] = sinusoid(frames, 256)
    rows_ref[...] = sinusoid(rows, 384)
    columns_ref[...] = sinusoid(lax.broadcasted_iota(jnp.int32, (16, 384), 0), 384)
    for frame in range(4):
        for row in range(4):
            for part in range(3):
                cols = slice(part * GROUP, part * GROUP + GROUP)
                raw = pixel_ref[frame, row, :, cols].astype(F32)
                center = raw - lane_mean(raw)
                spread = jnp.sqrt(jnp.sum(center * center, axis=-1, keepdims=True) * (1.0 / (GROUP - 1)))
                target = (center * (1.0 / (spread + 1e-06))).astype(BF)
                own_ref[frame, row, :, cols] = target
                if row > 0 and frame == 0:
                    first_row_ref[0, row - 1, :, cols] = target
                if row > 0 and 0 < frame < 3:
                    row_ref[frame - 1, row - 1, :, cols] = target
                if row > 0 and frame == 3:
                    last_row_ref[0, row - 1, :, cols] = target
                if frame == 3:
                    time_ref[0, row, :, cols] = target


def unpack_kernel(scale, back_ref, rows_ref, total_ref):
    rows = back_ref[:, :4, :D].astype(F32)
    after = back_ref[:, 4:, :D].astype(F32)
    after = jnp.concatenate([after[1:], after[:1]], axis=0)
    rows_ref[...] = (rows + after).astype(BF)
    sums = jnp.sum(back_ref[:, :, D:].astype(F32), axis=0)
    total_ref[...] = (sums[:, :128] + sums[:, 128:]) * scale


def shapes(*items):
    return [jax.ShapeDtypeStruct(dims, kind) for dims, kind in items]


def call(kernel, outputs, scratch, in_specs, limit):
    return pl.pallas_call(
        kernel,
        in_specs=in_specs,
        out_specs=[pl.BlockSpec(memory_space=VMEM)] * len(outputs),
        out_shape=shapes(*outputs),
        scratch_shapes=scratch,
        compiler_params=pltpu.CompilerParams(vmem_limit_bytes=limit << 20),
    )


def in_space(space, count):
    return [pl.BlockSpec(memory_space=space)] * count


def half_outputs(slots):
    return [
        ((HALF, D), BF),
        ((HALF, 3 * D), BF),
        ((HALF // WIN, PAIRS, WIN, 128), BF),
        ((HALF, 128), F32),
        ((slots, HALF), BF),
    ]


def pack_part(*operands):
    outputs = [((16, 8, D + 128), BF), ((8, 128), jnp.int32), ((8, 128), BF), ((4, 4, 16, PIX), BF)]
    scratch = [
        pltpu.SMEM((4, 16), jnp.int32),
        pltpu.SMEM((2, 2), jnp.int32),
        pltpu.VMEM((16, 4, D), BF),
        pltpu.SemaphoreType.DMA((5,)),
    ]
    return call(pack_kernel, outputs, scratch, in_space(HBM, 5), 8)(*operands)


def target_part(totals, *operands):
    outputs = [((frames, rows, 16, PIX), BF) for frames, rows in ((4, 4), (1, 3), (2, 3), (1, 3), (1, 4))]
    outputs += [((8, 256), F32), ((8, 384), F32), ((16, 384), F32)]
    kernel = functools.partial(target_kernel, totals)
    return call(kernel, outputs, [], in_space(VMEM, 2), 8)(*operands)


def early_part(*operands):
    outputs = half_outputs(SLOTS) + [((HALF, D), BF), ((D, 3 * D), BF), ((D, D), BF)]
    scratch = [pltpu.VMEM((HALF, D), F32), pltpu.VMEM((HALF, D), BF), pltpu.SemaphoreType.DMA((4,))]
    return call(early_kernel, outputs, scratch, in_space(VMEM, 6) + in_space(HBM, 2), 20)(*operands)


def late_part(*operands):
    outputs = half_outputs(2 * SLOTS) + [((TOK, D), F32), ((TOK, 128), F32), ((TOK, PIX), F32), ((D, PIX), BF)]
    scratch = [
        pltpu.VMEM((HALF, D), F32),
        pltpu.VMEM((HALF, D), BF),
        pltpu.VMEM((TOK, D), BF),
        pltpu.VMEM((TOK, D), F32),
        pltpu.VMEM((TOK, D), BF),
        pltpu.SemaphoreType.DMA,
    ]
    return call(late_kernel, outputs, scratch, in_space(VMEM, 11) + in_space(HBM, 1), 28)(*operands)


def backward_part(*operands):
    outputs = [((SLOTS, D), BF), ((32, D), BF), ((8, 128), F32)]
    scratch = [
        pltpu.VMEM((5, 7, 16, PIX), BF),
        pltpu.VMEM((TOK, PIX), BF),
        pltpu.VMEM((TOK, D), BF),
        pltpu.VMEM((TOK, D), F32),
        pltpu.VMEM((TOK, D), F32),
        pltpu.VMEM((TOK, 3 * D), BF),
    ]
    return call(backward_kernel, outputs, scratch, in_space(SMEM, 1) + in_space(VMEM, 22), 34)(*operands)


def move(value, axis, steps):
    count = lax.axis_size(axis)
    return lax.ppermute(value, axis, [(at, (at + steps) % count) for at in range(count)])


def per_device(visible, slot_pos, window_shift, mask_token, w_qkv, w_out, w_head, pixels):
    frame_count, row_count = pixels.shape[:2]
    peers, slots = slot_pos.shape[2:]
    hold = functools.partial(pltpu.with_memory_space_constraint, memory_space=HBM)
    packed, shift_rows, mask_rows, near_pixels = pack_part(
        hold(slot_pos.reshape(peers, slots).T),
        hold(window_shift),
        hold(mask_token.reshape(8, 128)),
        hold(visible.reshape(peers, slots, D)),
        hold(pixels),
    )
    own = lax.all_to_all(packed, ROW, split_axis=0, concat_axis=0, tiled=True).reshape(SLOTS, D + 128)
    behind = move(own, TM, 1)
    frame_total = frame_count * lax.axis_size(TM)
    row_total = row_count * lax.axis_size(ROW)
    own_target, first_row_target, row_target, last_row_target, time_target, *positions = target_part(
        (frame_total, row_total), shift_rows, near_pixels
    )
    last_row_target = move(last_row_target, ROW, 1)
    first_row_target = move(first_row_target, ROW, 1)
    row_target = move(row_target, ROW, 1)
    time_target = move(time_target, TM, 1)
    corner_target = move(last_row_target, TM, 1)

    tables = (mask_rows, *positions)
    *half_1, heads_1, w_qkv, w_out = early_part(shift_rows, own, *tables, hold(w_qkv), hold(w_out))
    *half_0, head_normed, head_scale, predicted, w_head = late_part(
        shift_rows, own, behind, *tables, half_1[0], heads_1, w_qkv, w_out, hold(w_head)
    )
    own_picked, behind_rows, local_total = backward_part(
        window_shift, *half_0, *half_1, head_normed, head_scale, predicted, w_qkv, w_out, w_head,
        own_target, first_row_target, row_target, last_row_target, time_target, corner_target,
    )
    other = move(local_total, "tm_1", 1)
    from_next = move(behind_rows, TM, -1)
    local_total = local_total + other
    pairs = [(at, at ^ 1) for at in range(lax.axis_size("tm_0"))]
    local_total = local_total + lax.ppermute(local_total, "tm_0", pairs)
    far = move(local_total, "tm_0", 2)
    give = call(give_kernel, [((peers, 8, D + 256), BF)], [], in_space(VMEM, 6), 8)
    (sent,) = give(shift_rows, own, own_picked, from_next, local_total, far)
    back = lax.all_to_all(sent, ROW, split_axis=0, concat_axis=0, tiled=True)
    grad_scale = (frame_total * row_total * pixels.shape[2]) ** (-0.5)
    outputs = [((peers, slots, D), BF), ((8, 128), F32)]
    unpack = call(functools.partial(unpack_kernel, grad_scale), outputs, [], in_space(VMEM, 1), 8)
    d_visible, d_mask = unpack(back)
    return (d_visible.reshape(visible.shape), d_mask.reshape(D))


def solution(mesh):
    torus = Mesh(mesh.devices.reshape(4, 2, 4, 4), ALL)
    return jax.shard_map(
        per_device,
        mesh=torus,
        in_specs=(
            P(TM, ROW, None, None, None),
            P(TM, ROW, None, None),
            P(),
            P(),
            P(),
            P(),
            P(),
            P(TM, ROW, None, None),
        ),
        out_specs=(P(TM, ROW, None, None, None), P()),
        check_vma=False,
    )
```

```python
import functools
import math

import jax
import jax.numpy as jnp
from jax import lax
from jax.experimental import pallas as pl
from jax.experimental.pallas import tpu as pltpu
from jax.sharding import Mesh
from jax.sharding import PartitionSpec as P

WT = 2
WH = 4
WW = 8
D = 1024
PIX = 1536
GROUP = PIX // 3
TOK = 256
HALF = TOK // 2
WIN = WT * WH * WW
PAIRS = D // 128
SLOTS = 128
TM = ("tm_0", "tm_1")
ROW = ("row_0", "row_1")
ALL = TM + ROW
BF = jnp.bfloat16
F32 = jnp.float32
NT_DIMS = (((1,), (1,)), ((), ()))
TN_DIMS = (((0,), (0,)), ((), ()))
NN_DIMS = (((1,), (0,)), ((), ()))
VMEM = pltpu.MemorySpace.VMEM
SMEM = pltpu.MemorySpace.SMEM
HBM = pltpu.MemorySpace.HBM


def dot(a, b, dims):
    return lax.dot_general(a, b, dims, preferred_element_type=F32)


def lane_mean(values):
    return jnp.sum(values, axis=-1, keepdims=True) * (1.0 / values.shape[-1])


def normalise(values):
    center = values - lane_mean(values)
    scale = lax.rsqrt(lane_mean(center * center) + 1e-05)
    return center * scale, scale


def normalise_back(cotangent, normed, scale):
    return scale * (cotangent - lane_mean(cotangent) - normed * lane_mean(cotangent * normed))


def two_heads(rows):
    first = lax.broadcasted_iota(jnp.int32, rows.shape, 1) < 64
    zero = jnp.zeros_like(rows)
    return jnp.concatenate([jnp.where(first, rows, zero), jnp.where(first, zero, rows)], axis=0)


def own_head(rows):
    first = lax.broadcasted_iota(jnp.int32, (WIN, 128), 1) < 64
    return jnp.where(first, rows[:WIN], rows[WIN:])


def slot_one_hot(shift_ref, rows_ref, behind, frame_pair):
    place = rows_ref[:, D : D + 128].astype(F32).astype(jnp.int32)
    frame = place >> 6
    row = (place >> 4) & 3
    column = place & 15
    group = column >> 3
    slot = lax.broadcasted_iota(jnp.int32, (SLOTS, 128), 0) & 7
    lane = lax.broadcasted_iota(jnp.int32, (SLOTS, 128), 1)
    frame = frame + jnp.where(group == 0, shift_ref[0:1], shift_ref[1:2]) - 4 * behind
    row = row + jnp.where(group == 0, shift_ref[2:3], shift_ref[3:4]) + jnp.where(slot >= 4, 4, 0)
    inside = (place >= 0) & ((frame >> 1) == frame_pair) & (row >= 0) & (row < 4)
    token = group * 64 + ((frame & 1) * 32) + row * 8 + (column & 7)
    token = jnp.where(inside, token, -1)
    return jnp.where(token == lane, 1.0, 0.0).astype(BF)


def embed(frame_pair, mask_ref, frames_ref, rows_ref, columns_ref, chosen_ref, seen_ref, embedded_ref, normed_ref):
    mask = mask_ref[...].astype(F32)
    mask = jnp.concatenate([mask[at : at + 1] for at in range(8)], axis=1)
    for block in range(HALF // 16):
        group, half = divmod(block, 4)
        at_frame = group * 4 + frame_pair * 2 + half // 2
        rows = slice(block * 16, block * 16 + 16)
        start = jnp.where(jnp.concatenate([seen_ref[rows]] * 8, axis=1) > 0, chosen_ref[rows], mask)
        position = []
        for at in range(2):
            at_row = group * 4 + (half % 2) * 2 + at
            position.append(
                jnp.concatenate(
                    [
                        jnp.broadcast_to(frames_ref[at_frame : at_frame + 1], (8, 256)),
                        jnp.broadcast_to(rows_ref[at_row : at_row + 1], (8, 384)),
                        columns_ref[group * 8 : group * 8 + 8],
                    ],
                    axis=1,
                )
            )
        embedded = (start + jnp.concatenate(position, axis=0)).astype(BF)
        embedded_ref[rows] = embedded
        normed_ref[rows] = normalise(embedded.astype(F32))[0].astype(BF)


def project(at, normed_ref, w_qkv_ref, qkv_ref):
    for part in range(2):
        cols = slice(at * D + part * 512, at * D + part * 512 + 512)
        qkv_ref[:, cols] = dot(normed_ref[...], w_qkv_ref[:, cols], NN_DIMS).astype(BF)


def attend(qkv_ref, probs_ref, heads_ref):
    for window in range(HALF // WIN):
        rows = slice(window * WIN, window * WIN + WIN)
        scores = []
        for pair in range(PAIRS):
            q = qkv_ref[rows, pair * 128 : pair * 128 + 128]
            k = qkv_ref[rows, D + pair * 128 : D + pair * 128 + 128]
            scores.append(dot(k, two_heads(q), NT_DIMS) * 0.125)
        probs = []
        for pair in range(PAIRS):
            weights = jnp.exp(scores[pair] - jnp.max(scores[pair], axis=0, keepdims=True))
            probs.append((weights * (1.0 / jnp.sum(weights, axis=0, keepdims=True))).astype(BF))
            probs_ref[window, pair] = probs[pair]
        for pair in range(PAIRS):
            v = qkv_ref[rows, 2 * D + pair * 128 : 2 * D + pair * 128 + 128]
            heads_ref[rows, pair * 128 : pair * 128 + 128] = own_head(dot(probs[pair], v, TN_DIMS)).astype(BF)


def early_kernel(
    shift_ref, own_ref, mask_ref, frames_ref, rows_ref, columns_ref, w_qkv_hbm, w_out_hbm, w_head_hbm,
    embedded_ref, qkv_ref, probs_ref, seen_ref, one_hot_ref, heads_ref, w_qkv_ref, w_out_ref, w_head_ref,
    chosen_ref, normed_ref, sems,
):
    copies = [
        pltpu.make_async_copy(
            w_qkv_hbm.at[:, pl.ds(at * D, D)], w_qkv_ref.at[:, pl.ds(at * D, D)], sems.at[at]
        )
        for at in range(3)
    ]
    copies.append(pltpu.make_async_copy(w_out_hbm, w_out_ref, sems.at[3]))
    copies.append(pltpu.make_async_copy(w_head_hbm, w_head_ref, sems.at[4]))
    for copy in copies:
        copy.start()
    one_hot_ref[...] = slot_one_hot(shift_ref, own_ref, 0, 1)
    chosen_ref[...] = dot(one_hot_ref[...], own_ref[:, :D], TN_DIMS)
    seen_ref[...] = dot(one_hot_ref[...], jnp.ones((SLOTS, 128), BF), TN_DIMS)
    embed(1, mask_ref, frames_ref, rows_ref, columns_ref, chosen_ref, seen_ref, embedded_ref, normed_ref)
    for at in range(3):
        copies[at].wait()
        project(at, normed_ref, w_qkv_ref, qkv_ref)
    attend(qkv_ref, probs_ref, heads_ref)
    copies[3].wait()
    copies[4].wait()


def late_kernel(
    shift_ref, own_ref, behind_ref, mask_ref, frames_ref, rows_ref, columns_ref, embedded_1_ref, heads_1_ref,
    w_qkv_ref, w_out_ref, w_head_ref,
    embedded_ref, qkv_ref, probs_ref, seen_ref, one_hot_ref, head_normed_ref, scale_ref, predicted_ref,
    chosen_ref, normed_ref, heads_ref, residual_ref, narrow_ref,
):
    one_hot_ref[:SLOTS] = slot_one_hot(shift_ref, own_ref, 0, 0)
    one_hot_ref[SLOTS:] = slot_one_hot(shift_ref, behind_ref, 1, 0)
    own_hot = one_hot_ref[:SLOTS]
    behind_hot = one_hot_ref[SLOTS:]
    chosen_ref[...] = dot(own_hot, own_ref[:, :D], TN_DIMS) + dot(behind_hot, behind_ref[:, :D], TN_DIMS)
    seen_ref[...] = dot(one_hot_ref[...], jnp.ones((2 * SLOTS, 128), BF), TN_DIMS)
    embed(0, mask_ref, frames_ref, rows_ref, columns_ref, chosen_ref, seen_ref, embedded_ref, normed_ref)
    for at in range(3):
        project(at, normed_ref, w_qkv_ref, qkv_ref)
    heads_ref[HALF:] = heads_1_ref[...]
    attend(qkv_ref, probs_ref, heads_ref)
    for part in range(2):
        cols = slice(part * 512, part * 512 + 512)
        attn = dot(heads_ref[...], w_out_ref[:, cols], NN_DIMS).astype(BF).astype(F32)
        residual_ref[:HALF, cols] = embedded_ref[:, cols].astype(F32) + attn[:HALF]
        residual_ref[HALF:, cols] = embedded_1_ref[:, cols].astype(F32) + attn[HALF:]
    for block in range(TOK // 16):
        rows = slice(block * 16, block * 16 + 16)
        normed, scale = normalise(residual_ref[rows])
        head_normed_ref[rows] = normed
        scale_ref[rows] = jnp.broadcast_to(scale, (16, 128))
        narrow_ref[rows] = normed.astype(BF)
    for part in range(3):
        cols = slice(part * GROUP, part * GROUP + GROUP)
        predicted_ref[:, cols] = dot(narrow_ref[...], w_head_ref[:, cols], NN_DIMS)


def backward_kernel(
    shift_ref, embedded_0_ref, qkv_0_ref, probs_0_ref, seen_0_ref, one_hot_0_ref,
    embedded_1_ref, qkv_1_ref, probs_1_ref, seen_1_ref, one_hot_1_ref,
    normed_ref, scale_ref, predicted_ref, w_qkv_ref, w_out_ref, w_head_ref,
    own_target, row_target, last_row_target, time_target, corner_target,
    own_picked_ref, behind_rows_ref, total_ref,
    target_ref, error_ref, narrow_ref, wide_ref, stream_ref, dqkv_ref,
):
    embedded_refs = (embedded_0_ref, embedded_1_ref)
    qkv_refs = (qkv_0_ref, qkv_1_ref)
    probs_refs = (probs_0_ref, probs_1_ref)
    seen_refs = (seen_0_ref, seen_1_ref)
    target_ref[1:, :4] = own_target[...]
    target_ref[:1, :4] = time_target[...]
    for frame in range(5):
        halo_ref, at_frame = (
            (corner_target, 0) if frame == 0 else (last_row_target, 0) if frame == 4 else (row_target, frame - 1)
        )
        target_ref[frame, 4] = halo_ref[at_frame, 0]
        halves = halo_ref[at_frame, 1].astype(F32)
        for at in range(2):
            half = halves[at * 8 : at * 8 + 8]
            target_ref[frame, 5 + at] = jnp.concatenate([half, half], axis=0).astype(BF)

    for block in range(TOK // 16):
        frame_pair, rest = divmod(block, 8)
        group, half = divmod(rest, 4)
        rows = slice(block * 16, block * 16 + 16)
        local = slice(rest * 16, rest * 16 + 16)
        masked = 1.0 - jnp.concatenate([seen_refs[frame_pair][local]] * 12, axis=1)
        target = jnp.concatenate(
            [
                target_ref[
                    frame_pair * 2 + half // 2 - shift_ref[0, group] + 1,
                    (half % 2) * 2 + at + ((4 - shift_ref[1, group]) & 3),
                    group * 8 : group * 8 + 8,
                ].astype(F32)
                for at in range(2)
            ],
            axis=0,
        )
        error_ref[rows] = (masked * (predicted_ref[rows] - target)).astype(BF)

    for part in range(2):
        cols = slice(part * 512, part * 512 + 512)
        wide_ref[:, cols] = dot(error_ref[...], w_head_ref[cols, :], NT_DIMS)

    for block in range(TOK // 16):
        rows = slice(block * 16, block * 16 + 16)
        scale = jnp.concatenate([scale_ref[rows]] * 8, axis=1)
        cotangent = wide_ref[rows].astype(BF).astype(F32)
        grad = normalise_back(cotangent, normed_ref[rows], scale)
        stream_ref[rows] = grad
        narrow_ref[rows] = grad.astype(BF)

    narrow_ref[...] = dot(narrow_ref[...], w_out_ref[...], NT_DIMS).astype(BF)

    for window in range(TOK // WIN):
        rows = slice(window * WIN, window * WIN + WIN)
        frame_pair, group = divmod(window, 2)
        local = slice(group * WIN, group * WIN + WIN)
        qkv_ref = qkv_refs[frame_pair]
        probs_ref = probs_refs[frame_pair]
        cols = [[slice(at * D + pair * 128, at * D + pair * 128 + 128) for at in range(3)] for pair in range(PAIRS)]
        d_probs = []
        out_heads = []
        for pair in range(PAIRS):
            out_heads.append(two_heads(narrow_ref[rows, cols[pair][0]]))
            d_probs.append(dot(qkv_ref[local, cols[pair][2]], out_heads[pair], NT_DIMS))
        for pair in range(PAIRS):
            dqkv_ref[rows, cols[pair][2]] = dot(probs_ref[group, pair], out_heads[pair], NN_DIMS).astype(BF)
        d_scores = []
        for pair in range(PAIRS):
            probs = probs_ref[group, pair].astype(F32)
            cotangent = d_probs[pair].astype(BF).astype(F32)
            mean = jnp.sum(cotangent * probs, axis=0, keepdims=True)
            d_scores.append((probs * (cotangent - mean) * 0.125).astype(BF))
        for pair in range(PAIRS):
            q_heads = two_heads(qkv_ref[local, cols[pair][0]])
            dqkv_ref[rows, cols[pair][1]] = dot(d_scores[pair], q_heads, NN_DIMS).astype(BF)
        for pair in range(PAIRS):
            d_q = own_head(dot(d_scores[pair], qkv_ref[local, cols[pair][1]], TN_DIMS))
            dqkv_ref[rows, cols[pair][0]] = d_q.astype(BF)

    for part in range(2):
        cols = slice(part * 512, part * 512 + 512)
        wide_ref[:, cols] = dot(dqkv_ref[...], w_qkv_ref[cols, :], NT_DIMS)

    total = jnp.zeros((8, D), F32)
    for block in range(TOK // 16):
        frame_pair, rest = divmod(block, 8)
        rows = slice(block * 16, block * 16 + 16)
        local = slice(rest * 16, rest * 16 + 16)
        normed, scale = normalise(embedded_refs[frame_pair][local].astype(F32))
        cotangent = wide_ref[rows].astype(BF).astype(F32)
        grad = stream_ref[rows] + normalise_back(cotangent, normed, scale)
        narrow_ref[rows] = grad.astype(BF)
        part = (1.0 - jnp.concatenate([seen_refs[frame_pair][local]] * 8, axis=1)) * grad
        total = total + part[:8] + part[8:]
    total = jnp.sum(total, axis=0, keepdims=True)
    total_ref[...] = jnp.concatenate([total[:, at * 128 : at * 128 + 128] for at in range(8)], axis=0)
    behind_rows_ref[...] = jnp.where(
        shift_ref[0, 1] == 1, narrow_ref[WIN : WIN + 32].astype(F32), narrow_ref[:32].astype(F32)
    ).astype(BF)
    own_picked = dot(one_hot_0_ref[:SLOTS], narrow_ref[:HALF], NN_DIMS)
    own_picked_ref[...] = (own_picked + dot(one_hot_1_ref[...], narrow_ref[HALF:], NN_DIMS)).astype(BF)


def give_kernel(
    shift_ref, own_ref, picked_ref, next_ref, total_ref, turned_1_ref, turned_2_ref, turned_3_ref, sent_ref
):
    place = own_ref[:, D : D + 128].astype(F32).astype(jnp.int32)
    row = (place >> 4) & 3
    column = place & 15
    slot = lax.broadcasted_iota(jnp.int32, (SLOTS, 128), 0) & 7
    lane = lax.broadcasted_iota(jnp.int32, (SLOTS, 128), 1)
    late = jnp.where(column < 8, shift_ref[0:1], shift_ref[1:2])
    row = row + jnp.where(column < 8, shift_ref[2:3], shift_ref[3:4]) + jnp.where(slot >= 4, 4, 0)
    inside = (place >= 192) & (late == 1) & (row >= 0) & (row < 4)
    token = jnp.where(inside, row * 8 + (column & 7), -1)
    one_hot = jnp.where(token == lane, 1.0, 0.0).astype(BF)
    rows = jnp.concatenate([next_ref[...], jnp.zeros((SLOTS - 32, D), BF)], axis=0)
    picked = picked_ref[...].astype(F32) + dot(one_hot, rows, NN_DIMS)
    sent_ref[:, :, :D] = picked.reshape(16, 8, D).astype(BF)
    total = (total_ref[...] + turned_2_ref[...]) + (turned_1_ref[...] + turned_3_ref[...])
    high = total.astype(BF)
    low = (total - high.astype(F32)).astype(BF)
    for peer in range(16):
        sent_ref[peer, :, D : D + 128] = high
        sent_ref[peer, :, D + 128 :] = low


def pack_kernel(
    place_hbm, shift_hbm, mask_hbm, rows_hbm, pixel_hbm,
    packed_ref, shift_rows_ref, mask_ref, pixel_ref,
    place_ref, shift_ref, rows_ref, sems,
):
    copies = [
        pltpu.make_async_copy(source, target, sems.at[at])
        for at, (source, target) in enumerate(
            [
                (rows_hbm, rows_ref),
                (place_hbm, place_ref),
                (shift_hbm, shift_ref),
                (mask_hbm, mask_ref),
                (pixel_hbm, pixel_ref),
            ]
        )
    ]
    for copy in copies:
        copy.start()
    copies[1].wait()
    slot = lax.broadcasted_iota(jnp.int32, (8, 128), 0)
    peers = rows_ref.shape[0]
    for peer in range(peers):
        places = jnp.zeros((8, 128), jnp.int32)
        for at in range(8):
            source = peer if at < 4 else (peer + 1) % peers
            places = jnp.where(slot == at, place_ref[at % 4, source], places)
        packed_ref[peer, :, D:] = places.astype(F32).astype(BF)
    copies[2].wait()
    shifts = jnp.zeros((8, 128), jnp.int32)
    for group in range(2):
        shifts = jnp.where(slot == group, shift_ref[0, group], shifts)
        shifts = jnp.where(slot == 2 + group, -((4 - shift_ref[1, group]) & 3), shifts)
    shift_rows_ref[...] = shifts
    copies[0].wait()
    rows = rows_ref[...].astype(F32)
    after = jnp.concatenate([rows[1:], rows[:1]], axis=0)
    packed_ref[:, :, :D] = jnp.concatenate([rows, after], axis=1).astype(BF)
    copies[3].wait()
    copies[4].wait()


def sinusoid(coordinate, channel_count):
    half_count = channel_count // 2
    lane = lax.broadcasted_iota(jnp.int32, (coordinate.shape[0], channel_count), 1)
    channel = jnp.where(lane < half_count, lane, lane - half_count).astype(F32)
    angles = coordinate.astype(F32) * jnp.exp(-math.log(10000.0) * channel / half_count)
    return jnp.where(lane < half_count, jnp.sin(angles), jnp.cos(angles))


def grid_coordinates(start, offsets_ref, first, total, channel_count):
    row = lax.broadcasted_iota(jnp.int32, (8, 128), 0)
    offset = jnp.where(row < 4, offsets_ref[first : first + 1], offsets_ref[first + 1 : first + 2])
    coordinate = start + (row & 3) - offset
    coordinate = jnp.where(coordinate < 0, coordinate + total, coordinate)
    coordinate = jnp.where(coordinate >= total, coordinate - total, coordinate)
    return jnp.concatenate([coordinate] * (channel_count // 128), axis=1)


def target_kernel(
    totals, shift_rows_ref, pixel_ref, own_ref, row_ref, last_row_ref, time_ref, frames_ref, rows_ref, columns_ref
):
    frames = grid_coordinates(lax.axis_index(TM) * 4, shift_rows_ref, 0, totals[0], 256)
    rows = grid_coordinates(lax.axis_index(ROW) * 4, shift_rows_ref, 2, totals[1], 384)
    frames_ref[...] = sinusoid(frames, 256)
    rows_ref[...] = sinusoid(rows, 384)
    columns_ref[...] = sinusoid(lax.broadcasted_iota(jnp.int32, (16, 384), 0), 384)
    second = jnp.concatenate([shift_rows_ref[2:3]] * (GROUP // 128), axis=1) == -1
    for frame in range(4):
        halo_ref, at_frame = (last_row_ref, 0) if frame == 3 else (row_ref, frame)
        for part in range(3):
            cols = slice(part * GROUP, part * GROUP + GROUP)
            picked = []
            for row in range(4):
                raw = pixel_ref[frame, row, :, cols].astype(F32)
                center = raw - lane_mean(raw)
                spread = jnp.sqrt(jnp.sum(center * center, axis=-1, keepdims=True) * (1.0 / (GROUP - 1)))
                target = center * (1.0 / (spread + 1e-06))
                own_ref[frame, row, :, cols] = target.astype(BF)
                if frame == 3:
                    time_ref[0, row, :, cols] = target.astype(BF)
                if row == 0:
                    halo_ref[at_frame, 0, :, cols] = target.astype(BF)
                if row in (1, 2):
                    picked.append(jnp.where(second, target[8:], target[:8]))
            halo_ref[at_frame, 1, :, cols] = jnp.concatenate(picked, axis=0).astype(BF)


def unpack_kernel(scale, back_ref, rows_ref, total_ref):
    rows = back_ref[:, :4, :D].astype(F32)
    before = back_ref[:, 4:, :D].astype(F32)
    before = jnp.concatenate([before[-1:], before[:-1]], axis=0)
    rows_ref[...] = (rows + before).astype(BF)
    sums = jnp.sum(back_ref[:, :, D:].astype(F32), axis=0)
    total_ref[...] = (sums[:, :128] + sums[:, 128:]) * scale


def shapes(*items):
    return [jax.ShapeDtypeStruct(dims, kind) for dims, kind in items]


def call(kernel, outputs, scratch, in_specs, limit):
    return pl.pallas_call(
        kernel,
        in_specs=in_specs,
        out_specs=[pl.BlockSpec(memory_space=VMEM)] * len(outputs),
        out_shape=shapes(*outputs),
        scratch_shapes=scratch,
        compiler_params=pltpu.CompilerParams(vmem_limit_bytes=limit << 20),
    )


def in_space(space, count):
    return [pl.BlockSpec(memory_space=space)] * count


def half_outputs(slots):
    return [
        ((HALF, D), BF),
        ((HALF, 3 * D), BF),
        ((HALF // WIN, PAIRS, WIN, 128), BF),
        ((HALF, 128), F32),
        ((slots, HALF), BF),
    ]


def pack_part(*operands):
    outputs = [((16, 8, D + 128), BF), ((8, 128), jnp.int32), ((8, 128), BF), ((4, 4, 16, PIX), BF)]
    scratch = [
        pltpu.SMEM((4, 16), jnp.int32),
        pltpu.SMEM((2, 2), jnp.int32),
        pltpu.VMEM((16, 4, D), BF),
        pltpu.SemaphoreType.DMA((5,)),
    ]
    return call(pack_kernel, outputs, scratch, in_space(HBM, 5), 8)(*operands)


def target_part(totals, *operands):
    outputs = [((frames, rows, 16, PIX), BF) for frames, rows in ((4, 4), (3, 2), (1, 2), (1, 4))]
    outputs += [((8, 256), F32), ((8, 384), F32), ((16, 384), F32)]
    kernel = functools.partial(target_kernel, totals)
    return call(kernel, outputs, [], in_space(VMEM, 2), 8)(*operands)


def early_part(*operands):
    outputs = half_outputs(SLOTS) + [((HALF, D), BF), ((D, 3 * D), BF), ((D, D), BF), ((D, PIX), BF)]
    scratch = [pltpu.VMEM((HALF, D), F32), pltpu.VMEM((HALF, D), BF), pltpu.SemaphoreType.DMA((5,))]
    return call(early_kernel, outputs, scratch, in_space(VMEM, 6) + in_space(HBM, 3), 20)(*operands)


def late_part(*operands):
    outputs = half_outputs(2 * SLOTS) + [((TOK, D), F32), ((TOK, 128), F32), ((TOK, PIX), F32)]
    scratch = [
        pltpu.VMEM((HALF, D), F32),
        pltpu.VMEM((HALF, D), BF),
        pltpu.VMEM((TOK, D), BF),
        pltpu.VMEM((TOK, D), F32),
        pltpu.VMEM((TOK, D), BF),
    ]
    return call(late_kernel, outputs, scratch, in_space(VMEM, 12), 26)(*operands)


def backward_part(*operands):
    outputs = [((SLOTS, D), BF), ((32, D), BF), ((8, 128), F32)]
    scratch = [
        pltpu.VMEM((5, 7, 16, PIX), BF),
        pltpu.VMEM((TOK, PIX), BF),
        pltpu.VMEM((TOK, D), BF),
        pltpu.VMEM((TOK, D), F32),
        pltpu.VMEM((TOK, D), F32),
        pltpu.VMEM((TOK, 3 * D), BF),
    ]
    return call(backward_kernel, outputs, scratch, in_space(SMEM, 1) + in_space(VMEM, 21), 34)(*operands)


def move(value, axis, steps):
    count = lax.axis_size(axis)
    return lax.ppermute(value, axis, [(at, (at + steps) % count) for at in range(count)])


def per_device(visible, slot_pos, window_shift, mask_token, w_qkv, w_out, w_head, pixels):
    frame_count, row_count = pixels.shape[:2]
    peers, slots = slot_pos.shape[2:]
    hold = functools.partial(pltpu.with_memory_space_constraint, memory_space=HBM)
    packed, shift_rows, mask_rows, near_pixels = pack_part(
        hold(slot_pos.reshape(peers, slots).T),
        hold(window_shift),
        hold(mask_token.reshape(8, 128)),
        hold(visible.reshape(peers, slots, D)),
        hold(pixels),
    )
    own = lax.all_to_all(packed, ROW, split_axis=0, concat_axis=0, tiled=True).reshape(SLOTS, D + 128)
    behind = move(own, TM, 1)
    frame_total = frame_count * lax.axis_size(TM)
    row_total = row_count * lax.axis_size(ROW)
    own_target, row_target, last_row_target, time_target, *positions = target_part(
        (frame_total, row_total), shift_rows, near_pixels
    )
    last_row_target = move(last_row_target, ROW, -1)
    row_target = move(row_target, ROW, -1)
    time_target = move(time_target, TM, 1)
    corner_target = move(last_row_target, TM, 1)

    tables = (mask_rows, *positions)
    *half_1, heads_1, w_qkv, w_out, w_head = early_part(
        shift_rows, own, *tables, hold(w_qkv), hold(w_out), hold(w_head)
    )
    *half_0, head_normed, head_scale, predicted = late_part(
        shift_rows, own, behind, *tables, half_1[0], heads_1, w_qkv, w_out, w_head
    )
    own_picked, behind_rows, local_total = backward_part(
        window_shift, *half_0, *half_1, head_normed, head_scale, predicted, w_qkv, w_out, w_head,
        own_target, row_target, last_row_target, time_target, corner_target,
    )
    other = move(local_total, "tm_1", 1)
    from_next = move(behind_rows, TM, -1)
    local_total = local_total + other
    turned = []
    for step in (1, 2, 3):
        turned.append(move(local_total, "tm_0", step))
    give = call(give_kernel, [((peers, 8, D + 256), BF)], [], in_space(VMEM, 8), 8)
    (sent,) = give(shift_rows, own, own_picked, from_next, local_total, *turned)
    back = lax.all_to_all(sent, ROW, split_axis=0, concat_axis=0, tiled=True)
    grad_scale = (frame_total * row_total * pixels.shape[2]) ** (-0.5)
    outputs = [((peers, slots, D), BF), ((8, 128), F32)]
    unpack = call(functools.partial(unpack_kernel, grad_scale), outputs, [], in_space(VMEM, 1), 8)
    d_visible, d_mask = unpack(back)
    return (d_visible.reshape(visible.shape), d_mask.reshape(D))


def solution(mesh):
    torus = Mesh(mesh.devices.reshape(4, 2, 4, 4), ALL)
    return jax.shard_map(
        per_device,
        mesh=torus,
        in_specs=(
            P(TM, ROW, None, None, None),
            P(TM, ROW, None, None),
            P(),
            P(),
            P(),
            P(),
            P(),
            P(TM, ROW, None, None),
        ),
        out_specs=(P(TM, ROW, None, None, None), P()),
        check_vma=False,
    )
```

```python
import functools
import math

import jax
import jax.numpy as jnp
from jax import lax
from jax.experimental import pallas as pl
from jax.experimental.pallas import tpu as pltpu
from jax.sharding import Mesh
from jax.sharding import PartitionSpec as P

WT = 2
WH = 4
WW = 8
D = 1024
PIX = 1536
GROUP = PIX // 3
TOK = 256
HALF = TOK // 2
WIN = WT * WH * WW
PAIRS = D // 128
SLOTS = 128
TM = ("tm_0", "tm_1")
ROW = ("row_0", "row_1")
ALL = TM + ROW
BF = jnp.bfloat16
F32 = jnp.float32
NT_DIMS = (((1,), (1,)), ((), ()))
TN_DIMS = (((0,), (0,)), ((), ()))
NN_DIMS = (((1,), (0,)), ((), ()))
VMEM = pltpu.MemorySpace.VMEM
SMEM = pltpu.MemorySpace.SMEM
HBM = pltpu.MemorySpace.HBM


def dot(a, b, dims):
    return lax.dot_general(a, b, dims, preferred_element_type=F32)


def lane_mean(values):
    return jnp.sum(values, axis=-1, keepdims=True) * (1.0 / values.shape[-1])


def normalise(values):
    center = values - lane_mean(values)
    scale = lax.rsqrt(lane_mean(center * center) + 1e-05)
    return center * scale, scale


def normalise_back(cotangent, normed, scale):
    return scale * (cotangent - lane_mean(cotangent) - normed * lane_mean(cotangent * normed))


def two_heads(rows):
    first = lax.broadcasted_iota(jnp.int32, rows.shape, 1) < 64
    zero = jnp.zeros_like(rows)
    return jnp.concatenate([jnp.where(first, rows, zero), jnp.where(first, zero, rows)], axis=0)


def own_head(rows):
    first = lax.broadcasted_iota(jnp.int32, (WIN, 128), 1) < 64
    return jnp.where(first, rows[:WIN], rows[WIN:])


def slot_one_hot(shift_ref, rows_ref, behind, frame_pair):
    place = rows_ref[:, D : D + 128].astype(F32).astype(jnp.int32)
    frame = place >> 6
    row = (place >> 4) & 3
    column = place & 15
    group = column >> 3
    slot = lax.broadcasted_iota(jnp.int32, (SLOTS, 128), 0) & 7
    lane = lax.broadcasted_iota(jnp.int32, (SLOTS, 128), 1)
    frame = frame + jnp.where(group == 0, shift_ref[0:1], shift_ref[1:2]) - 4 * behind
    row = row + jnp.where(group == 0, shift_ref[2:3], shift_ref[3:4]) + jnp.where(slot >= 4, 4, 0)
    inside = (place >= 0) & ((frame >> 1) == frame_pair) & (row >= 0) & (row < 4)
    token = group * 64 + ((frame & 1) * 32) + row * 8 + (column & 7)
    token = jnp.where(inside, token, -1)
    return jnp.where(token == lane, 1.0, 0.0).astype(BF)


def embed(frame_pair, mask_ref, frames_ref, rows_ref, columns_ref, chosen_ref, seen_ref, embedded_ref, normed_ref):
    mask = mask_ref[...].astype(F32)
    mask = jnp.concatenate([mask[at : at + 1] for at in range(8)], axis=1)
    for block in range(HALF // 16):
        group, half = divmod(block, 4)
        at_frame = group * 4 + frame_pair * 2 + half // 2
        rows = slice(block * 16, block * 16 + 16)
        start = jnp.where(jnp.concatenate([seen_ref[rows]] * 8, axis=1) > 0, chosen_ref[rows], mask)
        position = []
        for at in range(2):
            at_row = group * 4 + (half % 2) * 2 + at
            position.append(
                jnp.concatenate(
                    [
                        jnp.broadcast_to(frames_ref[at_frame : at_frame + 1], (8, 256)),
                        jnp.broadcast_to(rows_ref[at_row : at_row + 1], (8, 384)),
                        columns_ref[group * 8 : group * 8 + 8],
                    ],
                    axis=1,
                )
            )
        embedded = (start + jnp.concatenate(position, axis=0)).astype(BF)
        embedded_ref[rows] = embedded
        normed_ref[rows] = normalise(embedded.astype(F32))[0].astype(BF)


def project(at, normed_ref, w_qkv_ref, qkv_ref):
    for part in range(2):
        cols = slice(at * D + part * 512, at * D + part * 512 + 512)
        qkv_ref[:, cols] = dot(normed_ref[...], w_qkv_ref[:, cols], NN_DIMS).astype(BF)


def attend(qkv_ref, probs_ref, heads_ref):
    units = [(window, pair) for window in range(HALF // WIN) for pair in range(PAIRS)]
    rows = [slice(window * WIN, window * WIN + WIN) for window, pair in units]
    scores = []
    for at, (window, pair) in enumerate(units):
        q = qkv_ref[rows[at], pair * 128 : pair * 128 + 128]
        k = qkv_ref[rows[at], D + pair * 128 : D + pair * 128 + 128]
        scores.append(dot(k, two_heads(q), NT_DIMS) * 0.125)
    probs = []
    for at, unit in enumerate(units):
        weights = jnp.exp(scores[at] - jnp.max(scores[at], axis=0, keepdims=True))
        probs.append((weights * (1.0 / jnp.sum(weights, axis=0, keepdims=True))).astype(BF))
        probs_ref[unit] = probs[at]
    for at, (window, pair) in enumerate(units):
        v = qkv_ref[rows[at], 2 * D + pair * 128 : 2 * D + pair * 128 + 128]
        heads_ref[rows[at], pair * 128 : pair * 128 + 128] = own_head(dot(probs[at], v, TN_DIMS)).astype(BF)


def early_kernel(
    shift_ref, own_ref, mask_ref, frames_ref, rows_ref, columns_ref, w_qkv_hbm, w_out_hbm, w_head_hbm,
    embedded_ref, qkv_ref, probs_ref, seen_ref, one_hot_ref, heads_ref, w_qkv_ref, w_out_ref, w_head_ref,
    chosen_ref, normed_ref, sems,
):
    copies = [
        pltpu.make_async_copy(
            w_qkv_hbm.at[:, pl.ds(at * D, D)], w_qkv_ref.at[:, pl.ds(at * D, D)], sems.at[at]
        )
        for at in range(3)
    ]
    copies.append(pltpu.make_async_copy(w_out_hbm, w_out_ref, sems.at[3]))
    copies.append(pltpu.make_async_copy(w_head_hbm, w_head_ref, sems.at[4]))
    for copy in copies:
        copy.start()
    one_hot_ref[...] = slot_one_hot(shift_ref, own_ref, 0, 1)
    chosen_ref[...] = dot(one_hot_ref[...], own_ref[:, :D], TN_DIMS)
    seen_ref[...] = dot(one_hot_ref[...], jnp.ones((SLOTS, 128), BF), TN_DIMS)
    embed(1, mask_ref, frames_ref, rows_ref, columns_ref, chosen_ref, seen_ref, embedded_ref, normed_ref)
    for at in range(3):
        copies[at].wait()
        project(at, normed_ref, w_qkv_ref, qkv_ref)
    attend(qkv_ref, probs_ref, heads_ref)
    copies[3].wait()
    copies[4].wait()


def late_kernel(
    shift_ref, own_ref, behind_ref, mask_ref, frames_ref, rows_ref, columns_ref, embedded_1_ref, heads_1_ref,
    w_qkv_ref, w_out_ref, w_head_ref,
    embedded_ref, qkv_ref, probs_ref, seen_ref, one_hot_ref, head_normed_ref, scale_ref, predicted_ref,
    chosen_ref, normed_ref, heads_ref, residual_ref, narrow_ref,
):
    one_hot_ref[:SLOTS] = slot_one_hot(shift_ref, own_ref, 0, 0)
    one_hot_ref[SLOTS:] = slot_one_hot(shift_ref, behind_ref, 1, 0)
    own_hot = one_hot_ref[:SLOTS]
    behind_hot = one_hot_ref[SLOTS:]
    chosen_ref[...] = dot(own_hot, own_ref[:, :D], TN_DIMS) + dot(behind_hot, behind_ref[:, :D], TN_DIMS)
    seen_ref[...] = dot(one_hot_ref[...], jnp.ones((2 * SLOTS, 128), BF), TN_DIMS)
    embed(0, mask_ref, frames_ref, rows_ref, columns_ref, chosen_ref, seen_ref, embedded_ref, normed_ref)
    for at in range(3):
        project(at, normed_ref, w_qkv_ref, qkv_ref)
    heads_ref[HALF:] = heads_1_ref[...]
    attend(qkv_ref, probs_ref, heads_ref)
    for part in range(2):
        cols = slice(part * 512, part * 512 + 512)
        attn = dot(heads_ref[...], w_out_ref[:, cols], NN_DIMS).astype(BF).astype(F32)
        residual_ref[:HALF, cols] = embedded_ref[:, cols].astype(F32) + attn[:HALF]
        residual_ref[HALF:, cols] = embedded_1_ref[:, cols].astype(F32) + attn[HALF:]
    for block in range(TOK // 16):
        rows = slice(block * 16, block * 16 + 16)
        normed, scale = normalise(residual_ref[rows])
        head_normed_ref[rows] = normed
        scale_ref[rows] = jnp.broadcast_to(scale, (16, 128))
        narrow_ref[rows] = normed.astype(BF)
    for part in range(3):
        cols = slice(part * GROUP, part * GROUP + GROUP)
        predicted_ref[:, cols] = dot(narrow_ref[...], w_head_ref[:, cols], NN_DIMS)


def backward_kernel(
    shift_ref, embedded_0_ref, qkv_0_ref, probs_0_ref, seen_0_ref, one_hot_0_ref,
    embedded_1_ref, qkv_1_ref, probs_1_ref, seen_1_ref, one_hot_1_ref,
    normed_ref, scale_ref, predicted_ref, w_qkv_ref, w_out_ref, w_head_ref,
    own_target, row_target, last_row_target, time_target, corner_target,
    own_picked_ref, behind_rows_ref, total_ref,
    target_ref, error_ref, narrow_ref, wide_ref, stream_ref, dqkv_ref,
):
    embedded_refs = (embedded_0_ref, embedded_1_ref)
    qkv_refs = (qkv_0_ref, qkv_1_ref)
    probs_refs = (probs_0_ref, probs_1_ref)
    seen_refs = (seen_0_ref, seen_1_ref)
    target_ref[1:, :4] = own_target[...]
    target_ref[:1, :4] = time_target[...]
    for frame in range(5):
        halo_ref, at_frame = (
            (corner_target, 0) if frame == 0 else (last_row_target, 0) if frame == 4 else (row_target, frame - 1)
        )
        target_ref[frame, 4] = halo_ref[at_frame, 0]
        halves = halo_ref[at_frame, 1].astype(F32)
        for at in range(2):
            half = halves[at * 8 : at * 8 + 8]
            target_ref[frame, 5 + at] = jnp.concatenate([half, half], axis=0).astype(BF)

    for block in range(TOK // 16):
        frame_pair, rest = divmod(block, 8)
        group, half = divmod(rest, 4)
        rows = slice(block * 16, block * 16 + 16)
        local = slice(rest * 16, rest * 16 + 16)
        masked = 1.0 - jnp.concatenate([seen_refs[frame_pair][local]] * 12, axis=1)
        target = jnp.concatenate(
            [
                target_ref[
                    frame_pair * 2 + half // 2 - shift_ref[0, group] + 1,
                    (half % 2) * 2 + at + ((4 - shift_ref[1, group]) & 3),
                    group * 8 : group * 8 + 8,
                ].astype(F32)
                for at in range(2)
            ],
            axis=0,
        )
        error_ref[rows] = (masked * (predicted_ref[rows] - target)).astype(BF)

    for part in range(2):
        cols = slice(part * 512, part * 512 + 512)
        wide_ref[:, cols] = dot(error_ref[...], w_head_ref[cols, :], NT_DIMS)

    for block in range(TOK // 16):
        rows = slice(block * 16, block * 16 + 16)
        scale = jnp.concatenate([scale_ref[rows]] * 8, axis=1)
        cotangent = wide_ref[rows].astype(BF).astype(F32)
        grad = normalise_back(cotangent, normed_ref[rows], scale)
        stream_ref[rows] = grad
        narrow_ref[rows] = grad.astype(BF)

    narrow_ref[...] = dot(narrow_ref[...], w_out_ref[...], NT_DIMS).astype(BF)

    for frame_pair in range(2):
        qkv_ref = qkv_refs[frame_pair]
        probs_ref = probs_refs[frame_pair]
        units = [(group, pair) for group in range(2) for pair in range(PAIRS)]
        local = [slice(group * WIN, group * WIN + WIN) for group, pair in units]
        rows = [slice((frame_pair * 2 + group) * WIN, (frame_pair * 2 + group + 1) * WIN) for group, pair in units]
        cols = [[slice(at * D + pair * 128, at * D + pair * 128 + 128) for at in range(3)] for group, pair in units]
        d_probs = []
        out_heads = []
        for at, unit in enumerate(units):
            out_heads.append(two_heads(narrow_ref[rows[at], cols[at][0]]))
            d_probs.append(dot(qkv_ref[local[at], cols[at][2]], out_heads[at], NT_DIMS))
        for at, unit in enumerate(units):
            dqkv_ref[rows[at], cols[at][2]] = dot(probs_ref[unit], out_heads[at], NN_DIMS).astype(BF)
        d_scores = []
        for at, unit in enumerate(units):
            probs = probs_ref[unit].astype(F32)
            cotangent = d_probs[at].astype(BF).astype(F32)
            mean = jnp.sum(cotangent * probs, axis=0, keepdims=True)
            d_scores.append((probs * (cotangent - mean) * 0.125).astype(BF))
        for at, unit in enumerate(units):
            q_heads = two_heads(qkv_ref[local[at], cols[at][0]])
            dqkv_ref[rows[at], cols[at][1]] = dot(d_scores[at], q_heads, NN_DIMS).astype(BF)
        for at, unit in enumerate(units):
            d_q = own_head(dot(d_scores[at], qkv_ref[local[at], cols[at][1]], TN_DIMS))
            dqkv_ref[rows[at], cols[at][0]] = d_q.astype(BF)

    for part in range(2):
        cols = slice(part * 512, part * 512 + 512)
        wide_ref[:, cols] = dot(dqkv_ref[...], w_qkv_ref[cols, :], NT_DIMS)

    total = jnp.zeros((8, D), F32)
    for block in range(TOK // 16):
        frame_pair, rest = divmod(block, 8)
        rows = slice(block * 16, block * 16 + 16)
        local = slice(rest * 16, rest * 16 + 16)
        normed, scale = normalise(embedded_refs[frame_pair][local].astype(F32))
        cotangent = wide_ref[rows].astype(BF).astype(F32)
        grad = stream_ref[rows] + normalise_back(cotangent, normed, scale)
        narrow_ref[rows] = grad.astype(BF)
        part = (1.0 - jnp.concatenate([seen_refs[frame_pair][local]] * 8, axis=1)) * grad
        total = total + part[:8] + part[8:]
    total = jnp.sum(total, axis=0, keepdims=True)
    total_ref[...] = jnp.concatenate([total[:, at * 128 : at * 128 + 128] for at in range(8)], axis=0)
    behind_rows_ref[...] = jnp.where(
        shift_ref[0, 1] == 1, narrow_ref[WIN : WIN + 32].astype(F32), narrow_ref[:32].astype(F32)
    ).astype(BF)
    own_picked = dot(one_hot_0_ref[:SLOTS], narrow_ref[:HALF], NN_DIMS)
    own_picked_ref[...] = (own_picked + dot(one_hot_1_ref[...], narrow_ref[HALF:], NN_DIMS)).astype(BF)


def give_kernel(
    shift_ref, own_ref, picked_ref, next_ref, total_ref, turned_1_ref, turned_2_ref, turned_3_ref, sent_ref
):
    place = own_ref[:, D : D + 128].astype(F32).astype(jnp.int32)
    row = (place >> 4) & 3
    column = place & 15
    slot = lax.broadcasted_iota(jnp.int32, (SLOTS, 128), 0) & 7
    lane = lax.broadcasted_iota(jnp.int32, (SLOTS, 128), 1)
    late = jnp.where(column < 8, shift_ref[0:1], shift_ref[1:2])
    row = row + jnp.where(column < 8, shift_ref[2:3], shift_ref[3:4]) + jnp.where(slot >= 4, 4, 0)
    inside = (place >= 192) & (late == 1) & (row >= 0) & (row < 4)
    token = jnp.where(inside, row * 8 + (column & 7), -1)
    one_hot = jnp.where(token == lane, 1.0, 0.0).astype(BF)
    rows = jnp.concatenate([next_ref[...], jnp.zeros((SLOTS - 32, D), BF)], axis=0)
    picked = picked_ref[...].astype(F32) + dot(one_hot, rows, NN_DIMS)
    sent_ref[:, :, :D] = picked.reshape(16, 8, D).astype(BF)
    total = (total_ref[...] + turned_2_ref[...]) + (turned_1_ref[...] + turned_3_ref[...])
    high = total.astype(BF)
    low = (total - high.astype(F32)).astype(BF)
    for peer in range(16):
        sent_ref[peer, :, D : D + 128] = high
        sent_ref[peer, :, D + 128 :] = low


def pack_kernel(
    place_hbm, shift_hbm, mask_hbm, rows_hbm,
    packed_ref, shift_rows_ref, mask_ref,
    place_ref, shift_ref, rows_ref, sems,
):
    copies = [
        pltpu.make_async_copy(source, target, sems.at[at])
        for at, (source, target) in enumerate(
            [
                (rows_hbm, rows_ref),
                (place_hbm, place_ref),
                (shift_hbm, shift_ref),
                (mask_hbm, mask_ref),
            ]
        )
    ]
    for copy in copies:
        copy.start()
    copies[1].wait()
    slot = lax.broadcasted_iota(jnp.int32, (8, 128), 0)
    peers = rows_ref.shape[0]
    for peer in range(peers):
        places = jnp.zeros((8, 128), jnp.int32)
        for at in range(8):
            source = peer if at < 4 else (peer + 1) % peers
            places = jnp.where(slot == at, place_ref[at % 4, source], places)
        packed_ref[peer, :, D:] = places.astype(F32).astype(BF)
    copies[2].wait()
    shifts = jnp.zeros((8, 128), jnp.int32)
    for group in range(2):
        shifts = jnp.where(slot == group, shift_ref[0, group], shifts)
        shifts = jnp.where(slot == 2 + group, -((4 - shift_ref[1, group]) & 3), shifts)
    shift_rows_ref[...] = shifts
    copies[0].wait()
    rows = rows_ref[...].astype(F32)
    after = jnp.concatenate([rows[1:], rows[:1]], axis=0)
    packed_ref[:, :, :D] = jnp.concatenate([rows, after], axis=1).astype(BF)
    copies[3].wait()


def sinusoid(coordinate, channel_count):
    half_count = channel_count // 2
    lane = lax.broadcasted_iota(jnp.int32, (coordinate.shape[0], channel_count), 1)
    channel = jnp.where(lane < half_count, lane, lane - half_count).astype(F32)
    angles = coordinate.astype(F32) * jnp.exp(-math.log(10000.0) * channel / half_count)
    return jnp.where(lane < half_count, jnp.sin(angles), jnp.cos(angles))


def grid_coordinates(start, offsets_ref, first, total, channel_count):
    row = lax.broadcasted_iota(jnp.int32, (8, 128), 0)
    offset = jnp.where(row < 4, offsets_ref[first : first + 1], offsets_ref[first + 1 : first + 2])
    coordinate = start + (row & 3) - offset
    coordinate = jnp.where(coordinate < 0, coordinate + total, coordinate)
    coordinate = jnp.where(coordinate >= total, coordinate - total, coordinate)
    return jnp.concatenate([coordinate] * (channel_count // 128), axis=1)


def target_kernel(
    totals, shift_rows_ref, pixel_hbm, own_ref, row_ref, last_row_ref, time_ref, frames_ref, rows_ref, columns_ref,
    pixel_ref, sems,
):
    copies = [pltpu.make_async_copy(pixel_hbm.at[at], pixel_ref.at[at], sems.at[at]) for at in range(4)]
    for copy in copies:
        copy.start()
    frames = grid_coordinates(lax.axis_index(TM) * 4, shift_rows_ref, 0, totals[0], 256)
    rows = grid_coordinates(lax.axis_index(ROW) * 4, shift_rows_ref, 2, totals[1], 384)
    frames_ref[...] = sinusoid(frames, 256)
    rows_ref[...] = sinusoid(rows, 384)
    columns_ref[...] = sinusoid(lax.broadcasted_iota(jnp.int32, (16, 384), 0), 384)
    second = jnp.concatenate([shift_rows_ref[2:3]] * (GROUP // 128), axis=1) == -1
    for frame in range(4):
        copies[frame].wait()
        halo_ref, at_frame = (last_row_ref, 0) if frame == 3 else (row_ref, frame)
        for part in range(3):
            cols = slice(part * GROUP, part * GROUP + GROUP)
            picked = []
            for row in range(4):
                raw = pixel_ref[frame, row, :, cols].astype(F32)
                center = raw - lane_mean(raw)
                spread = jnp.sqrt(jnp.sum(center * center, axis=-1, keepdims=True) * (1.0 / (GROUP - 1)))
                target = center * (1.0 / (spread + 1e-06))
                own_ref[frame, row, :, cols] = target.astype(BF)
                if frame == 3:
                    time_ref[0, row, :, cols] = target.astype(BF)
                if row == 0:
                    halo_ref[at_frame, 0, :, cols] = target.astype(BF)
                if row in (1, 2):
                    picked.append(jnp.where(second, target[8:], target[:8]))
            halo_ref[at_frame, 1, :, cols] = jnp.concatenate(picked, axis=0).astype(BF)


def unpack_kernel(scale, back_ref, rows_ref, total_ref):
    rows = back_ref[:, :4, :D].astype(F32)
    before = back_ref[:, 4:, :D].astype(F32)
    before = jnp.concatenate([before[-1:], before[:-1]], axis=0)
    rows_ref[...] = (rows + before).astype(BF)
    sums = jnp.sum(back_ref[:, :, D:].astype(F32), axis=0)
    total_ref[...] = (sums[:, :128] + sums[:, 128:]) * scale


def shapes(*items):
    return [jax.ShapeDtypeStruct(dims, kind) for dims, kind in items]


def call(kernel, outputs, scratch, in_specs, limit):
    return pl.pallas_call(
        kernel,
        in_specs=in_specs,
        out_specs=[pl.BlockSpec(memory_space=VMEM)] * len(outputs),
        out_shape=shapes(*outputs),
        scratch_shapes=scratch,
        compiler_params=pltpu.CompilerParams(vmem_limit_bytes=limit << 20),
    )


def in_space(space, count):
    return [pl.BlockSpec(memory_space=space)] * count


def half_outputs(slots):
    return [
        ((HALF, D), BF),
        ((HALF, 3 * D), BF),
        ((HALF // WIN, PAIRS, WIN, 128), BF),
        ((HALF, 128), F32),
        ((slots, HALF), BF),
    ]


def pack_part(*operands):
    outputs = [((16, 8, D + 128), BF), ((8, 128), jnp.int32), ((8, 128), BF)]
    scratch = [
        pltpu.SMEM((4, 16), jnp.int32),
        pltpu.SMEM((2, 2), jnp.int32),
        pltpu.VMEM((16, 4, D), BF),
        pltpu.SemaphoreType.DMA((4,)),
    ]
    return call(pack_kernel, outputs, scratch, in_space(HBM, 4), 8)(*operands)


def target_part(totals, *operands):
    outputs = [((frames, rows, 16, PIX), BF) for frames, rows in ((4, 4), (3, 2), (1, 2), (1, 4))]
    outputs += [((8, 256), F32), ((8, 384), F32), ((16, 384), F32)]
    kernel = functools.partial(target_kernel, totals)
    scratch = [pltpu.VMEM((4, 4, 16, PIX), BF), pltpu.SemaphoreType.DMA((4,))]
    return call(kernel, outputs, scratch, in_space(VMEM, 1) + in_space(HBM, 1), 8)(*operands)


def early_part(*operands):
    outputs = half_outputs(SLOTS) + [((HALF, D), BF), ((D, 3 * D), BF), ((D, D), BF), ((D, PIX), BF)]
    scratch = [pltpu.VMEM((HALF, D), F32), pltpu.VMEM((HALF, D), BF), pltpu.SemaphoreType.DMA((5,))]
    return call(early_kernel, outputs, scratch, in_space(VMEM, 6) + in_space(HBM, 3), 20)(*operands)


def late_part(*operands):
    outputs = half_outputs(2 * SLOTS) + [((TOK, D), F32), ((TOK, 128), F32), ((TOK, PIX), F32)]
    scratch = [
        pltpu.VMEM((HALF, D), F32),
        pltpu.VMEM((HALF, D), BF),
        pltpu.VMEM((TOK, D), BF),
        pltpu.VMEM((TOK, D), F32),
        pltpu.VMEM((TOK, D), BF),
    ]
    return call(late_kernel, outputs, scratch, in_space(VMEM, 12), 26)(*operands)


def backward_part(*operands):
    outputs = [((SLOTS, D), BF), ((32, D), BF), ((8, 128), F32)]
    scratch = [
        pltpu.VMEM((5, 7, 16, PIX), BF),
        pltpu.VMEM((TOK, PIX), BF),
        pltpu.VMEM((TOK, D), BF),
        pltpu.VMEM((TOK, D), F32),
        pltpu.VMEM((TOK, D), F32),
        pltpu.VMEM((TOK, 3 * D), BF),
    ]
    return call(backward_kernel, outputs, scratch, in_space(SMEM, 1) + in_space(VMEM, 21), 34)(*operands)


def move(value, axis, steps):
    count = lax.axis_size(axis)
    return lax.ppermute(value, axis, [(at, (at + steps) % count) for at in range(count)])


def per_device(visible, slot_pos, window_shift, mask_token, w_qkv, w_out, w_head, pixels):
    frame_count, row_count = pixels.shape[:2]
    peers, slots = slot_pos.shape[2:]
    hold = functools.partial(pltpu.with_memory_space_constraint, memory_space=HBM)
    packed, shift_rows, mask_rows = pack_part(
        hold(slot_pos.reshape(peers, slots).T),
        hold(window_shift),
        hold(mask_token.reshape(8, 128)),
        hold(visible.reshape(peers, slots, D)),
    )
    own = lax.all_to_all(packed, ROW, split_axis=0, concat_axis=0, tiled=True).reshape(SLOTS, D + 128)
    behind = move(own, TM, 1)
    frame_total = frame_count * lax.axis_size(TM)
    row_total = row_count * lax.axis_size(ROW)
    own_target, row_target, last_row_target, time_target, *positions = target_part(
        (frame_total, row_total), shift_rows, hold(pixels)
    )
    last_row_target = move(last_row_target, ROW, -1)
    row_target = move(row_target, ROW, -1)
    time_target = move(time_target, TM, 1)
    corner_target = move(last_row_target, TM, 1)

    tables = (mask_rows, *positions)
    *half_1, heads_1, w_qkv, w_out, w_head = early_part(
        shift_rows, own, *tables, hold(w_qkv), hold(w_out), hold(w_head)
    )
    *half_0, head_normed, head_scale, predicted = late_part(
        shift_rows, own, behind, *tables, half_1[0], heads_1, w_qkv, w_out, w_head
    )
    own_picked, behind_rows, local_total = backward_part(
        window_shift, *half_0, *half_1, head_normed, head_scale, predicted, w_qkv, w_out, w_head,
        own_target, row_target, last_row_target, time_target, corner_target,
    )
    other = move(local_total, "tm_1", 1)
    from_next = move(behind_rows, TM, -1)
    local_total = local_total + other
    turned = []
    for step in (1, 2, 3):
        turned.append(move(local_total, "tm_0", step))
    give = call(give_kernel, [((peers, 8, D + 256), BF)], [], in_space(VMEM, 8), 8)
    (sent,) = give(shift_rows, own, own_picked, from_next, local_total, *turned)
    back = lax.all_to_all(sent, ROW, split_axis=0, concat_axis=0, tiled=True)
    grad_scale = (frame_total * row_total * pixels.shape[2]) ** (-0.5)
    outputs = [((peers, slots, D), BF), ((8, 128), F32)]
    unpack = call(functools.partial(unpack_kernel, grad_scale), outputs, [], in_space(VMEM, 1), 8)
    d_visible, d_mask = unpack(back)
    return (d_visible.reshape(visible.shape), d_mask.reshape(D))


def solution(mesh):
    torus = Mesh(mesh.devices.reshape(4, 2, 4, 4), ALL)
    return jax.shard_map(
        per_device,
        mesh=torus,
        in_specs=(
            P(TM, ROW, None, None, None),
            P(TM, ROW, None, None),
            P(),
            P(),
            P(),
            P(),
            P(),
            P(TM, ROW, None, None),
        ),
        out_specs=(P(TM, ROW, None, None, None), P()),
        check_vma=False,
    )
```
